32 devices in a mesh: lev: 4 (over z), wav: 8 (over y, x, core).
Axes of the slice: x: 2, y: 2, z: 4, core: 2. Of those that a mesh axis runs over, the one named last changes fastest.
Arguments:
- grid_field: float32 [8, 1216, 1216], P('lev', 'wav'), may hold values from -6 to 6
- truncation_limit: int32 [1216], replicated, may hold values from -1 to 607, as said below
- diffusion_order: int32 [8], P('lev'), may hold values from 1 to 4
- diffusion_strength: float32 [8], P('lev'), may hold values from 2 to 50
- mass_weight: float32 [8], P('lev'), may hold values from 0.25 to 4
Outputs:
- filtered: float32 [8, 1216, 1216], P('lev', 'wav')
- energies: float32 [8], P('lev')
- total_energy: float32 [], replicated
The draws below stay inside these ranges and needn't reach their ends.
Inputs may be any that keep to these rules, and one draw needn't show every extreme that they name: `truncation_limit`: the largest |wavenumber(q)| kept at index p, with wavenumber(m) = m below 608 and m - 1216 otherwise; the kept set is an ellipse about wavenumber zero; the value at p equals the value at 1216 - p; -1 where nothing is kept; the value at p = 0 is 607.
All inputs are finite; a program needn't handle non-finite values.
Results may differ from the reference program's by a relative error of at most 0.000071.
Values sent between devices are 32-bit elements.
A program may use at most 64 MiB of HBM per device.

```python
import math
import jax
import jax.numpy as jnp
from jax import lax

N = 1216
SLABS = 8


def draw_truncation_limit(key, part):
    axis_second = jax.random.randint(key, (), 3 * N // 10, N // 2)
    axis_first = N // 2 - 1
    positions = jnp.arange(N, dtype=jnp.int32)
    distance = jnp.abs(jnp.where(positions < N // 2, positions, positions - N))
    steps_first = jnp.arange(N // 2 + 1, dtype=jnp.int32)
    scaled_second = distance * 1000 // axis_second
    scaled_first = steps_first * 1000 // axis_first
    inside = scaled_second[:, None] ** 2 + scaled_first[None, :] ** 2 <= 1000000
    return (jnp.sum(inside.astype(jnp.int32), axis=1) - 1).astype(jnp.int32)


def set_ends(drawn, key, smallest, largest):
    place = [jax.random.randint(jax.random.fold_in(key, axis), (), 0, length) for axis, length in enumerate(drawn.shape)]
    longest = drawn.shape.index(max(drawn.shape))
    neighbour = place[:longest] + [(place[longest] + 1) % drawn.shape[longest]] + place[longest + 1:]
    return drawn.at[tuple(place)].set(smallest).at[tuple(neighbour)].set(largest)


def block_levels(key, extent, pieces, low, largest):
    loudness, own = 1.0, jax.random.fold_in(key, 6)
    for position, shards_of in pieces:
        draws = jnp.exp(jax.random.uniform(jax.random.fold_in(own, position), (shards_of,), jnp.float32, low / len(pieces), largest / len(pieces)))
        loudness = loudness * jnp.repeat(draws, extent[position] // shards_of).reshape([-1 if axis == position else 1 for axis in range(len(extent))])
    return loudness


def centred(own_key, extent, spread, bound, split=(), kind=jnp.bfloat16):
    gain = block_levels(own_key, extent, split, -0.22, 0.18) if split else 1.0
    drawn = jax.random.normal(own_key, extent, jnp.float32) * spread * gain
    return jnp.minimum(jnp.maximum(drawn, -bound), bound).astype(kind)


def setup_inputs(seed: int = 0) -> dict:
    key_list = jax.random.split(jax.random.key(seed), 6)
    grid_field = centred(key_list[0], (SLABS, N, N), 1.0, 6.0, ((0, 4), (1, 8)), jnp.float32)
    truncation_limit = draw_truncation_limit(jax.random.fold_in(key_list[5], 71), 0)
    diffusion_order = set_ends(jax.random.randint(key_list[2], (SLABS,), 1, 5), jax.random.fold_in(key_list[2], 1), 1, 4).astype(jnp.int32)
    diffusion_strength = jnp.clip(jnp.exp(math.log(50.0) - 3.218876 * jax.random.uniform(key_list[3], (SLABS,), jnp.float32) ** block_levels(key_list[3], (SLABS,), ((0, 4),), -0.2, 0.2)), 2.0, 50.0)
    mass_weight = jnp.clip(jnp.exp(math.log(4.0) - 2.7725887 * jax.random.uniform(key_list[4], (SLABS,), jnp.float32) ** block_levels(key_list[4], (SLABS,), ((0, 4),), -0.2, 0.2)), 0.25, 4.0)
    return dict(grid_field=grid_field, truncation_limit=truncation_limit, diffusion_order=diffusion_order, diffusion_strength=diffusion_strength, mass_weight=mass_weight)


def signed(positions, length):
    return jnp.where(positions < length // 2, positions, positions - length)


def reference(grid_field, truncation_limit, diffusion_order, diffusion_strength, mass_weight):
    positions = jnp.arange(N, dtype=jnp.int32)
    signed_index = signed(positions, N)
    wavenumber = signed_index.astype(jnp.float32)
    scaled_radius = (wavenumber[:, None] ** 2 + wavenumber[None, :] ** 2) / (0.5 * N) ** 2
    inside = (jnp.abs(signed_index)[None, :] <= truncation_limit[:, None]).astype(jnp.float32)

    def one_slab(members):
        slab_field, degree, strength = members
        spectrum = jnp.fft.fft2(slab_field).T
        damping = inside / (1.0 + strength * jnp.power(scaled_radius, degree.astype(jnp.float32)))
        damped = spectrum * damping
        energy = jnp.sum(jnp.real(damped) ** 2 + jnp.imag(damped) ** 2) / float(N) ** 4
        filtered = jnp.real(jnp.fft.ifft2(damped.T))
        return filtered, energy

    filtered, energies = lax.map(one_slab, (grid_field, diffusion_order, diffusion_strength))
    total_energy = jnp.sum(mass_weight * energies) / SLABS
    return filtered, energies, total_energy
```

```python
import functools

import jax
import jax.numpy as jnp
import numpy as np
from jax import lax
from jax.experimental import pallas as pl
from jax.experimental.pallas import tpu as pltpu
from jax.sharding import PartitionSpec as P

product_precision = lax.Precision.HIGH


def tables(length):
    step = 32
    coarse = -(-length // step)
    columns = np.arange(length)
    high = 2.0 * np.pi / length * (np.arange(coarse)[:, None] * step * columns[None, :] % length)
    low = 2.0 * np.pi / length * (np.arange(step)[:, None] * columns[None, :] % length)
    cos_high, sin_high = (jnp.asarray(f(high), jnp.float32)[:, None] for f in (np.cos, np.sin))
    cos_low, sin_low = (jnp.asarray(f(low), jnp.float32)[None] for f in (np.cos, np.sin))
    cosine = cos_high * cos_low - sin_high * sin_low
    sine = sin_high * cos_low + cos_high * sin_low
    return tuple(t.reshape(coarse * step, length)[:length] for t in (cosine, sine))


def signed(positions, length):
    return jnp.where(positions < length // 2, positions, positions - length)


def transform(values, cosine_table, sine_table, direction):
    with_cosine = jnp.einsum("scpi,iq->scpq", values, cosine_table, precision=product_precision)
    with_sine = jnp.einsum("scpi,iq->scpq", values, sine_table, precision=product_precision)
    if direction < 0:
        real_part = with_cosine[:, 0] + with_sine[:, 1]
        imaginary = with_cosine[:, 1] - with_sine[:, 0]
    else:
        real_part = with_cosine[:, 0] - with_sine[:, 1]
        imaginary = with_cosine[:, 1] + with_sine[:, 0]
    return jnp.stack([real_part, imaginary], axis=1)


def damping(wave_rows, limits, length, diffusion_order, diffusion_strength):
    wave_first = signed(jnp.arange(length, dtype=jnp.int32), length)
    rows_float = wave_rows.astype(jnp.float32)
    first_float = wave_first.astype(jnp.float32)
    scaled_radius = (rows_float[:, None] ** 2 + first_float[None, :] ** 2) / (0.5 * length) ** 2
    inside = (jnp.abs(wave_first)[None, :] <= limits[:, None]).astype(jnp.float32)
    powered = jnp.power(scaled_radius[None], diffusion_order.astype(jnp.float32)[:, None, None])
    return inside[None] / (1.0 + diffusion_strength[:, None, None] * powered)


def mirrored(values):
    return jnp.roll(jnp.flip(values, -1), 1, -1)


def half_plane(
    grid_field, truncation_limit, diffusion_order, diffusion_strength, cosine_table, sine_table
):
    length = grid_field.shape[2]
    half = length // 2
    row_real = jnp.einsum("sij,jl->sli", grid_field, cosine_table[:, :half], precision=product_precision)
    row_imag = -jnp.einsum("sij,jl->sli", grid_field, sine_table[:, :half], precision=product_precision)
    nyquist = jnp.einsum("sij,j->si", grid_field, cosine_table[:, half], precision=product_precision)
    zero_row = (jnp.arange(half, dtype=jnp.int32) == 0)[None, :, None]
    row_imag = jnp.where(zero_row, nyquist[:, None, :], row_imag)
    along_rows = jnp.stack([row_real, row_imag], axis=1)
    spectrum = transform(
        lax.all_to_all(along_rows, "wav", split_axis=2, concat_axis=3, tiled=True),
        cosine_table,
        sine_table,
        -1,
    )
    column_count = spectrum.shape[2]
    wav_index = lax.axis_index("wav")
    offset = wav_index * column_count
    wave_rows = offset + jnp.arange(column_count, dtype=jnp.int32)
    limits = lax.dynamic_slice(truncation_limit, (offset,), (column_count,))
    damp_main = damping(wave_rows, limits, length, diffusion_order, diffusion_strength)
    nyquist_rows = signed(jnp.full((1,), half, jnp.int32), length)
    damp_top = damping(
        nyquist_rows, truncation_limit[half : half + 1], length, diffusion_order, diffusion_strength
    )[:, 0]
    damped = spectrum * damp_main[:, None]
    packed_real = spectrum[:, 0, 0, :]
    packed_imag = spectrum[:, 1, 0, :]
    back_real = mirrored(packed_real)
    back_imag = mirrored(packed_imag)
    zero_real = (packed_real + back_real) * 0.5 * damp_main[:, 0]
    zero_imag = (packed_imag - back_imag) * 0.5 * damp_main[:, 0]
    top_real = (packed_imag + back_imag) * 0.5 * damp_top
    top_imag = (back_real - packed_real) * 0.5 * damp_top
    is_zero = wave_rows == 0
    column_weight = jnp.where(is_zero, 0.0, 2.0).astype(jnp.float32)
    edge = jnp.sum(zero_real**2 + zero_imag**2 + top_real**2 + top_imag**2, axis=-1)
    main_sum = jnp.sum(damped * damped * column_weight[None, None, :, None], axis=(1, 2, 3))
    partial_value = (main_sum + jnp.where(wav_index == 0, edge, 0.0)) / float(length) ** 4
    zero_column = is_zero[None, :, None]
    repacked = jnp.stack(
        [
            jnp.where(zero_column, (zero_real - top_imag)[:, None, :], damped[:, 0]),
            jnp.where(zero_column, (zero_imag + top_real)[:, None, :], damped[:, 1]),
        ],
        axis=1,
    )
    along_first = transform(repacked, cosine_table, sine_table, 1)
    inverse_area = 1.0 / float(length) ** 2
    received = lax.all_to_all(along_first, "wav", split_axis=3, concat_axis=2, tiled=True)
    row_weight = jnp.where(jnp.arange(half, dtype=jnp.int32) == 0, 1.0, 2.0).astype(jnp.float32)[
        :, None
    ]
    with_cosine = jnp.einsum(
        "spi,pj->sij", received[:, 0] * row_weight, cosine_table[:half], precision=product_precision
    )
    with_sine = jnp.einsum(
        "spi,pj->sij", received[:, 1] * row_weight, sine_table[:half], precision=product_precision
    )
    top_term = received[:, 1, 0, :][:, :, None] * cosine_table[half][None, None, :]
    filtered = (with_cosine - with_sine + top_term) * inverse_area
    return (filtered, partial_value)


LANES = 128
HALF = LANES // 2
MESH = pl.DeviceIdType.MESH


def halves(values):
    high = values.astype(jnp.bfloat16)
    return high, (values - high.astype(jnp.float32)).astype(jnp.bfloat16)


def product(left, right):
    dot = functools.partial(jnp.dot, preferred_element_type=jnp.float32)
    return dot(left[0], right[0]) + dot(left[1], right[0]) + dot(left[0], right[1])


def swap(value):
    count = value.shape[1] // LANES
    turned = [pltpu.roll(value[:, n * LANES : (n + 1) * LANES], HALF, 1) for n in range(count)]
    return jnp.concatenate(turned, 1) if count > 1 else turned[0]


def eight_points(x, sign, signs):
    turn = signs if sign < 0 else -signs

    def four(p, q, r, t):
        a0, a1, a2, a3 = p + r, p - r, q + t, swap(q - t) * turn
        return a0 + a2, a1 + a3, a0 - a2, a1 - a3

    e = four(x[0], x[2], x[4], x[6])
    o = four(x[1], x[3], x[5], x[7])
    root = 0.5**0.5
    odd = (
        o[0],
        root * (o[1] + swap(o[1]) * turn),
        swap(o[2]) * turn,
        root * (swap(o[3]) * turn - o[3]),
    )
    return [e[n] + odd[n] for n in range(4)] + [e[n] - odd[n] for n in range(4)]


def pieces(rows, group_rows, groups):
    found = []
    for group in range(groups):
        start, stop = group * group_rows, min((group + 1) * group_rows, 2 * rows)
        while start < stop:
            part = start // rows
            end = min(stop, (part + 1) * rows)
            found.append((group, start - group * group_rows, part, start - part * rows, end - start))
            start = end
    return found


def fused_kernel(
    sizes,
    grid_hbm, limit_hbm, order_hbm, strength_hbm, mass_hbm, coarse_hbm, fine_hbm,
    back_coarse_hbm, back_fine_hbm, twiddle_hbm, base_hbm,
    sum_ref, tail_ref, tail_table, energy_ref,
    grid, limit_ref, order_ref, strength_ref, mass_ref, coarse_ref, fine_ref,
    back_coarse, back_fine, twiddle, base, grid_parts, table, back_table,
    sent_a, sent_b, sent_c, got_a, got_b, got_c, back_a, back_b, back_c, home_a, home_b, home_c,
    rest, work, damp, energy_sums, energy_mine, energy_wav, energy_lev,
    load_sems, send_sems, recv_sems, local_sems, wav_send, wav_recv, lev_send, lev_recv, ready,
):
    slabs, rows, length, wav, lev, quarters, columns, padded, tail, groups, group_rows, fine_rows = sizes
    half = length // 2
    quarter_lanes = LANES // 2
    part_lanes = quarter_lanes // 2
    me = lax.axis_index("wav")
    level = lax.axis_index("lev")
    my_quarter, my_slab = me // slabs, me % slabs

    barrier = pltpu.get_barrier_semaphore()

    @pl.loop(1, wav)
    def _(step):
        pl.semaphore_signal(barrier, inc=1, device_id=(level, (me + step) % wav), device_id_type=MESH)

    for other in range(1, lev):
        @pl.when(level < other)
        def _():
            pl.semaphore_signal(barrier, inc=1, device_id=(other, me), device_id_type=MESH)

    loads = [
        pltpu.make_async_copy(src, dst, load_sems.at[n])
        for n, (src, dst) in enumerate(
            (
                (coarse_hbm, coarse_ref), (fine_hbm, fine_ref), (grid_hbm, grid),
                (limit_hbm, limit_ref), (order_hbm, order_ref), (strength_hbm, strength_ref),
                (mass_hbm, mass_ref), (twiddle_hbm, twiddle), (base_hbm, base),
                (back_coarse_hbm, back_coarse), (back_fine_hbm, back_fine),
            )
        )
    ]
    for load in loads:
        load.start()

    def quarter_of(step):
        down, across = 1 - step % 2, 1 - step // 2
        y, x = my_quarter // 2, my_quarter % 2
        return (y + down - 2 * y * down) * 2 + (x + across - 2 * x * across)

    def push(source, target, phase, w):
        @pl.when(w != me)
        def _():
            pltpu.make_async_remote_copy(
                src_ref=source.at[w], dst_ref=target.at[me],
                send_sem=send_sems.at[phase, w], recv_sem=recv_sems.at[phase, me],
                device_id=(level, w), device_id_type=MESH,
            ).start()

        @pl.when(w == me)
        def _():
            pltpu.make_async_copy(source.at[w], target.at[w], local_sems.at[phase]).start()

    def push_all(source, target, phase):
        @pl.loop(0, quarters)
        def _(step):
            for slab in range(slabs):
                push(source, target, phase, quarter_of(step) * slabs + slab)

    def arrive(source, target, phase, w):
        @pl.when(w != me)
        def _():
            pltpu.make_async_remote_copy(
                src_ref=source.at[w], dst_ref=target.at[w],
                send_sem=send_sems.at[phase, w], recv_sem=recv_sems.at[phase, w],
                device_id=(level, w), device_id_type=MESH,
            ).wait()

        @pl.when(w == me)
        def _():
            pltpu.make_async_copy(source.at[w], target.at[w], local_sems.at[phase]).wait()

    lane = lax.broadcasted_iota(jnp.int32, (1, LANES), 1)
    signs = jnp.where(lane < HALF, 1.0, -1.0)
    layout = pieces(rows, group_rows, groups)
    wide = (0, HALF)

    def inside_part(starts, part):
        return (lane >= starts[part]) & (lane < starts[part] + tail)

    def pack(tile, starts):
        shifted = {}
        for group, at, part, start, count in layout:
            piece = jnp.where(inside_part(starts, part), tile(start, count), 0.0)
            shift = (group * tail - starts[part]) % LANES
            shifted.setdefault(group, []).append(pltpu.roll(piece, shift, 1) if shift else piece)
        packed = jnp.zeros((group_rows, LANES), jnp.float32)
        for found in shifted.values():
            whole = jnp.concatenate(found, 0) if len(found) > 1 else found[0]
            if whole.shape[0] < group_rows:
                fill = jnp.zeros((group_rows - whole.shape[0], LANES), jnp.float32)
                whole = jnp.concatenate([whole, fill], 0)
            packed = packed + whole
        return packed

    def unpack(packed, starts):
        found = {0: [], 1: []}
        for group, at, part, start, count in layout:
            piece = packed[at : at + count]
            shift = (starts[part] - group * tail) % LANES
            piece = pltpu.roll(piece, shift, 1) if shift else piece
            found[part].append(jnp.where(inside_part(starts, part), piece, 0.0))
        return jnp.concatenate(found[0], 0) + jnp.concatenate(found[1], 0)

    def quarter_starts(quarter):
        first = quarter % 2 * quarter_lanes
        return (first, first + part_lanes)

    loads[0].wait()
    loads[1].wait()

    @pl.loop(0, quarters + 1)
    def _(step):
        last = step // quarters
        piece = quarter_of(step % quarters) * (1 - last) + quarters * last
        cos_f, sin_f = fine_ref[0, piece], fine_ref[1, piece]

        @pl.loop(0, length // fine_rows, unroll=2)
        def _(block):
            cos_c, sin_c = coarse_ref[0, piece, pl.ds(block, 1)], coarse_ref[1, piece, pl.ds(block, 1)]
            span = pl.ds(pl.multiple_of(block * fine_rows, fine_rows), fine_rows)
            value_high, value_low = halves(cos_c * cos_f - sin_c * sin_f)
            table[0, span] = value_high
            table[1, span] = value_low

        @pl.when(step == 0)
        def _():
            loads[2].wait()
            high, low = halves(grid[...])
            grid_parts[0] = high
            grid_parts[1] = low

        result = product((grid_parts[0], grid_parts[1]), (table[0], table[1]))
        for slab in range(slabs):
            w = piece * slabs + slab
            sent_a[w] = result[slab * rows : (slab + 1) * rows, :LANES]
            sent_b[w] = result[slab * rows : (slab + 1) * rows, LANES:]

        @pl.when(step == 0)
        def _():
            pl.semaphore_wait(barrier, wav - 1 + level)

        @pl.when(step < quarters)
        def _():
            for slab in range(slabs):
                push(sent_a, got_a, 0, piece * slabs + slab)

        @pl.when(step == quarters - 1)
        def _():
            push_all(sent_b, got_b, 1)

    for quarter in range(quarters):
        from_ref = sent_b if quarter // 2 else sent_a
        for slab in range(slabs):
            sent_c[quarter * slabs + slab] = pack(
                lambda start, many: from_ref[wav + slab, start : start + many], quarter_starts(quarter)
            )
    push_all(sent_c, got_c, 2)

    for other in range(lev - 1):
        @pl.when(other < level)
        def _():
            pl.semaphore_signal(ready.at[level], inc=1, device_id=(other, me), device_id_type=MESH)

    for load in loads[3:]:
        load.wait()
    place = lax.broadcasted_iota(jnp.int32, (1, 3 * LANES), 1)
    column = place // LANES * HALF + place % HALF
    wave = my_quarter * columns + column
    valid = (column < columns) | ((column == columns) & (wave == half))
    single = (wave == 0) | (wave == half)
    out_weight = jnp.where(single, 1.0, 2.0) / float(length) ** 2
    energy_weight = jnp.where(single, 1.0, 0.5)
    all_limits = limit_ref[...].reshape(1, length)
    limits = jnp.full((1, 3 * LANES), -1, jnp.int32)
    for quarter in range(quarters):
        found = []
        for tile in range(3):
            start = quarter * columns + tile * HALF
            found += [all_limits[:, start : start + HALF]] * 2
        limits = jnp.where(my_quarter == quarter, jnp.concatenate(found, 1), limits)
    limits = jnp.where(valid, limits, -1)
    order = order_ref[my_slab]
    strength = strength_ref[my_slab]
    wave_square = wave.astype(jnp.float32) ** 2

    @pl.loop(0, wav)
    def _(m):
        row = lax.broadcasted_iota(jnp.int32, (padded, 1), 0)
        q = row * wav + m
        signed_q = jnp.where(q < half, q, q - length)
        radius = (wave_square + signed_q.astype(jnp.float32) ** 2) / (0.5 * length) ** 2
        square = radius * radius
        powered = jnp.where(order >= 3, square, 1.0) * jnp.where(order % 2 == 1, radius, square)
        inside = (jnp.abs(signed_q) <= limits) & (row < rows)
        damp[m] = jnp.where(inside, out_weight / (1.0 + strength * powered), 0.0)
        work[m, rows:] = jnp.zeros((padded - rows, LANES), jnp.float32)

    blocks = LANES // fine_rows
    plain = 2 * quarters * blocks

    def back_piece(at, target, span):
        cos_c, sin_c = back_coarse[0, pl.ds(at, 1)], back_coarse[1, pl.ds(at, 1)]
        value_high, value_low = halves(cos_c * back_fine[0] - sin_c * back_fine[1])
        target[0, span] = value_high
        target[1, span] = value_low

    @pl.loop(0, 2 * quarters)
    def _(n):
        @pl.loop(0, blocks)
        def _(block):
            span = pl.ds(pl.multiple_of(block * fine_rows, fine_rows), fine_rows)
            back_piece(n * blocks + block, back_table.at[n], span)

    @pl.loop(0, 2 * blocks)
    def _(block):
        back_piece(plain + block, tail_table, pl.ds(pl.multiple_of(block * fine_rows, fine_rows), fine_rows))

    sum_ref[...] = jnp.zeros_like(sum_ref)
    energy_sums[...] = jnp.zeros_like(energy_sums)

    def along(value):
        value_high, value_low = halves(value)
        stacked = jnp.concatenate([value_high, value_high, value_low], 0)
        return jnp.dot(base[...], stacked, preferred_element_type=jnp.float32)

    block_rows = 24
    batch = 2

    def in_blocks(body):
        @pl.loop(0, rows // block_rows)
        def _(block):
            body(pl.multiple_of(block * block_rows, 8), block_rows)

        if rows % block_rows:
            body(rows - rows % block_rows, rows % block_rows)

    def middle(tile, source, target):
        span_of = slice(tile * LANES, (tile + 1) * LANES)
        all_signs = jnp.concatenate([signs] * batch, 1)

        def split(start, many):
            span = pl.ds(start, many)
            for m, value in enumerate(eight_points([source[w, span] for w in range(wav)], -1, signs)):
                work[m, span] = value

        in_blocks(split)

        def residues(first, sums):
            found = range(first, first + batch)
            beside = lambda pick: jnp.concatenate([pick(m) for m in found], 1)
            packed_turn = beside(lambda m: twiddle[m])
            other_turn = swap(packed_turn)
            low = jnp.concatenate([lane] * batch, 1) < HALF
            cos_t = jnp.where(low, packed_turn, other_turn)
            sin_t = jnp.where(low, other_turn, -packed_turn)
            value = beside(lambda m: work[m])
            both = along(value * cos_t + swap(value) * sin_t)
            value = both[:padded] + swap(both[padded:]) * all_signs
            value = value * beside(lambda m: damp[m, :, span_of])
            sums = sums + jnp.sum((value * value).reshape(padded // 8, 8, batch * LANES), axis=0)
            both = along(value)
            value = both[:padded] - swap(both[padded:]) * all_signs
            value = value * cos_t - swap(value) * sin_t
            for n, m in enumerate(found):
                work[m] = value[:, n * LANES : (n + 1) * LANES]
            return sums

        sums = jnp.zeros((8, batch * LANES), jnp.float32)
        for first in range(0, wav, batch):
            sums = residues(first, sums)
        sums = sum(sums[:, n * LANES : (n + 1) * LANES] for n in range(batch))
        energy_sums[...] += sums * energy_weight[:, span_of]

        if tile == 2:
            announce()

        def join(start, many):
            span = pl.ds(start, many)
            for w, value in enumerate(eight_points([work[m, span] for m in range(wav)], 1, signs)):
                target[w, span] = value

        in_blocks(join)

    def wav_copy(target, slot):
        return pltpu.make_async_remote_copy(
            src_ref=energy_mine, dst_ref=energy_wav.at[slot],
            send_sem=wav_send.at[target], recv_sem=wav_recv.at[slot],
            device_id=(level, target), device_id_type=MESH,
        )

    def lev_copy(target, slot):
        return pltpu.make_async_remote_copy(
            src_ref=energy_lev.at[level], dst_ref=energy_lev.at[slot],
            send_sem=lev_send.at[target], recv_sem=lev_recv.at[slot],
            device_id=(target, me), device_id_type=MESH,
        )

    def announce():
        mine = jnp.sum(energy_sums[...], axis=0, keepdims=True)
        energy_mine[...] = mine
        energy_wav[me] = mine

        @pl.loop(1, wav)
        def _(step):
            wav_copy((me + step) % wav, me).start()

    @pl.loop(0, wav)
    def _(w):
        arrive(sent_a, got_a, 0, w)

    middle(0, got_a, back_a)
    push_all(back_a, home_a, 3)

    @pl.loop(0, wav)
    def _(w):
        arrive(sent_b, got_b, 1, w)

    middle(1, got_b, back_b)
    push_all(back_b, home_b, 4)

    @pl.loop(0, wav)
    def _(w):
        arrive(sent_c, got_c, 2, w)
        rest[w] = unpack(got_c[w], wide)

    middle(2, rest, rest)

    @pl.loop(0, quarters)
    def _(step):
        for slab in range(slabs):
            w = quarter_of(step) * slabs + slab
            back_c[w] = pack(lambda start, many: rest[w, start : start + many], wide)
            push(back_c, home_c, 5, w)

    def finish(tile, phase, back, home):
        @pl.loop(0, quarters // 2)
        def _(pair):
            found, right = [], ([], [])
            for n in range(2):
                quarter = quarter_of((2 * pair + n + quarters - 1) % quarters)
                stacked = []
                for slab in range(slabs):
                    w = quarter * slabs + slab
                    arrive(back, home, phase, w)
                    stacked.append(home[w])
                found.append(jnp.concatenate(stacked, 0))
                for part in range(2):
                    right[part].append(back_table[tile * quarters + quarter, part])
            left = halves(jnp.concatenate(found, 1))
            sum_ref[...] += product(left, [jnp.concatenate(part, 0) for part in right])

    finish(0, 3, back_a, home_a)
    finish(1, 4, back_b, home_b)

    @pl.loop(1, wav)
    def _(step):
        source = (me + step) % wav
        wav_copy(source, source).wait()

    slab_sums = []
    for slab in range(slabs):
        total = energy_wav[slab]
        for quarter in range(1, quarters):
            total = total + energy_wav[quarter * slabs + slab]
        slab_sums.append(total)
    weighted = slab_sums[0] * mass_ref[0]
    for slab in range(1, slabs):
        weighted = weighted + slab_sums[slab] * mass_ref[slab]
    energy_lev[level] = weighted

    for other in range(1, lev):
        @pl.when(level < other)
        def _():
            pl.semaphore_wait(ready.at[other], 1)

    for other in range(lev):
        @pl.when(level != other)
        def _():
            lev_copy(other, level).start()

    @pl.loop(0, wav)
    def _(w):
        arrive(back_c, home_c, 5, w)

    for side in range(2):
        for slab in range(slabs):
            value = sum(
                unpack(home_c[quarter * slabs + slab], quarter_starts(quarter))
                for quarter in range(2 * side, 2 * side + 2)
            )
            value_high, value_low = halves(value)
            at = (slice(slab * rows, (slab + 1) * rows), slice(side * LANES, (side + 1) * LANES))
            tail_ref[(0,) + at] = value_high
            tail_ref[(1,) + at] = value_low

    for other in range(lev):
        @pl.when(level != other)
        def _():
            lev_copy(other, other).wait()

    total = energy_lev[0]
    for other in range(1, lev):
        total = total + energy_lev[other]
    fill = jnp.zeros((8 - slabs - 1, LANES), jnp.float32)
    energy_ref[...] = jnp.concatenate(slab_sums + [total / (lev * slabs), fill], 0)


def last_kernel(
    slabs, spans, sum_ref, tail_ref, tail_table, energy_ref, out_hbm, energies_hbm, total_hbm,
    out, energies, total, sems,
):
    sums = jnp.sum(energy_ref[...], axis=1, keepdims=True)
    for slab in range(slabs):
        energies[slab] = sums[slab, 0]
    total[0] = sums[slabs, 0]
    copies = [
        pltpu.make_async_copy(energies, energies_hbm, sems.at[0]),
        pltpu.make_async_copy(total, total_hbm, sems.at[1]),
    ]
    for copy in copies:
        copy.start()
    left = (tail_ref[0], tail_ref[1])
    for n, (start, stop) in enumerate(spans):
        out[:, start:stop] = sum_ref[:, start:stop] + product(
            left, (tail_table[0, :, start:stop], tail_table[1, :, start:stop])
        )
        copies.append(
            pltpu.make_async_copy(out.at[:, start:stop], out_hbm.at[:, start:stop], sems.at[2 + n])
        )
        copies[-1].start()
    for copy in copies:
        copy.wait()


def cos_sin(phases, length):
    angles = 2.0 * np.pi / length * (phases % length)
    return np.stack([np.cos(angles), np.sin(angles)])


def fused(grid_field, truncation_limit, diffusion_order, diffusion_strength, mass_weight):
    slabs, rows, length = grid_field.shape
    wav, lev = lax.axis_size("wav"), lax.axis_size("lev")
    quarters = wav // slabs
    columns = length // 2 // quarters
    tail = columns + 1 - LANES
    groups = LANES // tail
    group_rows = -(-(-(-2 * rows // groups)) // 8) * 8
    padded = -(-rows // 16) * 16
    fine_rows = 32
    sizes = (slabs, rows, length, wav, lev, quarters, columns, padded, tail, groups, group_rows, fine_rows)
    turn = length // 4
    place = np.arange(2 * LANES)
    starts = np.arange(quarters) * columns
    plain_waves = starts[:, None] + (place // LANES * HALF + place % HALF)[None]
    plain_phase = np.broadcast_to((place % LANES >= HALF) * turn, plain_waves.shape)
    part = LANES // 4
    tail_waves = (starts[place // HALF] + LANES + place % part)[None]
    tail_phase = (place % HALF >= part)[None] * turn
    waves = np.concatenate([plain_waves, tail_waves])
    phase = np.concatenate([plain_phase, tail_phase])
    steps = np.arange(length // fine_rows) * fine_rows
    near = np.arange(fine_rows)
    positions = np.arange(length)
    single = lambda array: jnp.asarray(array, jnp.float32)
    coarse = single(cos_sin(steps[None, :, None] * waves[:, None, :], length))
    fine = single(cos_sin(near[None, :, None] * waves[:, None, :] + phase[:, None, :], length))
    by_tile = lambda array: np.concatenate(
        [array[:quarters, :LANES].ravel(), array[:quarters, LANES:].ravel(), array[quarters]]
    )[::fine_rows]
    back_coarse = single(
        cos_sin(by_tile(waves)[:, None] * positions[None] + by_tile(phase)[:, None], length)
    )
    back_fine = single(cos_sin(near[:, None] * positions[None], length))
    inner = np.arange(padded)
    turns = cos_sin(np.arange(wav)[:, None, None] * inner[None, :, None], length)
    twiddle = single(np.repeat(turns, HALF, 3).transpose(1, 2, 0, 3).reshape(wav, padded, LANES))
    base_exact = cos_sin(wav * inner[:, None] * inner[None], length)
    base_exact = base_exact * ((inner[:, None] < rows) & (inner[None] < rows))
    base_exact = base_exact.reshape(2 * padded, padded).astype(np.float32)
    base_high = base_exact.astype(jnp.bfloat16)
    base_low = (base_exact - base_high.astype(np.float32)).astype(jnp.bfloat16)
    base = jnp.asarray(np.concatenate([base_high, base_low, base_high], 1))
    vmem, hbm = pl.BlockSpec(memory_space=pltpu.VMEM), pl.BlockSpec(memory_space=pltpu.HBM)
    f32, bf16, i32 = jnp.float32, jnp.bfloat16, jnp.int32
    sent = pltpu.VMEM((wav + slabs, rows, LANES), f32)
    whole = pltpu.VMEM((wav, rows, LANES), f32)
    small = pltpu.VMEM((wav, group_rows, LANES), f32)
    dma = pltpu.SemaphoreType.DMA
    partial_sum, tails, tail_table, energy_rows = pl.pallas_call(
        functools.partial(fused_kernel, sizes),
        out_shape=(
            jax.ShapeDtypeStruct((slabs * rows, length), f32),
            jax.ShapeDtypeStruct((2, slabs * rows, 2 * LANES), bf16),
            jax.ShapeDtypeStruct((2, 2 * LANES, length), bf16),
            jax.ShapeDtypeStruct((8, LANES), f32),
        ),
        in_specs=[hbm] * 11,
        out_specs=(vmem,) * 4,
        scratch_shapes=[
            pltpu.VMEM((slabs * rows, length), f32),
            pltpu.VMEM((length,), i32),
            pltpu.SMEM((slabs,), i32),
            pltpu.SMEM((slabs,), f32),
            pltpu.SMEM((slabs,), f32),
            pltpu.VMEM(coarse.shape, f32),
            pltpu.VMEM(fine.shape, f32),
            pltpu.VMEM(back_coarse.shape, f32),
            pltpu.VMEM(back_fine.shape, f32),
            pltpu.VMEM(twiddle.shape, f32),
            pltpu.VMEM(base.shape, bf16),
            pltpu.VMEM((2, slabs * rows, length), bf16),
            pltpu.VMEM((2, length, 2 * LANES), bf16),
            pltpu.VMEM((2 * quarters, 2, LANES, length), bf16),
            sent, sent, small, whole, whole, small, whole, whole, small, whole, whole, small,
            whole,
            pltpu.VMEM((wav, padded, LANES), f32),
            pltpu.VMEM((wav, padded, 3 * LANES), f32),
            pltpu.VMEM((8, LANES), f32),
            pltpu.VMEM((1, LANES), f32),
            pltpu.VMEM((wav, 1, LANES), f32),
            pltpu.VMEM((lev, 1, LANES), f32),
            dma((11,)), dma((6, wav)), dma((6, wav)), dma((6,)),
            dma((wav,)), dma((wav,)), dma((lev,)), dma((lev,)),
            pltpu.SemaphoreType.REGULAR((lev,)),
        ],
        compiler_params=pltpu.CompilerParams(
            collective_id=0, has_side_effects=True, vmem_limit_bytes=40 * 1024 * 1024
        ),
        name="fused_step",
    )(
        *(
            pltpu.with_memory_space_constraint(array, pltpu.HBM)
            for array in (
                grid_field.reshape(slabs * rows, length), truncation_limit, diffusion_order,
                diffusion_strength, mass_weight, coarse, fine, back_coarse, back_fine, twiddle, base,
            )
        )
    )
    spans = [(at, min(at + 2 * LANES, length)) for at in range(0, length, 2 * LANES)]
    filtered, energies, total = pl.pallas_call(
        functools.partial(last_kernel, slabs, spans),
        out_shape=(
            jax.ShapeDtypeStruct((slabs * rows, length), f32),
            jax.ShapeDtypeStruct((slabs,), f32),
            jax.ShapeDtypeStruct((1,), f32),
        ),
        in_specs=[vmem] * 4,
        out_specs=(hbm,) * 3,
        scratch_shapes=[
            pltpu.VMEM((slabs * rows, length), f32),
            pltpu.SMEM((slabs,), f32),
            pltpu.SMEM((1,), f32),
            dma((2 + len(spans),)),
        ],
        compiler_params=pltpu.CompilerParams(vmem_limit_bytes=12 * 1024 * 1024),
        name="last_product",
    )(partial_sum, tails, tail_table, energy_rows)
    return filtered.reshape(slabs, rows, length), energies, total[0]


def fits(shape):
    slabs, rows, length = shape
    wav = lax.axis_size("wav")
    if wav != 8 or slabs != 2 or rows % 8 or length % 16 or length != rows * wav:
        return False
    columns = length * slabs // 2 // wav
    return length % 32 == 0 and LANES <= columns < LANES + LANES // 4


def local(grid_field, truncation_limit, diffusion_order, diffusion_strength, mass_weight):
    slab_count, row_count, length = grid_field.shape
    if fits(grid_field.shape):
        return fused(
            grid_field, truncation_limit, diffusion_order, diffusion_strength, mass_weight
        )
    cosine_table, sine_table = tables(length)
    filtered, partial_value = half_plane(
        grid_field, truncation_limit, diffusion_order, diffusion_strength, cosine_table, sine_table
    )
    total_slabs = lax.axis_size("lev") * slab_count
    energies = lax.psum(partial_value, "wav")
    weighted_sum = lax.psum(jnp.sum(mass_weight * energies), "lev")
    total_energy = weighted_sum / total_slabs
    return (filtered, energies, total_energy)


def solution(mesh):
    placed = (P("lev", "wav", None), P(), P("lev"), P("lev"), P("lev"))
    return jax.shard_map(
        local,
        mesh=mesh,
        in_specs=placed,
        out_specs=(P("lev", "wav", None), P("lev"), P()),
        check_vma=False,
    )
```

```python
import functools

import jax
import jax.numpy as jnp
import numpy as np
from jax import lax
from jax.experimental import pallas as pl
from jax.experimental.pallas import tpu as pltpu
from jax.sharding import PartitionSpec as P

product_precision = lax.Precision.HIGH


def tables(length):
    step = 32
    coarse = -(-length // step)
    columns = np.arange(length)
    high = 2.0 * np.pi / length * (np.arange(coarse)[:, None] * step * columns[None, :] % length)
    low = 2.0 * np.pi / length * (np.arange(step)[:, None] * columns[None, :] % length)
    cos_high, sin_high = (jnp.asarray(f(high), jnp.float32)[:, None] for f in (np.cos, np.sin))
    cos_low, sin_low = (jnp.asarray(f(low), jnp.float32)[None] for f in (np.cos, np.sin))
    cosine = cos_high * cos_low - sin_high * sin_low
    sine = sin_high * cos_low + cos_high * sin_low
    return tuple(t.reshape(coarse * step, length)[:length] for t in (cosine, sine))


def signed(positions, length):
    return jnp.where(positions < length // 2, positions, positions - length)


def transform(values, cosine_table, sine_table, direction):
    with_cosine = jnp.einsum("scpi,iq->scpq", values, cosine_table, precision=product_precision)
    with_sine = jnp.einsum("scpi,iq->scpq", values, sine_table, precision=product_precision)
    if direction < 0:
        real_part = with_cosine[:, 0] + with_sine[:, 1]
        imaginary = with_cosine[:, 1] - with_sine[:, 0]
    else:
        real_part = with_cosine[:, 0] - with_sine[:, 1]
        imaginary = with_cosine[:, 1] + with_sine[:, 0]
    return jnp.stack([real_part, imaginary], axis=1)


def damping(wave_rows, limits, length, diffusion_order, diffusion_strength):
    wave_first = signed(jnp.arange(length, dtype=jnp.int32), length)
    rows_float = wave_rows.astype(jnp.float32)
    first_float = wave_first.astype(jnp.float32)
    scaled_radius = (rows_float[:, None] ** 2 + first_float[None, :] ** 2) / (0.5 * length) ** 2
    inside = (jnp.abs(wave_first)[None, :] <= limits[:, None]).astype(jnp.float32)
    powered = jnp.power(scaled_radius[None], diffusion_order.astype(jnp.float32)[:, None, None])
    return inside[None] / (1.0 + diffusion_strength[:, None, None] * powered)


def mirrored(values):
    return jnp.roll(jnp.flip(values, -1), 1, -1)


def half_plane(
    grid_field, truncation_limit, diffusion_order, diffusion_strength, cosine_table, sine_table
):
    length = grid_field.shape[2]
    half = length // 2
    row_real = jnp.einsum("sij,jl->sli", grid_field, cosine_table[:, :half], precision=product_precision)
    row_imag = -jnp.einsum("sij,jl->sli", grid_field, sine_table[:, :half], precision=product_precision)
    nyquist = jnp.einsum("sij,j->si", grid_field, cosine_table[:, half], precision=product_precision)
    zero_row = (jnp.arange(half, dtype=jnp.int32) == 0)[None, :, None]
    row_imag = jnp.where(zero_row, nyquist[:, None, :], row_imag)
    along_rows = jnp.stack([row_real, row_imag], axis=1)
    spectrum = transform(
        lax.all_to_all(along_rows, "wav", split_axis=2, concat_axis=3, tiled=True),
        cosine_table,
        sine_table,
        -1,
    )
    column_count = spectrum.shape[2]
    wav_index = lax.axis_index("wav")
    offset = wav_index * column_count
    wave_rows = offset + jnp.arange(column_count, dtype=jnp.int32)
    limits = lax.dynamic_slice(truncation_limit, (offset,), (column_count,))
    damp_main = damping(wave_rows, limits, length, diffusion_order, diffusion_strength)
    nyquist_rows = signed(jnp.full((1,), half, jnp.int32), length)
    damp_top = damping(
        nyquist_rows, truncation_limit[half : half + 1], length, diffusion_order, diffusion_strength
    )[:, 0]
    damped = spectrum * damp_main[:, None]
    packed_real = spectrum[:, 0, 0, :]
    packed_imag = spectrum[:, 1, 0, :]
    back_real = mirrored(packed_real)
    back_imag = mirrored(packed_imag)
    zero_real = (packed_real + back_real) * 0.5 * damp_main[:, 0]
    zero_imag = (packed_imag - back_imag) * 0.5 * damp_main[:, 0]
    top_real = (packed_imag + back_imag) * 0.5 * damp_top
    top_imag = (back_real - packed_real) * 0.5 * damp_top
    is_zero = wave_rows == 0
    column_weight = jnp.where(is_zero, 0.0, 2.0).astype(jnp.float32)
    edge = jnp.sum(zero_real**2 + zero_imag**2 + top_real**2 + top_imag**2, axis=-1)
    main_sum = jnp.sum(damped * damped * column_weight[None, None, :, None], axis=(1, 2, 3))
    partial_value = (main_sum + jnp.where(wav_index == 0, edge, 0.0)) / float(length) ** 4
    zero_column = is_zero[None, :, None]
    repacked = jnp.stack(
        [
            jnp.where(zero_column, (zero_real - top_imag)[:, None, :], damped[:, 0]),
            jnp.where(zero_column, (zero_imag + top_real)[:, None, :], damped[:, 1]),
        ],
        axis=1,
    )
    along_first = transform(repacked, cosine_table, sine_table, 1)
    inverse_area = 1.0 / float(length) ** 2
    received = lax.all_to_all(along_first, "wav", split_axis=3, concat_axis=2, tiled=True)
    row_weight = jnp.where(jnp.arange(half, dtype=jnp.int32) == 0, 1.0, 2.0).astype(jnp.float32)[
        :, None
    ]
    with_cosine = jnp.einsum(
        "spi,pj->sij", received[:, 0] * row_weight, cosine_table[:half], precision=product_precision
    )
    with_sine = jnp.einsum(
        "spi,pj->sij", received[:, 1] * row_weight, sine_table[:half], precision=product_precision
    )
    top_term = received[:, 1, 0, :][:, :, None] * cosine_table[half][None, None, :]
    filtered = (with_cosine - with_sine + top_term) * inverse_area
    return (filtered, partial_value)


LANES = 128
HALF = LANES // 2
MESH = pl.DeviceIdType.MESH


def halves(values):
    high = values.astype(jnp.bfloat16)
    return high, (values - high.astype(jnp.float32)).astype(jnp.bfloat16)


def product(left, right):
    dot = functools.partial(jnp.dot, preferred_element_type=jnp.float32)
    return dot(left[0], right[0]) + dot(left[1], right[0]) + dot(left[0], right[1])


def swap(value):
    count = value.shape[1] // LANES
    turned = [pltpu.roll(value[:, n * LANES : (n + 1) * LANES], HALF, 1) for n in range(count)]
    return jnp.concatenate(turned, 1) if count > 1 else turned[0]


def eight_points(x, sign, signs):
    turn = signs if sign < 0 else -signs

    def four(p, q, r, t):
        a0, a1, a2, a3 = p + r, p - r, q + t, swap(q - t) * turn
        return a0 + a2, a1 + a3, a0 - a2, a1 - a3

    e = four(x[0], x[2], x[4], x[6])
    o = four(x[1], x[3], x[5], x[7])
    root = 0.5**0.5
    odd = (
        o[0],
        root * (o[1] + swap(o[1]) * turn),
        swap(o[2]) * turn,
        root * (swap(o[3]) * turn - o[3]),
    )
    return [e[n] + odd[n] for n in range(4)] + [e[n] - odd[n] for n in range(4)]


def pieces(rows, group_rows, groups):
    found = []
    for group in range(groups):
        start, stop = group * group_rows, min((group + 1) * group_rows, 2 * rows)
        while start < stop:
            part = start // rows
            end = min(stop, (part + 1) * rows)
            found.append((group, start - group * group_rows, part, start - part * rows, end - start))
            start = end
    return found


def fused_kernel(
    sizes,
    grid_hbm, limit_hbm, order_hbm, strength_hbm, mass_hbm, seeds_hbm, back_seeds_hbm, twiddle_hbm, base_hbm,
    sum_ref, tail_ref, tail_table, energy_ref,
    grid, limit_ref, order_ref, strength_ref, mass_ref, seeds, back_seeds, twiddle, base,
    grid_parts, table, back_table,
    sent_a, sent_b, sent_c, got_a, got_b, got_c, back_a, back_b, back_c, home_a, home_b, home_c,
    rest, work, damp, energy_sums, energy_wav, energy_lev,
    load_sems, send_sems, recv_sems, energy_sems, ready,
):
    slabs, rows, length, wav, lev, quarters, columns, padded, tail, groups, group_rows, fine_rows = sizes
    half = length // 2
    quarter_lanes = LANES // 2
    part_lanes = quarter_lanes // 2
    me = lax.axis_index("wav")
    level = lax.axis_index("lev")
    my_quarter, my_slab = me // slabs, me % slabs

    barrier = pltpu.get_barrier_semaphore()

    @pl.loop(1, wav)
    def _(step):
        pl.semaphore_signal(barrier, inc=1, device_id=(level, (me + step) % wav), device_id_type=MESH)

    for other in range(1, lev):
        @pl.when(level < other)
        def _():
            pl.semaphore_signal(barrier, inc=1, device_id=(other, me), device_id_type=MESH)

    def quarter_of(step):
        down, across = 1 - step % 2, 1 - step // 2
        y, x = my_quarter // 2, my_quarter % 2
        return (y + down - 2 * y * down) * 2 + (x + across - 2 * x * across)

    spans = [slice(at, min(at + 4 * LANES, length)) for at in range(0, length, 4 * LANES)]
    ahead = quarter_of(0)
    def load(source, target, sem):
        copy = pltpu.make_async_copy(source, target, load_sems.at[sem])
        copy.start()
        return copy

    first_load = load(seeds_hbm.at[:, ahead], seeds.at[:, quarters + 1], 0)
    grid_loads = [load(grid_hbm.at[:, span], grid.at[:, span], 1 + n) for n, span in enumerate(spans)]
    seeds_load = load(seeds_hbm, seeds.at[:, : quarters + 1], 1 + len(spans))

    def push(source, target, phase, recv, w):
        @pl.when(w != me)
        def _():
            pltpu.make_async_remote_copy(
                src_ref=source.at[w], dst_ref=target.at[me],
                send_sem=send_sems.at[phase], recv_sem=recv_sems.at[recv],
                device_id=(level, w), device_id_type=MESH,
            ).start()

        @pl.when(w == me)
        def _():
            target[w] = source[w]

    def push_steps(source, target, phase, recv, steps, by_step=0):
        @pl.loop(*steps)
        def _(step):
            for slab in range(slabs):
                push(source, target, phase, recv + by_step * step, quarter_of(step) * slabs + slab)

    def push_all(source, target, phase, recv, by_step=0):
        push_steps(source, target, phase, recv, (0, quarters), by_step)

    def batch_of(source, target, phase, recv, first, count):
        return pltpu.make_async_remote_copy(
            src_ref=source.at[pl.ds(first, count)], dst_ref=target.at[pl.ds(first, count)],
            send_sem=send_sems.at[phase], recv_sem=recv_sems.at[recv],
            device_id=(level, (me + 1) % wav), device_id_type=MESH,
        )

    def arrive_all(source, target, phase, recv):
        batch_of(source, target, phase, recv, 0, wav - 1).wait_recv()

    def arrive_step(source, target, phase, recv, step):
        if step == quarters - 1:
            first, count = me + 1 - 2 * my_slab, 1
        else:
            first, count = quarter_of(step) * slabs, slabs
        batch_of(source, target, phase, recv + step, first, count).wait_recv()

    lane = lax.broadcasted_iota(jnp.int32, (1, LANES), 1)
    signs = jnp.where(lane < HALF, 1.0, -1.0)
    layout = pieces(rows, group_rows, groups)
    wide = (0, HALF)

    def inside_part(starts, part):
        return (lane >= starts[part]) & (lane < starts[part] + tail)

    def pack(tile, starts):
        shifted = {}
        for group, at, part, start, count in layout:
            piece = jnp.where(inside_part(starts, part), tile(start, count), 0.0)
            shift = (group * tail - starts[part]) % LANES
            shifted.setdefault(group, []).append(pltpu.roll(piece, shift, 1) if shift else piece)
        packed = jnp.zeros((group_rows, LANES), jnp.float32)
        for found in shifted.values():
            whole = jnp.concatenate(found, 0) if len(found) > 1 else found[0]
            if whole.shape[0] < group_rows:
                fill = jnp.zeros((group_rows - whole.shape[0], LANES), jnp.float32)
                whole = jnp.concatenate([whole, fill], 0)
            packed = packed + whole
        return packed

    def unpack(packed, starts):
        found = {0: [], 1: []}
        for group, at, part, start, count in layout:
            piece = packed[at : at + count]
            shift = (starts[part] - group * tail) % LANES
            piece = pltpu.roll(piece, shift, 1) if shift else piece
            found[part].append(jnp.where(inside_part(starts, part), piece, 0.0))
        return jnp.concatenate(found[0], 0) + jnp.concatenate(found[1], 0)

    def quarter_starts(quarter):
        first = quarter % 2 * quarter_lanes
        return (first, first + part_lanes)

    def make_table(piece):
        cos_f, sin_f = seeds[0, piece, :fine_rows], seeds[1, piece, :fine_rows]

        @pl.loop(0, length // fine_rows, unroll=2)
        def _(block):
            at = pl.ds(fine_rows + block, 1)
            cos_c, sin_c = seeds[0, piece, at], seeds[1, piece, at]
            span = pl.ds(pl.multiple_of(block * fine_rows, fine_rows), fine_rows)
            value_high, value_low = halves(cos_c * cos_f - sin_c * sin_f)
            table[0, span] = value_high
            table[1, span] = value_low

    def keep(result, piece):
        for slab in range(slabs):
            w = piece * slabs + slab
            sent_a[w] = result[slab * rows : (slab + 1) * rows, :LANES]
            sent_b[w] = result[slab * rows : (slab + 1) * rows, LANES:]

    first_load.wait()
    make_table(quarters + 1)
    for grid_load, span in zip(grid_loads, spans):
        grid_load.wait()
        high, low = halves(grid[:, span])
        grid_parts[0, :, span] = high
        grid_parts[1, :, span] = low
    keep(product((grid_parts[0], grid_parts[1]), (table[0], table[1])), ahead)
    pl.semaphore_wait(barrier, wav - 1 + level)
    for slab in range(slabs):
        push(sent_a, got_a, 0, 0, ahead * slabs + slab)

    later = (
        (limit_hbm, limit_ref), (order_hbm, order_ref), (strength_hbm, strength_ref), (mass_hbm, mass_ref),
        (twiddle_hbm, twiddle), (base_hbm, base), (back_seeds_hbm, back_seeds),
    )
    free_sems = [n for n in range(len(later) + 1) if n != 1 + len(spans)]
    other_loads = [load(source, target, sem) for (source, target), sem in zip(later, free_sems)]
    seeds_load.wait()

    @pl.loop(1, quarters + 1)
    def _(step):
        last = step // quarters
        piece = quarter_of(step % quarters) * (1 - last) + quarters * last
        make_table(piece)
        keep(product((grid_parts[0], grid_parts[1]), (table[0], table[1])), piece)

        @pl.when(step < quarters)
        def _():
            for slab in range(slabs):
                push(sent_a, got_a, 0, 0, piece * slabs + slab)

        @pl.when(step == quarters - 1)
        def _():
            push_all(sent_b, got_b, 1, 1)

    for quarter in range(quarters):
        from_ref = sent_b if quarter // 2 else sent_a
        for slab in range(slabs):
            sent_c[quarter * slabs + slab] = pack(
                lambda start, many: from_ref[wav + slab, start : start + many], quarter_starts(quarter)
            )
    push_all(sent_c, got_c, 2, 2)

    for other in range(lev - 1):
        @pl.when(other < level)
        def _():
            pl.semaphore_signal(ready, inc=1, device_id=(other, me), device_id_type=MESH)

    for other_load in other_loads:
        other_load.wait()
    place = lax.broadcasted_iota(jnp.int32, (1, 3 * LANES), 1)
    column = place // LANES * HALF + place % HALF
    wave = my_quarter * columns + column
    valid = (column < columns) | ((column == columns) & (wave == half))
    single = (wave == 0) | (wave == half)
    out_weight = jnp.where(single, 1.0, 2.0) / float(length) ** 2
    energy_weight = jnp.where(single, 1.0, 0.5)
    all_limits = limit_ref[...].reshape(1, length)
    limits = jnp.full((1, 3 * LANES), -1, jnp.int32)
    for quarter in range(quarters):
        found = []
        for tile in range(3):
            start = quarter * columns + tile * HALF
            found += [all_limits[:, start : start + HALF]] * 2
        limits = jnp.where(my_quarter == quarter, jnp.concatenate(found, 1), limits)
    limits = jnp.where(valid, limits, -1)
    order = order_ref[my_slab]
    strength = strength_ref[my_slab]
    wave_square = wave.astype(jnp.float32) ** 2

    @pl.loop(0, wav)
    def _(m):
        row = lax.broadcasted_iota(jnp.int32, (padded, 1), 0)
        q = row * wav + m
        signed_q = jnp.where(q < half, q, q - length)
        radius = (wave_square + signed_q.astype(jnp.float32) ** 2) / (0.5 * length) ** 2
        square = radius * radius
        powered = jnp.where(order >= 3, square, 1.0) * jnp.where(order % 2 == 1, radius, square)
        inside = (jnp.abs(signed_q) <= limits) & (row < rows)
        damp[m] = jnp.where(inside, out_weight / (1.0 + strength * powered), 0.0)
        work[m, rows:] = jnp.zeros((padded - rows, LANES), jnp.float32)

    blocks = LANES // fine_rows
    plain = 2 * quarters * blocks

    arrivals = [quarters - 1] + list(range(quarters - 1))

    def back_piece(at, target, span):
        row = pl.ds(fine_rows + at, 1)
        cos_c, sin_c = back_seeds[0, row], back_seeds[1, row]
        value_high, value_low = halves(cos_c * back_seeds[0, :fine_rows] - sin_c * back_seeds[1, :fine_rows])
        target[0, span] = value_high
        target[1, span] = value_low

    @pl.loop(0, 2 * quarters)
    def _(n):
        @pl.loop(0, blocks)
        def _(block):
            span = pl.ds(pl.multiple_of(block * fine_rows, fine_rows), fine_rows)
            back_piece(n * blocks + block, back_table.at[n], span)

    for place_of, step in enumerate(arrivals):
        for part in range(2):
            block = 2 * place_of + part
            back_piece(
                plain + 2 * quarter_of(step) + part, tail_table, slice(block * fine_rows, (block + 1) * fine_rows)
            )

    sum_ref[...] = jnp.zeros_like(sum_ref)
    energy_sums[...] = jnp.zeros_like(energy_sums)

    def along(value):
        value_high, value_low = halves(value)
        stacked = jnp.concatenate([value_high, value_high, value_low], 0)
        return jnp.dot(base[...], stacked, preferred_element_type=jnp.float32)

    block_rows = 24
    batch = 2

    def in_blocks(body):
        for start in range(0, rows, block_rows):
            body(start, min(block_rows, rows - start))

    def middle(tile, source, target):
        span_of = slice(tile * LANES, (tile + 1) * LANES)
        all_signs = jnp.concatenate([signs] * batch, 1)

        def split(start, many):
            span = pl.ds(start, many)
            for m, value in enumerate(eight_points([source[w, span] for w in range(wav)], -1, signs)):
                work[m, span] = value

        in_blocks(split)

        def residues(first, sums):
            found = range(first, first + batch)
            beside = lambda pick: jnp.concatenate([pick(m) for m in found], 1)
            packed_turn = beside(lambda m: twiddle[m])
            other_turn = swap(packed_turn)
            low = jnp.concatenate([lane] * batch, 1) < HALF
            cos_t = jnp.where(low, packed_turn, other_turn)
            sin_t = jnp.where(low, other_turn, -packed_turn)
            value = beside(lambda m: work[m])
            both = along(value * cos_t + swap(value) * sin_t)
            value = both[:padded] + swap(both[padded:]) * all_signs
            value = value * beside(lambda m: damp[m, :, span_of])
            sums = sums + jnp.sum((value * value).reshape(padded // 8, 8, batch * LANES), axis=0)
            both = along(value)
            value = both[:padded] - swap(both[padded:]) * all_signs
            value = value * cos_t - swap(value) * sin_t
            for n, m in enumerate(found):
                work[m] = value[:, n * LANES : (n + 1) * LANES]
            return sums

        sums = jnp.zeros((8, batch * LANES), jnp.float32)
        for first in range(0, wav, batch):
            sums = residues(first, sums)
        sums = sum(sums[:, n * LANES : (n + 1) * LANES] for n in range(batch))
        energy_sums[...] += sums * energy_weight[:, span_of]

        if tile == 2:
            announce()

        def join(start, many):
            span = pl.ds(start, many)
            for w, value in enumerate(eight_points([work[m, span] for m in range(wav)], 1, signs)):
                target[w, span] = value

        in_blocks(join)

    def wav_copy(target, slot, count=1):
        return pltpu.make_async_remote_copy(
            src_ref=energy_wav.at[pl.ds(slot, count)], dst_ref=energy_wav.at[pl.ds(slot, count)],
            send_sem=energy_sems.at[0], recv_sem=energy_sems.at[1],
            device_id=(level, target), device_id_type=MESH,
        )

    def lev_copy(target, slot, count=1):
        return pltpu.make_async_remote_copy(
            src_ref=energy_lev.at[pl.ds(slot, count)], dst_ref=energy_lev.at[pl.ds(slot, count)],
            send_sem=energy_sems.at[2], recv_sem=energy_sems.at[3],
            device_id=(target, me), device_id_type=MESH,
        )

    def announce():
        energy_wav[me] = jnp.sum(energy_sums[...], axis=0, keepdims=True)

        @pl.loop(1, wav)
        def _(step):
            wav_copy((me + step) % wav, me).start()

        push_steps(back_b, home_b, 4, 4, (1, quarters - 1), 1)

    arrive_all(sent_a, got_a, 0, 0)
    middle(0, got_a, back_a)
    push_all(back_a, home_a, 3, 3)
    arrive_all(sent_b, got_b, 1, 1)
    middle(1, got_b, back_b)
    push_steps(back_b, home_b, 4, 4, (0, 1), 1)
    push_steps(back_b, home_b, 4, 4, (quarters - 1, quarters), 1)
    arrive_all(sent_c, got_c, 2, 2)

    @pl.loop(0, wav)
    def _(w):
        rest[w] = unpack(got_c[w], wide)

    middle(2, rest, rest)

    @pl.loop(0, quarters)
    def _(step):
        for slab in range(slabs):
            w = quarter_of(step) * slabs + slab
            back_c[w] = pack(lambda start, many: rest[w, start : start + many], wide)
            push(back_c, home_c, 5, 4 + quarters + step, w)

    def add_pair(tile, home, steps):
        found, right = [], ([], [])
        for step in steps:
            quarter = quarter_of(step)
            found.append(jnp.concatenate([home[quarter * slabs + slab] for slab in range(slabs)], 0))
            for part in range(2):
                right[part].append(back_table[tile * quarters + quarter, part])
        left = halves(jnp.concatenate(found, 1))
        sum_ref[...] += product(left, [jnp.concatenate(part, 0) for part in right])

    arrive_all(back_a, home_a, 3, 3)

    @pl.loop(0, quarters, step=2)
    def _(step):
        add_pair(0, home_a, (step, step + 1))

    wav_copy((me + 1) % wav, 0, wav - 1).wait()

    slab_sums = []
    for slab in range(slabs):
        total = energy_wav[slab]
        for quarter in range(1, quarters):
            total = total + energy_wav[quarter * slabs + slab]
        slab_sums.append(total)
    weighted = slab_sums[0] * mass_ref[0]
    for slab in range(1, slabs):
        weighted = weighted + slab_sums[slab] * mass_ref[slab]
    energy_lev[level] = weighted

    @pl.when(level < lev - 1)
    def _():
        pl.semaphore_wait(ready, lev - 1 - level)

    for other in range(lev):
        @pl.when(level != other)
        def _():
            lev_copy(other, level).start()

    for pair in range(0, quarters, 2):
        for step in arrivals[pair : pair + 2]:
            arrive_step(back_b, home_b, 4, 4, step)
        add_pair(1, home_b, arrivals[pair : pair + 2])

    for side in range(2):
        values = [jnp.zeros((rows, LANES), jnp.float32)] * slabs
        for place_of in range(2 * side, 2 * side + 2):
            arrive_step(back_c, home_c, 5, 4 + quarters, arrivals[place_of])
            for slab in range(slabs):
                w = quarter_of(arrivals[place_of]) * slabs + slab
                values[slab] = values[slab] + unpack(home_c[w], quarter_starts(place_of))
        for slab in range(slabs):
            value_high, value_low = halves(values[slab])
            at = (slice(slab * rows, (slab + 1) * rows), slice(side * LANES, (side + 1) * LANES))
            tail_ref[(0,) + at] = value_high
            tail_ref[(1,) + at] = value_low

    for phase, (source, target) in enumerate(
        ((sent_a, got_a), (sent_b, got_b), (sent_c, got_c), (back_a, home_a), (back_b, home_b), (back_c, home_c))
    ):
        batch_of(source, target, phase, 0, 0, wav - 1).wait_send()
    lev_copy((level + 1) % lev, 0, lev - 1).wait()

    total = energy_lev[0]
    for other in range(1, lev):
        total = total + energy_lev[other]
    fill = jnp.zeros((8 - slabs - 1, LANES), jnp.float32)
    energy_ref[...] = jnp.concatenate(slab_sums + [total / (lev * slabs), fill], 0)


def last_kernel(
    slabs, spans, sum_ref, tail_ref, tail_table, energy_ref, out_hbm, energies_hbm, total_hbm,
    out, energies, total, sems,
):
    sums = jnp.sum(energy_ref[...], axis=1, keepdims=True)
    for slab in range(slabs):
        energies[slab] = sums[slab, 0]
    total[0] = sums[slabs, 0]
    copies = [
        pltpu.make_async_copy(energies, energies_hbm, sems.at[0]),
        pltpu.make_async_copy(total, total_hbm, sems.at[1]),
    ]
    for copy in copies:
        copy.start()
    left = (tail_ref[0], tail_ref[1])
    for n, (start, stop) in enumerate(spans):
        out[:, start:stop] = sum_ref[:, start:stop] + product(
            left, (tail_table[0, :, start:stop], tail_table[1, :, start:stop])
        )
        copies.append(
            pltpu.make_async_copy(out.at[:, start:stop], out_hbm.at[:, start:stop], sems.at[2 + n])
        )
        copies[-1].start()
    for copy in copies:
        copy.wait()


def cos_sin(phases, length):
    angles = 2.0 * np.pi / length * (phases % length)
    return np.stack([np.cos(angles), np.sin(angles)])


def fused(grid_field, truncation_limit, diffusion_order, diffusion_strength, mass_weight):
    slabs, rows, length = grid_field.shape
    wav, lev = lax.axis_size("wav"), lax.axis_size("lev")
    quarters = wav // slabs
    columns = length // 2 // quarters
    tail = columns + 1 - LANES
    groups = LANES // tail
    group_rows = -(-(-(-2 * rows // groups)) // 8) * 8
    padded = -(-rows // 16) * 16
    fine_rows = 32
    sizes = (slabs, rows, length, wav, lev, quarters, columns, padded, tail, groups, group_rows, fine_rows)
    turn = length // 4
    place = np.arange(2 * LANES)
    starts = np.arange(quarters) * columns
    plain_waves = starts[:, None] + (place // LANES * HALF + place % HALF)[None]
    plain_phase = np.broadcast_to((place % LANES >= HALF) * turn, plain_waves.shape)
    part = LANES // 4
    tail_waves = (starts[place // HALF] + LANES + place % part)[None]
    tail_phase = (place % HALF >= part)[None] * turn
    waves = np.concatenate([plain_waves, tail_waves])
    phase = np.concatenate([plain_phase, tail_phase])
    steps = np.arange(length // fine_rows) * fine_rows
    near = np.arange(fine_rows)
    positions = np.arange(length)
    single = lambda array: jnp.asarray(array, jnp.float32)
    seeds = single(
        np.concatenate(
            [
                cos_sin(near[None, :, None] * waves[:, None, :] + phase[:, None, :], length),
                cos_sin(steps[None, :, None] * waves[:, None, :], length),
            ],
            2,
        )
    )
    by_tile = lambda array: np.concatenate(
        [array[:quarters, :LANES].ravel(), array[:quarters, LANES:].ravel(), array[quarters]]
    )[::fine_rows]
    back_seeds = single(
        np.concatenate(
            [
                cos_sin(near[:, None] * positions[None], length),
                cos_sin(by_tile(waves)[:, None] * positions[None] + by_tile(phase)[:, None], length),
            ],
            1,
        )
    )
    inner = np.arange(padded)
    turns = cos_sin(np.arange(wav)[:, None, None] * inner[None, :, None], length)
    twiddle = single(np.repeat(turns, HALF, 3).transpose(1, 2, 0, 3).reshape(wav, padded, LANES))
    base_exact = cos_sin(wav * inner[:, None] * inner[None], length)
    base_exact = base_exact * ((inner[:, None] < rows) & (inner[None] < rows))
    base_exact = base_exact.reshape(2 * padded, padded).astype(np.float32)
    base_high = base_exact.astype(jnp.bfloat16)
    base_low = (base_exact - base_high.astype(np.float32)).astype(jnp.bfloat16)
    base = jnp.asarray(np.concatenate([base_high, base_low, base_high], 1))
    vmem, hbm = pl.BlockSpec(memory_space=pltpu.VMEM), pl.BlockSpec(memory_space=pltpu.HBM)
    f32, bf16, i32 = jnp.float32, jnp.bfloat16, jnp.int32
    sent = pltpu.VMEM((wav + slabs, rows, LANES), f32)
    whole = pltpu.VMEM((wav, rows, LANES), f32)
    small = pltpu.VMEM((wav, group_rows, LANES), f32)
    dma = pltpu.SemaphoreType.DMA
    partial_sum, tails, tail_table, energy_rows = pl.pallas_call(
        functools.partial(fused_kernel, sizes),
        out_shape=(
            jax.ShapeDtypeStruct((slabs * rows, length), f32),
            jax.ShapeDtypeStruct((2, slabs * rows, 2 * LANES), bf16),
            jax.ShapeDtypeStruct((2, 2 * LANES, length), bf16),
            jax.ShapeDtypeStruct((8, LANES), f32),
        ),
        in_specs=[hbm] * 9,
        out_specs=(vmem,) * 4,
        scratch_shapes=[
            pltpu.VMEM((slabs * rows, length), f32),
            pltpu.VMEM((length,), i32),
            pltpu.SMEM((slabs,), i32),
            pltpu.SMEM((slabs,), f32),
            pltpu.SMEM((slabs,), f32),
            pltpu.VMEM((2, quarters + 2) + seeds.shape[2:], f32),
            pltpu.VMEM(back_seeds.shape, f32),
            pltpu.VMEM(twiddle.shape, f32),
            pltpu.VMEM(base.shape, bf16),
            pltpu.VMEM((2, slabs * rows, length), bf16),
            pltpu.VMEM((2, length, 2 * LANES), bf16),
            pltpu.VMEM((2 * quarters, 2, LANES, length), bf16),
            sent, sent, small, whole, whole, small, whole, whole, small, whole, whole, small,
            whole,
            pltpu.VMEM((wav, padded, LANES), f32),
            pltpu.VMEM((wav, padded, 3 * LANES), f32),
            pltpu.VMEM((8, LANES), f32),
            pltpu.VMEM((wav, 1, LANES), f32),
            pltpu.VMEM((lev, 1, LANES), f32),
            dma((8,)), dma((6,)), dma((4 + 2 * quarters,)), dma((4,)),
            pltpu.SemaphoreType.REGULAR,
        ],
        compiler_params=pltpu.CompilerParams(
            collective_id=0, has_side_effects=True, vmem_limit_bytes=40 * 1024 * 1024
        ),
        name="fused_step",
    )(
        *(
            pltpu.with_memory_space_constraint(array, pltpu.HBM)
            for array in (
                grid_field.reshape(slabs * rows, length), truncation_limit, diffusion_order,
                diffusion_strength, mass_weight, seeds, back_seeds, twiddle, base,
            )
        )
    )
    spans = [(at, min(at + 2 * LANES, length)) for at in range(0, length, 2 * LANES)]
    filtered, energies, total = pl.pallas_call(
        functools.partial(last_kernel, slabs, spans),
        out_shape=(
            jax.ShapeDtypeStruct((slabs * rows, length), f32),
            jax.ShapeDtypeStruct((slabs,), f32),
            jax.ShapeDtypeStruct((1,), f32),
        ),
        in_specs=[vmem] * 4,
        out_specs=(hbm,) * 3,
        scratch_shapes=[
            pltpu.VMEM((slabs * rows, length), f32),
            pltpu.SMEM((slabs,), f32),
            pltpu.SMEM((1,), f32),
            dma((2 + len(spans),)),
        ],
        compiler_params=pltpu.CompilerParams(vmem_limit_bytes=12 * 1024 * 1024),
        name="last_product",
    )(partial_sum, tails, tail_table, energy_rows)
    return filtered.reshape(slabs, rows, length), energies, total[0]


def fits(shape):
    slabs, rows, length = shape
    wav = lax.axis_size("wav")
    if wav != 8 or slabs != 2 or rows % 8 or length % 16 or length != rows * wav:
        return False
    columns = length * slabs // 2 // wav
    return length % 32 == 0 and LANES <= columns < LANES + LANES // 4


def local(grid_field, truncation_limit, diffusion_order, diffusion_strength, mass_weight):
    slab_count, row_count, length = grid_field.shape
    if fits(grid_field.shape):
        return fused(
            grid_field, truncation_limit, diffusion_order, diffusion_strength, mass_weight
        )
    cosine_table, sine_table = tables(length)
    filtered, partial_value = half_plane(
        grid_field, truncation_limit, diffusion_order, diffusion_strength, cosine_table, sine_table
    )
    total_slabs = lax.axis_size("lev") * slab_count
    energies = lax.psum(partial_value, "wav")
    weighted_sum = lax.psum(jnp.sum(mass_weight * energies), "lev")
    total_energy = weighted_sum / total_slabs
    return (filtered, energies, total_energy)


def solution(mesh):
    placed = (P("lev", "wav", None), P(), P("lev"), P("lev"), P("lev"))
    return jax.shard_map(
        local,
        mesh=mesh,
        in_specs=placed,
        out_specs=(P("lev", "wav", None), P("lev"), P()),
        check_vma=False,
    )
```

```python
import functools

import jax
import jax.numpy as jnp
import numpy as np
from jax import lax
from jax.experimental import pallas as pl
from jax.experimental.pallas import tpu as pltpu
from jax.sharding import PartitionSpec as P

product_precision = lax.Precision.HIGH


def tables(length):
    step = 32
    coarse = -(-length // step)
    columns = np.arange(length)
    high = 2.0 * np.pi / length * (np.arange(coarse)[:, None] * step * columns[None, :] % length)
    low = 2.0 * np.pi / length * (np.arange(step)[:, None] * columns[None, :] % length)
    cos_high, sin_high = (jnp.asarray(f(high), jnp.float32)[:, None] for f in (np.cos, np.sin))
    cos_low, sin_low = (jnp.asarray(f(low), jnp.float32)[None] for f in (np.cos, np.sin))
    cosine = cos_high * cos_low - sin_high * sin_low
    sine = sin_high * cos_low + cos_high * sin_low
    return tuple(t.reshape(coarse * step, length)[:length] for t in (cosine, sine))


def signed(positions, length):
    return jnp.where(positions < length // 2, positions, positions - length)


def transform(values, cosine_table, sine_table, direction):
    with_cosine = jnp.einsum("scpi,iq->scpq", values, cosine_table, precision=product_precision)
    with_sine = jnp.einsum("scpi,iq->scpq", values, sine_table, precision=product_precision)
    if direction < 0:
        real_part = with_cosine[:, 0] + with_sine[:, 1]
        imaginary = with_cosine[:, 1] - with_sine[:, 0]
    else:
        real_part = with_cosine[:, 0] - with_sine[:, 1]
        imaginary = with_cosine[:, 1] + with_sine[:, 0]
    return jnp.stack([real_part, imaginary], axis=1)


def damping(wave_rows, limits, length, diffusion_order, diffusion_strength):
    wave_first = signed(jnp.arange(length, dtype=jnp.int32), length)
    rows_float = wave_rows.astype(jnp.float32)
    first_float = wave_first.astype(jnp.float32)
    scaled_radius = (rows_float[:, None] ** 2 + first_float[None, :] ** 2) / (0.5 * length) ** 2
    inside = (jnp.abs(wave_first)[None, :] <= limits[:, None]).astype(jnp.float32)
    powered = jnp.power(scaled_radius[None], diffusion_order.astype(jnp.float32)[:, None, None])
    return inside[None] / (1.0 + diffusion_strength[:, None, None] * powered)


def mirrored(values):
    return jnp.roll(jnp.flip(values, -1), 1, -1)


def half_plane(
    grid_field, truncation_limit, diffusion_order, diffusion_strength, cosine_table, sine_table
):
    length = grid_field.shape[2]
    half = length // 2
    row_real = jnp.einsum("sij,jl->sli", grid_field, cosine_table[:, :half], precision=product_precision)
    row_imag = -jnp.einsum("sij,jl->sli", grid_field, sine_table[:, :half], precision=product_precision)
    nyquist = jnp.einsum("sij,j->si", grid_field, cosine_table[:, half], precision=product_precision)
    zero_row = (jnp.arange(half, dtype=jnp.int32) == 0)[None, :, None]
    row_imag = jnp.where(zero_row, nyquist[:, None, :], row_imag)
    along_rows = jnp.stack([row_real, row_imag], axis=1)
    spectrum = transform(
        lax.all_to_all(along_rows, "wav", split_axis=2, concat_axis=3, tiled=True),
        cosine_table,
        sine_table,
        -1,
    )
    column_count = spectrum.shape[2]
    wav_index = lax.axis_index("wav")
    offset = wav_index * column_count
    wave_rows = offset + jnp.arange(column_count, dtype=jnp.int32)
    limits = lax.dynamic_slice(truncation_limit, (offset,), (column_count,))
    damp_main = damping(wave_rows, limits, length, diffusion_order, diffusion_strength)
    nyquist_rows = signed(jnp.full((1,), half, jnp.int32), length)
    damp_top = damping(
        nyquist_rows, truncation_limit[half : half + 1], length, diffusion_order, diffusion_strength
    )[:, 0]
    damped = spectrum * damp_main[:, None]
    packed_real = spectrum[:, 0, 0, :]
    packed_imag = spectrum[:, 1, 0, :]
    back_real = mirrored(packed_real)
    back_imag = mirrored(packed_imag)
    zero_real = (packed_real + back_real) * 0.5 * damp_main[:, 0]
    zero_imag = (packed_imag - back_imag) * 0.5 * damp_main[:, 0]
    top_real = (packed_imag + back_imag) * 0.5 * damp_top
    top_imag = (back_real - packed_real) * 0.5 * damp_top
    is_zero = wave_rows == 0
    column_weight = jnp.where(is_zero, 0.0, 2.0).astype(jnp.float32)
    edge = jnp.sum(zero_real**2 + zero_imag**2 + top_real**2 + top_imag**2, axis=-1)
    main_sum = jnp.sum(damped * damped * column_weight[None, None, :, None], axis=(1, 2, 3))
    partial_value = (main_sum + jnp.where(wav_index == 0, edge, 0.0)) / float(length) ** 4
    zero_column = is_zero[None, :, None]
    repacked = jnp.stack(
        [
            jnp.where(zero_column, (zero_real - top_imag)[:, None, :], damped[:, 0]),
            jnp.where(zero_column, (zero_imag + top_real)[:, None, :], damped[:, 1]),
        ],
        axis=1,
    )
    along_first = transform(repacked, cosine_table, sine_table, 1)
    inverse_area = 1.0 / float(length) ** 2
    received = lax.all_to_all(along_first, "wav", split_axis=3, concat_axis=2, tiled=True)
    row_weight = jnp.where(jnp.arange(half, dtype=jnp.int32) == 0, 1.0, 2.0).astype(jnp.float32)[
        :, None
    ]
    with_cosine = jnp.einsum(
        "spi,pj->sij", received[:, 0] * row_weight, cosine_table[:half], precision=product_precision
    )
    with_sine = jnp.einsum(
        "spi,pj->sij", received[:, 1] * row_weight, sine_table[:half], precision=product_precision
    )
    top_term = received[:, 1, 0, :][:, :, None] * cosine_table[half][None, None, :]
    filtered = (with_cosine - with_sine + top_term) * inverse_area
    return (filtered, partial_value)


LANES = 128
HALF = LANES // 2
MESH = pl.DeviceIdType.MESH


def halves(values):
    high = values.astype(jnp.bfloat16)
    return high, (values - high.astype(jnp.float32)).astype(jnp.bfloat16)


def product(left, right):
    dot = functools.partial(jnp.dot, preferred_element_type=jnp.float32)
    return dot(left[0], right[0]) + dot(left[1], right[0]) + dot(left[0], right[1])


def swap(value):
    count = value.shape[1] // LANES
    turned = [pltpu.roll(value[:, n * LANES : (n + 1) * LANES], HALF, 1) for n in range(count)]
    return jnp.concatenate(turned, 1) if count > 1 else turned[0]


def eight_points(x, sign, signs):
    turn = signs if sign < 0 else -signs

    def four(p, q, r, t):
        a0, a1, a2, a3 = p + r, p - r, q + t, swap(q - t) * turn
        return a0 + a2, a1 + a3, a0 - a2, a1 - a3

    e = four(x[0], x[2], x[4], x[6])
    o = four(x[1], x[3], x[5], x[7])
    root = 0.5**0.5
    odd = (
        o[0],
        root * (o[1] + swap(o[1]) * turn),
        swap(o[2]) * turn,
        root * (swap(o[3]) * turn - o[3]),
    )
    return [e[n] + odd[n] for n in range(4)] + [e[n] - odd[n] for n in range(4)]


def pieces(rows, group_rows, groups):
    found = []
    for group in range(groups):
        start, stop = group * group_rows, min((group + 1) * group_rows, 2 * rows)
        while start < stop:
            part = start // rows
            end = min(stop, (part + 1) * rows)
            found.append((group, start - group * group_rows, part, start - part * rows, end - start))
            start = end
    return found


def fused_kernel(
    sizes,
    grid_hbm, limit_hbm, order_hbm, strength_hbm, mass_hbm, seeds_hbm, back_seeds_hbm, twiddle_hbm, base_hbm,
    sum_ref, tail_ref, tail_table, energy_ref,
    grid, limit_ref, order_ref, strength_ref, mass_ref, seeds, back_seeds, twiddle, base,
    grid_parts, table, back_table,
    sent_a, sent_b, sent_c, got_a, got_b, got_c, back_a, back_b, back_c, home_a, home_b, home_c,
    rest, work, damp, energy_sums, energy_wav, energy_lev,
    load_sems, send_sems, recv_sems, energy_sems, ready,
):
    slabs, rows, length, wav, lev, quarters, columns, padded, tail, groups, group_rows, fine_rows = sizes
    half = length // 2
    quarter_lanes = LANES // 2
    part_lanes = quarter_lanes // 2
    me = lax.axis_index("wav")
    level = lax.axis_index("lev")
    my_quarter, my_slab = me // slabs, me % slabs

    barrier = pltpu.get_barrier_semaphore()

    def quarter_of(step):
        down, across = 1 - step % 2, 1 - step // 2
        y, x = my_quarter // 2, my_quarter % 2
        return (y + down - 2 * y * down) * 2 + (x + across - 2 * x * across)

    early = -(-rows // 16) * 16
    spans = [slice(0, early), slice(early, slabs * rows)]
    ahead = quarter_of(0)
    def load(source, target, sem):
        copy = pltpu.make_async_copy(source, target, load_sems.at[sem])
        copy.start()
        return copy

    first_load = load(seeds_hbm.at[:, ahead], seeds.at[:, quarters + 1], 0)
    grid_loads = [load(grid_hbm.at[span], grid.at[span], 1 + n) for n, span in enumerate(spans)]
    seeds_load = load(seeds_hbm, seeds.at[:, : quarters + 1], 1 + len(spans))

    @pl.loop(1, wav)
    def _(step):
        pl.semaphore_signal(barrier, inc=1, device_id=(level, (me + step) % wav), device_id_type=MESH)

    for other in range(1, lev):
        @pl.when(level < other)
        def _():
            pl.semaphore_signal(barrier, inc=1, device_id=(other, me), device_id_type=MESH)

    def push(source, target, phase, recv, w):
        @pl.when(w != me)
        def _():
            pltpu.make_async_remote_copy(
                src_ref=source.at[w], dst_ref=target.at[me],
                send_sem=send_sems.at[phase], recv_sem=recv_sems.at[recv],
                device_id=(level, w), device_id_type=MESH,
            ).start()

        @pl.when(w == me)
        def _():
            target[w] = source[w]

    def push_quarter(source, target, phase, recv, quarter):
        for n in range(slabs):
            push(source, target, phase, recv, quarter * slabs + n)

    def push_all(source, target, phase, recv, by_step=0):
        @pl.loop(0, quarters)
        def _(step):
            push_quarter(source, target, phase, recv + by_step * step, quarter_of(step))

    def batch_of(source, target, phase, recv, first, count):
        return pltpu.make_async_remote_copy(
            src_ref=source.at[pl.ds(first, count)], dst_ref=target.at[pl.ds(first, count)],
            send_sem=send_sems.at[phase], recv_sem=recv_sems.at[recv],
            device_id=(level, (me + 1) % wav), device_id_type=MESH,
        )

    def arrive_all(source, target, phase, recv):
        batch_of(source, target, phase, recv, 0, wav - 1).wait_recv()

    def arrive_step(source, target, phase, recv, step):
        if step == quarters - 1:
            first, count = me + 1 - 2 * my_slab, 1
        else:
            first, count = quarter_of(step) * slabs, slabs
        batch_of(source, target, phase, recv + step, first, count).wait_recv()

    lane = lax.broadcasted_iota(jnp.int32, (1, LANES), 1)
    signs = jnp.where(lane < HALF, 1.0, -1.0)
    layout = pieces(rows, group_rows, groups)
    wide = (0, HALF)

    def inside_part(starts, part):
        return (lane >= starts[part]) & (lane < starts[part] + tail)

    def pack(tile, starts):
        shifted = {}
        for group, at, part, start, count in layout:
            piece = jnp.where(inside_part(starts, part), tile(start, count), 0.0)
            shift = (group * tail - starts[part]) % LANES
            shifted.setdefault(group, []).append(pltpu.roll(piece, shift, 1) if shift else piece)
        packed = jnp.zeros((group_rows, LANES), jnp.float32)
        for found in shifted.values():
            whole = jnp.concatenate(found, 0) if len(found) > 1 else found[0]
            if whole.shape[0] < group_rows:
                fill = jnp.zeros((group_rows - whole.shape[0], LANES), jnp.float32)
                whole = jnp.concatenate([whole, fill], 0)
            packed = packed + whole
        return packed

    def unpack(packed, starts):
        found = {0: [], 1: []}
        for group, at, part, start, count in layout:
            piece = packed[at : at + count]
            shift = (starts[part] - group * tail) % LANES
            piece = pltpu.roll(piece, shift, 1) if shift else piece
            found[part].append(jnp.where(inside_part(starts, part), piece, 0.0))
        return jnp.concatenate(found[0], 0) + jnp.concatenate(found[1], 0)

    def quarter_starts(quarter):
        first = quarter % 2 * quarter_lanes
        return (first, first + part_lanes)

    def make_table(piece, lanes):
        cos_f, sin_f = seeds[0, piece, :fine_rows, lanes], seeds[1, piece, :fine_rows, lanes]

        @pl.loop(0, length // fine_rows, unroll=2)
        def _(block):
            at = pl.ds(fine_rows + block, 1)
            cos_c, sin_c = seeds[0, piece, at][:, lanes], seeds[1, piece, at][:, lanes]
            span = pl.ds(pl.multiple_of(block * fine_rows, fine_rows), fine_rows)
            value_high, value_low = halves(cos_c * cos_f - sin_c * sin_f)
            table[0, span, lanes] = value_high
            table[1, span, lanes] = value_low

    def keep(result, piece):
        for slab in range(slabs):
            w = piece * slabs + slab
            sent_a[w] = result[slab * rows : (slab + 1) * rows, :LANES]
            sent_b[w] = result[slab * rows : (slab + 1) * rows, LANES:]

    front, behind = slice(0, LANES), slice(LANES, 2 * LANES)
    first_load.wait()
    make_table(quarters + 1, front)

    def first_rows(span):
        high, low = halves(grid[span])
        grid_parts[0, span] = high
        grid_parts[1, span] = low
        return product((grid_parts[0, span], grid_parts[1, span]), (table[0, :, front], table[1, :, front]))

    grid_loads[0].wait()
    result = first_rows(spans[0])
    sent_a[ahead * slabs] = result[:rows]
    if early > rows:
        sent_a[ahead * slabs + 1, : early - rows] = result[rows:]
    pl.semaphore_wait(barrier, wav - 1 + level)
    push(sent_a, got_a, 0, 0, ahead * slabs)
    grid_loads[1].wait()
    sent_a[ahead * slabs + 1, early - rows :] = first_rows(spans[1])
    push(sent_a, got_a, 0, 0, ahead * slabs + 1)
    make_table(quarters + 1, behind)
    result = product((grid_parts[0], grid_parts[1]), (table[0, :, behind], table[1, :, behind]))
    for slab in range(slabs):
        sent_b[ahead * slabs + slab] = result[slab * rows : (slab + 1) * rows]

    later = (
        (limit_hbm, limit_ref), (order_hbm, order_ref), (strength_hbm, strength_ref), (mass_hbm, mass_ref),
        (twiddle_hbm, twiddle), (base_hbm, base), (back_seeds_hbm, back_seeds),
    )
    free_sems = [n for n in range(len(later) + 1) if n != 1 + len(spans)]
    other_loads = [load(source, target, sem) for (source, target), sem in zip(later, free_sems)]
    seeds_load.wait()

    @pl.loop(0, quarters)
    def _(step):
        plain_step = (step + quarters - 1) // quarters
        piece = quarter_of(step) * plain_step + quarters * (1 - plain_step)
        make_table(piece, slice(0, 2 * LANES))
        keep(product((grid_parts[0], grid_parts[1]), (table[0], table[1])), piece)

        @pl.when(step == 0)
        def _():
            for quarter in range(quarters):
                from_ref = sent_b if quarter // 2 else sent_a
                for slab in range(slabs):
                    sent_c[quarter * slabs + slab] = pack(
                        lambda start, many: from_ref[wav + slab, start : start + many], quarter_starts(quarter)
                    )
            push_all(sent_c, got_c, 2, 2)

        @pl.when(step > 0)
        def _():
            push_quarter(sent_a, got_a, 0, 0, piece)

        @pl.when(step == quarters - 1)
        def _():
            push_all(sent_b, got_b, 1, 1)

    for other in range(lev - 1):
        @pl.when(other < level)
        def _():
            pl.semaphore_signal(ready, inc=1, device_id=(other, me), device_id_type=MESH)

    for other_load in other_loads:
        other_load.wait()
    place = lax.broadcasted_iota(jnp.int32, (1, 3 * LANES), 1)
    column = place // LANES * HALF + place % HALF
    wave = my_quarter * columns + column
    valid = (column < columns) | ((column == columns) & (wave == half))
    single = (wave == 0) | (wave == half)
    out_weight = jnp.where(single, 1.0, 2.0) / float(length) ** 2
    energy_weight = jnp.where(single, 1.0, 0.5)
    all_limits = limit_ref[...].reshape(1, length)
    limits = jnp.full((1, 3 * LANES), -1, jnp.int32)
    for quarter in range(quarters):
        found = []
        for tile in range(3):
            start = quarter * columns + tile * HALF
            found += [all_limits[:, start : start + HALF]] * 2
        limits = jnp.where(my_quarter == quarter, jnp.concatenate(found, 1), limits)
    limits = jnp.where(valid, limits, -1)
    order = order_ref[my_slab]
    strength = strength_ref[my_slab]
    wave_square = wave.astype(jnp.float32) ** 2

    @pl.loop(0, wav)
    def _(m):
        row = lax.broadcasted_iota(jnp.int32, (padded, 1), 0)
        q = row * wav + m
        signed_q = jnp.where(q < half, q, q - length)
        radius = (wave_square + signed_q.astype(jnp.float32) ** 2) / (0.5 * length) ** 2
        square = radius * radius
        powered = jnp.where(order >= 3, square, 1.0) * jnp.where(order % 2 == 1, radius, square)
        inside = (jnp.abs(signed_q) <= limits) & (row < rows)
        damp[m] = jnp.where(inside, out_weight / (1.0 + strength * powered), 0.0)
        work[m, rows:] = jnp.zeros((padded - rows, LANES), jnp.float32)

    blocks = LANES // fine_rows
    plain = 2 * quarters * blocks

    arrivals = [quarters - 1] + list(range(quarters - 1))

    def back_piece(at, target, span):
        row = pl.ds(fine_rows + at, 1)
        cos_c, sin_c = back_seeds[0, row], back_seeds[1, row]
        value_high, value_low = halves(cos_c * back_seeds[0, :fine_rows] - sin_c * back_seeds[1, :fine_rows])
        target[0, span] = value_high
        target[1, span] = value_low

    @pl.loop(0, 2 * quarters)
    def _(n):
        @pl.loop(0, blocks)
        def _(block):
            span = pl.ds(pl.multiple_of(block * fine_rows, fine_rows), fine_rows)
            back_piece(n * blocks + block, back_table.at[n], span)

    for place_of, step in enumerate(arrivals):
        for part in range(2):
            block = 2 * place_of + part
            back_piece(
                plain + 2 * quarter_of(step) + part, tail_table, slice(block * fine_rows, (block + 1) * fine_rows)
            )

    sum_ref[...] = jnp.zeros_like(sum_ref)
    energy_sums[...] = jnp.zeros_like(energy_sums)

    def along(value):
        value_high, value_low = halves(value)
        stacked = jnp.concatenate([value_high, value_high, value_low], 0)
        return jnp.dot(base[...], stacked, preferred_element_type=jnp.float32)

    block_rows = 24
    batch = 2

    def in_blocks(body):
        for start in range(0, rows, block_rows):
            body(start, min(block_rows, rows - start))

    def middle(tile, source, target):
        span_of = slice(tile * LANES, (tile + 1) * LANES)
        all_signs = jnp.concatenate([signs] * batch, 1)

        def split(start, many):
            span = pl.ds(start, many)
            for m, value in enumerate(eight_points([source[w, span] for w in range(wav)], -1, signs)):
                work[m, span] = value

        in_blocks(split)

        def residues(first, sums):
            found = range(first, first + batch)
            beside = lambda pick: jnp.concatenate([pick(m) for m in found], 1)
            packed_turn = beside(lambda m: twiddle[m])
            other_turn = swap(packed_turn)
            low = jnp.concatenate([lane] * batch, 1) < HALF
            cos_t = jnp.where(low, packed_turn, other_turn)
            sin_t = jnp.where(low, other_turn, -packed_turn)
            value = beside(lambda m: work[m])
            both = along(value * cos_t + swap(value) * sin_t)
            value = both[:padded] + swap(both[padded:]) * all_signs
            value = value * beside(lambda m: damp[m, :, span_of])
            sums = sums + jnp.sum((value * value).reshape(padded // 8, 8, batch * LANES), axis=0)
            both = along(value)
            value = both[:padded] - swap(both[padded:]) * all_signs
            value = value * cos_t - swap(value) * sin_t
            for n, m in enumerate(found):
                work[m] = value[:, n * LANES : (n + 1) * LANES]
            return sums

        sums = jnp.zeros((8, batch * LANES), jnp.float32)
        for first in range(0, wav, batch):
            sums = residues(first, sums)
        sums = sum(sums[:, n * LANES : (n + 1) * LANES] for n in range(batch))
        energy_sums[...] += sums * energy_weight[:, span_of]

        if tile == 1:
            announce()

        def join(start, many):
            span = pl.ds(start, many)
            for w, value in enumerate(eight_points([work[m, span] for m in range(wav)], 1, signs)):
                target[w, span] = value

        in_blocks(join)

    def wav_copy(target, slot, count=1):
        return pltpu.make_async_remote_copy(
            src_ref=energy_wav.at[pl.ds(slot, count)], dst_ref=energy_wav.at[pl.ds(slot, count)],
            send_sem=energy_sems.at[0], recv_sem=energy_sems.at[1],
            device_id=(level, target), device_id_type=MESH,
        )

    def lev_copy(target, slot, count=1):
        return pltpu.make_async_remote_copy(
            src_ref=energy_lev.at[pl.ds(slot, count)], dst_ref=energy_lev.at[pl.ds(slot, count)],
            send_sem=energy_sems.at[2], recv_sem=energy_sems.at[3],
            device_id=(target, me), device_id_type=MESH,
        )

    def announce():
        energy_wav[me] = jnp.sum(energy_sums[...], axis=0, keepdims=True)

        @pl.loop(1, wav)
        def _(step):
            wav_copy((me + step) % wav, me).start()

    arrive_all(sent_c, got_c, 2, 2)

    @pl.loop(0, wav)
    def _(w):
        rest[w] = unpack(got_c[w], wide)

    middle(2, rest, rest)

    @pl.loop(0, wav)
    def _(w):
        back_c[w] = pack(lambda start, many: rest[w, start : start + many], wide)

    arrive_all(sent_a, got_a, 0, 0)
    middle(0, got_a, back_a)
    push_all(back_a, home_a, 3, 3)
    arrive_all(sent_b, got_b, 1, 1)
    middle(1, got_b, back_b)
    push_all(back_b, home_b, 4, 4, 1)
    push_all(back_c, home_c, 5, 4 + quarters, 1)

    def add_pair(tile, home, steps):
        found, right = [], ([], [])
        for step in steps:
            quarter = quarter_of(step)
            found.append(jnp.concatenate([home[quarter * slabs + slab] for slab in range(slabs)], 0))
            for part in range(2):
                right[part].append(back_table[tile * quarters + quarter, part])
        left = halves(jnp.concatenate(found, 1))
        sum_ref[...] += product(left, [jnp.concatenate(part, 0) for part in right])

    arrive_all(back_a, home_a, 3, 3)

    @pl.loop(0, quarters, step=2)
    def _(step):
        add_pair(0, home_a, (step, step + 1))

    wav_copy((me + 1) % wav, 0, wav - 1).wait()

    slab_sums = []
    for slab in range(slabs):
        total = energy_wav[slab]
        for quarter in range(1, quarters):
            total = total + energy_wav[quarter * slabs + slab]
        slab_sums.append(total)
    weighted = slab_sums[0] * mass_ref[0]
    for slab in range(1, slabs):
        weighted = weighted + slab_sums[slab] * mass_ref[slab]
    energy_lev[level] = weighted

    @pl.when(level < lev - 1)
    def _():
        pl.semaphore_wait(ready, lev - 1 - level)

    for other in range(lev):
        @pl.when(level != other)
        def _():
            lev_copy(other, level).start()

    for pair in range(0, quarters, 2):
        for step in arrivals[pair : pair + 2]:
            arrive_step(back_b, home_b, 4, 4, step)
        add_pair(1, home_b, arrivals[pair : pair + 2])

    def collect_energies():
        lev_copy((level + 1) % lev, 0, lev - 1).wait()

        total = energy_lev[0]
        for other in range(1, lev):
            total = total + energy_lev[other]
        fill = jnp.zeros((8 - slabs - 1, LANES), jnp.float32)
        energy_ref[...] = jnp.concatenate(slab_sums + [total / (lev * slabs), fill], 0)

    for side in range(2):
        values = [jnp.zeros((rows, LANES), jnp.float32)] * slabs
        for place_of in range(2 * side, 2 * side + 2):
            if place_of == quarters - 1:
                collect_energies()
            arrive_step(back_c, home_c, 5, 4 + quarters, arrivals[place_of])
            for slab in range(slabs):
                w = quarter_of(arrivals[place_of]) * slabs + slab
                values[slab] = values[slab] + unpack(home_c[w], quarter_starts(place_of))
        for slab in range(slabs):
            value_high, value_low = halves(values[slab])
            at = (slice(slab * rows, (slab + 1) * rows), slice(side * LANES, (side + 1) * LANES))
            tail_ref[(0,) + at] = value_high
            tail_ref[(1,) + at] = value_low

    for phase, (source, target) in enumerate(
        ((sent_a, got_a), (sent_b, got_b), (sent_c, got_c), (back_a, home_a), (back_b, home_b), (back_c, home_c))
    ):
        batch_of(source, target, phase, 0, 0, wav - 1).wait_send()


def last_kernel(
    slabs, spans, sum_ref, tail_ref, tail_table, energy_ref, out_hbm, energies_hbm, total_hbm,
    out, energies, total, sems,
):
    copies = []

    def send(source, target):
        copies.append(pltpu.make_async_copy(source, target, sems.at[len(copies)]))
        copies[-1].start()

    def ready(span):
        return product((tail_ref[0], tail_ref[1]), (tail_table[0, :, span], tail_table[1, :, span]))

    def write(span, value):
        out[:, span] = sum_ref[:, span] + value
        send(out.at[:, span], out_hbm.at[:, span])

    held = ready(spans[0])
    for n in range(1, len(spans)):
        following = ready(spans[n])
        write(spans[n - 1], held)
        held = following
    write(spans[-1], held)
    sums = jnp.sum(energy_ref[...], axis=1, keepdims=True)
    for slab in range(slabs):
        energies[slab] = sums[slab, 0]
    total[0] = sums[slabs, 0]
    send(energies, energies_hbm)
    send(total, total_hbm)
    for copy in copies:
        copy.wait()


def cos_sin(phases, length):
    angles = 2.0 * np.pi / length * (phases % length)
    return np.stack([np.cos(angles), np.sin(angles)])


def fused(grid_field, truncation_limit, diffusion_order, diffusion_strength, mass_weight):
    slabs, rows, length = grid_field.shape
    wav, lev = lax.axis_size("wav"), lax.axis_size("lev")
    quarters = wav // slabs
    columns = length // 2 // quarters
    tail = columns + 1 - LANES
    groups = LANES // tail
    group_rows = -(-(-(-2 * rows // groups)) // 8) * 8
    padded = -(-rows // 16) * 16
    fine_rows = 32
    sizes = (slabs, rows, length, wav, lev, quarters, columns, padded, tail, groups, group_rows, fine_rows)
    turn = length // 4
    place = np.arange(2 * LANES)
    starts = np.arange(quarters) * columns
    plain_waves = starts[:, None] + (place // LANES * HALF + place % HALF)[None]
    plain_phase = np.broadcast_to((place % LANES >= HALF) * turn, plain_waves.shape)
    part = LANES // 4
    tail_waves = (starts[place // HALF] + LANES + place % part)[None]
    tail_phase = (place % HALF >= part)[None] * turn
    waves = np.concatenate([plain_waves, tail_waves])
    phase = np.concatenate([plain_phase, tail_phase])
    steps = np.arange(length // fine_rows) * fine_rows
    near = np.arange(fine_rows)
    positions = np.arange(length)
    single = lambda array: jnp.asarray(array, jnp.float32)
    seeds = single(
        np.concatenate(
            [
                cos_sin(near[None, :, None] * waves[:, None, :] + phase[:, None, :], length),
                cos_sin(steps[None, :, None] * waves[:, None, :], length),
            ],
            2,
        )
    )
    by_tile = lambda array: np.concatenate(
        [array[:quarters, :LANES].ravel(), array[:quarters, LANES:].ravel(), array[quarters]]
    )[::fine_rows]
    back_seeds = single(
        np.concatenate(
            [
                cos_sin(near[:, None] * positions[None], length),
                cos_sin(by_tile(waves)[:, None] * positions[None] + by_tile(phase)[:, None], length),
            ],
            1,
        )
    )
    inner = np.arange(padded)
    turns = cos_sin(np.arange(wav)[:, None, None] * inner[None, :, None], length)
    twiddle = single(np.repeat(turns, HALF, 3).transpose(1, 2, 0, 3).reshape(wav, padded, LANES))
    base_exact = cos_sin(wav * inner[:, None] * inner[None], length)
    base_exact = base_exact * ((inner[:, None] < rows) & (inner[None] < rows))
    base_exact = base_exact.reshape(2 * padded, padded).astype(np.float32)
    base_high = base_exact.astype(jnp.bfloat16)
    base_low = (base_exact - base_high.astype(np.float32)).astype(jnp.bfloat16)
    base = jnp.asarray(np.concatenate([base_high, base_low, base_high], 1))
    vmem, hbm = pl.BlockSpec(memory_space=pltpu.VMEM), pl.BlockSpec(memory_space=pltpu.HBM)
    f32, bf16, i32 = jnp.float32, jnp.bfloat16, jnp.int32
    sent = pltpu.VMEM((wav + slabs, rows, LANES), f32)
    whole = pltpu.VMEM((wav, rows, LANES), f32)
    small = pltpu.VMEM((wav, group_rows, LANES), f32)
    dma = pltpu.SemaphoreType.DMA
    partial_sum, tails, tail_table, energy_rows = pl.pallas_call(
        functools.partial(fused_kernel, sizes),
        out_shape=(
            jax.ShapeDtypeStruct((slabs * rows, length), f32),
            jax.ShapeDtypeStruct((2, slabs * rows, 2 * LANES), bf16),
            jax.ShapeDtypeStruct((2, 2 * LANES, length), bf16),
            jax.ShapeDtypeStruct((8, LANES), f32),
        ),
        in_specs=[hbm] * 9,
        out_specs=(vmem,) * 4,
        scratch_shapes=[
            pltpu.VMEM((slabs * rows, length), f32),
            pltpu.VMEM((length,), i32),
            pltpu.SMEM((slabs,), i32),
            pltpu.SMEM((slabs,), f32),
            pltpu.SMEM((slabs,), f32),
            pltpu.VMEM((2, quarters + 2) + seeds.shape[2:], f32),
            pltpu.VMEM(back_seeds.shape, f32),
            pltpu.VMEM(twiddle.shape, f32),
            pltpu.VMEM(base.shape, bf16),
            pltpu.VMEM((2, slabs * rows, length), bf16),
            pltpu.VMEM((2, length, 2 * LANES), bf16),
            pltpu.VMEM((2 * quarters, 2, LANES, length), bf16),
            sent, sent, small, whole, whole, small, whole, whole, small, whole, whole, small,
            whole,
            pltpu.VMEM((wav, padded, LANES), f32),
            pltpu.VMEM((wav, padded, 3 * LANES), f32),
            pltpu.VMEM((8, LANES), f32),
            pltpu.VMEM((wav, 1, LANES), f32),
            pltpu.VMEM((lev, 1, LANES), f32),
            dma((8,)), dma((6,)), dma((4 + 2 * quarters,)), dma((4,)),
            pltpu.SemaphoreType.REGULAR,
        ],
        compiler_params=pltpu.CompilerParams(
            collective_id=0, has_side_effects=True, vmem_limit_bytes=40 * 1024 * 1024
        ),
        name="fused_step",
    )(
        *(
            pltpu.with_memory_space_constraint(array, pltpu.HBM)
            for array in (
                grid_field.reshape(slabs * rows, length), truncation_limit, diffusion_order,
                diffusion_strength, mass_weight, seeds, back_seeds, twiddle, base,
            )
        )
    )
    spans = [slice(at, min(at + 2 * LANES, length)) for at in range(0, length, 2 * LANES)]
    filtered, energies, total = pl.pallas_call(
        functools.partial(last_kernel, slabs, spans),
        out_shape=(
            jax.ShapeDtypeStruct((slabs * rows, length), f32),
            jax.ShapeDtypeStruct((slabs,), f32),
            jax.ShapeDtypeStruct((1,), f32),
        ),
        in_specs=[vmem] * 4,
        out_specs=(hbm,) * 3,
        scratch_shapes=[
            pltpu.VMEM((slabs * rows, length), f32),
            pltpu.SMEM((slabs,), f32),
            pltpu.SMEM((1,), f32),
            dma((2 + len(spans),)),
        ],
        compiler_params=pltpu.CompilerParams(vmem_limit_bytes=12 * 1024 * 1024),
        name="last_product",
    )(partial_sum, tails, tail_table, energy_rows)
    return filtered.reshape(slabs, rows, length), energies, total[0]


def fits(shape):
    slabs, rows, length = shape
    wav = lax.axis_size("wav")
    if wav != 8 or slabs != 2 or rows % 8 or length % 16 or length != rows * wav:
        return False
    columns = length * slabs // 2 // wav
    return length % 32 == 0 and LANES <= columns < LANES + LANES // 4


def local(grid_field, truncation_limit, diffusion_order, diffusion_strength, mass_weight):
    slab_count, row_count, length = grid_field.shape
    if fits(grid_field.shape):
        return fused(
            grid_field, truncation_limit, diffusion_order, diffusion_strength, mass_weight
        )
    cosine_table, sine_table = tables(length)
    filtered, partial_value = half_plane(
        grid_field, truncation_limit, diffusion_order, diffusion_strength, cosine_table, sine_table
    )
    total_slabs = lax.axis_size("lev") * slab_count
    energies = lax.psum(partial_value, "wav")
    weighted_sum = lax.psum(jnp.sum(mass_weight * energies), "lev")
    total_energy = weighted_sum / total_slabs
    return (filtered, energies, total_energy)


def solution(mesh):
    placed = (P("lev", "wav", None), P(), P("lev"), P("lev"), P("lev"))
    return jax.shard_map(
        local,
        mesh=mesh,
        in_specs=placed,
        out_specs=(P("lev", "wav", None), P("lev"), P()),
        check_vma=False,
    )
```

```python
import functools

import jax
import jax.numpy as jnp
import numpy as np
from jax import lax
from jax.experimental import pallas as pl
from jax.experimental.pallas import tpu as pltpu
from jax.sharding import PartitionSpec as P

product_precision = lax.Precision.HIGH


def tables(length):
    step = 32
    coarse = -(-length // step)
    columns = np.arange(length)
    high = 2.0 * np.pi / length * (np.arange(coarse)[:, None] * step * columns[None, :] % length)
    low = 2.0 * np.pi / length * (np.arange(step)[:, None] * columns[None, :] % length)
    cos_high, sin_high = (jnp.asarray(f(high), jnp.float32)[:, None] for f in (np.cos, np.sin))
    cos_low, sin_low = (jnp.asarray(f(low), jnp.float32)[None] for f in (np.cos, np.sin))
    cosine = cos_high * cos_low - sin_high * sin_low
    sine = sin_high * cos_low + cos_high * sin_low
    return tuple(t.reshape(coarse * step, length)[:length] for t in (cosine, sine))


def signed(positions, length):
    return jnp.where(positions < length // 2, positions, positions - length)


def transform(values, cosine_table, sine_table, direction):
    with_cosine = jnp.einsum("scpi,iq->scpq", values, cosine_table, precision=product_precision)
    with_sine = jnp.einsum("scpi,iq->scpq", values, sine_table, precision=product_precision)
    if direction < 0:
        real_part = with_cosine[:, 0] + with_sine[:, 1]
        imaginary = with_cosine[:, 1] - with_sine[:, 0]
    else:
        real_part = with_cosine[:, 0] - with_sine[:, 1]
        imaginary = with_cosine[:, 1] + with_sine[:, 0]
    return jnp.stack([real_part, imaginary], axis=1)


def damping(wave_rows, limits, length, diffusion_order, diffusion_strength):
    wave_first = signed(jnp.arange(length, dtype=jnp.int32), length)
    rows_float = wave_rows.astype(jnp.float32)
    first_float = wave_first.astype(jnp.float32)
    scaled_radius = (rows_float[:, None] ** 2 + first_float[None, :] ** 2) / (0.5 * length) ** 2
    inside = (jnp.abs(wave_first)[None, :] <= limits[:, None]).astype(jnp.float32)
    powered = jnp.power(scaled_radius[None], diffusion_order.astype(jnp.float32)[:, None, None])
    return inside[None] / (1.0 + diffusion_strength[:, None, None] * powered)


def mirrored(values):
    return jnp.roll(jnp.flip(values, -1), 1, -1)


def half_plane(
    grid_field, truncation_limit, diffusion_order, diffusion_strength, cosine_table, sine_table
):
    length = grid_field.shape[2]
    half = length // 2
    row_real = jnp.einsum("sij,jl->sli", grid_field, cosine_table[:, :half], precision=product_precision)
    row_imag = -jnp.einsum("sij,jl->sli", grid_field, sine_table[:, :half], precision=product_precision)
    nyquist = jnp.einsum("sij,j->si", grid_field, cosine_table[:, half], precision=product_precision)
    zero_row = (jnp.arange(half, dtype=jnp.int32) == 0)[None, :, None]
    row_imag = jnp.where(zero_row, nyquist[:, None, :], row_imag)
    along_rows = jnp.stack([row_real, row_imag], axis=1)
    spectrum = transform(
        lax.all_to_all(along_rows, "wav", split_axis=2, concat_axis=3, tiled=True),
        cosine_table,
        sine_table,
        -1,
    )
    column_count = spectrum.shape[2]
    wav_index = lax.axis_index("wav")
    offset = wav_index * column_count
    wave_rows = offset + jnp.arange(column_count, dtype=jnp.int32)
    limits = lax.dynamic_slice(truncation_limit, (offset,), (column_count,))
    damp_main = damping(wave_rows, limits, length, diffusion_order, diffusion_strength)
    nyquist_rows = signed(jnp.full((1,), half, jnp.int32), length)
    damp_top = damping(
        nyquist_rows, truncation_limit[half : half + 1], length, diffusion_order, diffusion_strength
    )[:, 0]
    damped = spectrum * damp_main[:, None]
    packed_real = spectrum[:, 0, 0, :]
    packed_imag = spectrum[:, 1, 0, :]
    back_real = mirrored(packed_real)
    back_imag = mirrored(packed_imag)
    zero_real = (packed_real + back_real) * 0.5 * damp_main[:, 0]
    zero_imag = (packed_imag - back_imag) * 0.5 * damp_main[:, 0]
    top_real = (packed_imag + back_imag) * 0.5 * damp_top
    top_imag = (back_real - packed_real) * 0.5 * damp_top
    is_zero = wave_rows == 0
    column_weight = jnp.where(is_zero, 0.0, 2.0).astype(jnp.float32)
    edge = jnp.sum(zero_real**2 + zero_imag**2 + top_real**2 + top_imag**2, axis=-1)
    main_sum = jnp.sum(damped * damped * column_weight[None, None, :, None], axis=(1, 2, 3))
    partial_value = (main_sum + jnp.where(wav_index == 0, edge, 0.0)) / float(length) ** 4
    zero_column = is_zero[None, :, None]
    repacked = jnp.stack(
        [
            jnp.where(zero_column, (zero_real - top_imag)[:, None, :], damped[:, 0]),
            jnp.where(zero_column, (zero_imag + top_real)[:, None, :], damped[:, 1]),
        ],
        axis=1,
    )
    along_first = transform(repacked, cosine_table, sine_table, 1)
    inverse_area = 1.0 / float(length) ** 2
    received = lax.all_to_all(along_first, "wav", split_axis=3, concat_axis=2, tiled=True)
    row_weight = jnp.where(jnp.arange(half, dtype=jnp.int32) == 0, 1.0, 2.0).astype(jnp.float32)[
        :, None
    ]
    with_cosine = jnp.einsum(
        "spi,pj->sij", received[:, 0] * row_weight, cosine_table[:half], precision=product_precision
    )
    with_sine = jnp.einsum(
        "spi,pj->sij", received[:, 1] * row_weight, sine_table[:half], precision=product_precision
    )
    top_term = received[:, 1, 0, :][:, :, None] * cosine_table[half][None, None, :]
    filtered = (with_cosine - with_sine + top_term) * inverse_area
    return (filtered, partial_value)


LANES = 128
HALF = LANES // 2
MESH = pl.DeviceIdType.MESH


def halves(values):
    high = values.astype(jnp.bfloat16)
    return high, (values - high.astype(jnp.float32)).astype(jnp.bfloat16)


def product(left, right):
    left = jnp.concatenate([left[0], left[1], left[0]], 1)
    right = jnp.concatenate([right[0], right[0], right[1]], 0)
    return jnp.dot(left, right, preferred_element_type=jnp.float32)


def swap(value):
    count = value.shape[1] // LANES
    turned = [pltpu.roll(value[:, n * LANES : (n + 1) * LANES], HALF, 1) for n in range(count)]
    return jnp.concatenate(turned, 1) if count > 1 else turned[0]


def eight_points(x, sign, signs):
    turn = signs if sign < 0 else -signs

    def four(p, q, r, t):
        a0, a1, a2, a3 = p + r, p - r, q + t, swap(q - t) * turn
        return a0 + a2, a1 + a3, a0 - a2, a1 - a3

    e = four(x[0], x[2], x[4], x[6])
    o = four(x[1], x[3], x[5], x[7])
    root = 0.5**0.5
    odd = (
        o[0],
        root * (o[1] + swap(o[1]) * turn),
        swap(o[2]) * turn,
        root * (swap(o[3]) * turn - o[3]),
    )
    return [e[n] + odd[n] for n in range(4)] + [e[n] - odd[n] for n in range(4)]


def pieces(rows, group_rows, groups):
    found = []
    for group in range(groups):
        start, stop = group * group_rows, min((group + 1) * group_rows, 2 * rows)
        while start < stop:
            part = start // rows
            end = min(stop, (part + 1) * rows)
            found.append((group, start - group * group_rows, part, start - part * rows, end - start))
            start = end
    return found


def store_circle(target, span, steps, length):
    steps = steps.astype(jnp.float32)
    turn = jnp.floor(steps * (4.0 / length) + 0.5)
    angle = (steps - turn * (length // 4)) * (2.0 * np.pi / length)
    square = angle * angle
    cosine, sine = jnp.ones_like(angle), jnp.ones_like(angle)
    for n in range(10, 0, -2):
        cosine = 1.0 - cosine * square * (1.0 / (n * (n - 1)))
        sine = 1.0 - sine * square * (1.0 / (n * (n + 1)))
    sine = sine * angle
    quadrant = turn.astype(jnp.int32) % 4
    odd = quadrant % 2 == 1
    cos_part, sin_part = jnp.where(odd, sine, cosine), jnp.where(odd, cosine, sine)
    target[0, 0, span] = jnp.where((quadrant == 1) | (quadrant == 2), -cos_part, cos_part)
    target[1, 0, span] = jnp.where(quadrant >= 2, -sin_part, sin_part)


def fused_kernel(
    sizes,
    grid_hbm, limit_hbm, order_hbm, strength_hbm, mass_hbm, seeds_hbm, back_seeds_hbm, twiddle_hbm, base_hbm,
    sum_ref, tail_ref, tail_table, energy_ref,
    grid, limit_ref, order_ref, strength_ref, mass_ref, seeds, first_seeds, back_seeds, twiddle, base,
    grid_parts, table, back_table, near_table,
    sent_a, sent_b, sent_c, got_a, got_b, got_c, back_a, back_b, back_c, home_a, home_b, home_c,
    rest, work, damp, energy_sums, energy_wav, energy_lev,
    load_sems, send_sems, recv_sems, energy_sems, ready,
):
    slabs, rows, length, wav, lev, quarters, columns, padded, tail, groups, group_rows, fine_rows = sizes
    half = length // 2
    quarter_lanes = LANES // 2
    part_lanes = quarter_lanes // 2
    me = lax.axis_index("wav")
    level = lax.axis_index("lev")
    my_quarter, my_slab = me // slabs, me % slabs

    barrier = pltpu.get_barrier_semaphore()

    def quarter_of(step):
        down, across = 1 - step % 2, 1 - step // 2
        y, x = my_quarter // 2, my_quarter % 2
        return (y + down - 2 * y * down) * 2 + (x + across - 2 * x * across)

    early = -(-rows // 16) * 16
    spans = [slice(0, early), slice(early, slabs * rows)]
    ahead = quarter_of(0)
    def load(source, target, sem):
        copy = pltpu.make_async_copy(source, target, load_sems.at[sem])
        copy.start()
        return copy

    grid_loads = [load(grid_hbm.at[span], grid.at[span], n) for n, span in enumerate(spans)]
    seeds_load = load(seeds_hbm, seeds, len(spans))

    @pl.loop(1, wav)
    def _(step):
        pl.semaphore_signal(barrier, inc=1, device_id=(level, (me + step) % wav), device_id_type=MESH)

    for other in range(1, lev):
        @pl.when(level < other)
        def _():
            pl.semaphore_signal(barrier, inc=1, device_id=(other, me), device_id_type=MESH)

    def push(source, target, phase, recv, w):
        @pl.when(w != me)
        def _():
            pltpu.make_async_remote_copy(
                src_ref=source.at[w], dst_ref=target.at[me],
                send_sem=send_sems.at[phase], recv_sem=recv_sems.at[recv],
                device_id=(level, w), device_id_type=MESH,
            ).start()

        @pl.when(w == me)
        def _():
            target[w] = source[w]

    def push_quarter(source, target, phase, recv, quarter):
        for n in range(slabs):
            push(source, target, phase, recv, quarter * slabs + n)

    def push_all(source, target, phase, recv):
        @pl.loop(0, quarters)
        def _(step):
            push_quarter(source, target, phase, recv, quarter_of(step))

    def push_steps(source, target, phase, recv, steps):
        for step in steps:
            push_quarter(source, target, phase, recv, quarter_of(step))

    def batch_of(source, target, phase, recv, first, count):
        return pltpu.make_async_remote_copy(
            src_ref=source.at[pl.ds(first, count)], dst_ref=target.at[pl.ds(first, count)],
            send_sem=send_sems.at[phase], recv_sem=recv_sems.at[recv],
            device_id=(level, (me + 1) % wav), device_id_type=MESH,
        )

    def arrive(source, target, phase, recv, count):
        batch_of(source, target, phase, recv, 0, count).wait_recv()

    def sent_all(source, target, phase):
        batch_of(source, target, phase, 0, 0, wav - 1).wait_send()

    lane = lax.broadcasted_iota(jnp.int32, (1, LANES), 1)
    signs = jnp.where(lane < HALF, 1.0, -1.0)
    layout = pieces(rows, group_rows, groups)
    wide = (0, HALF)

    def inside_part(starts, part):
        return (lane >= starts[part]) & (lane < starts[part] + tail)

    def pack(tile, starts):
        shifted = {}
        for group, at, part, start, count in layout:
            piece = jnp.where(inside_part(starts, part), tile(start, count), 0.0)
            shift = (group * tail - starts[part]) % LANES
            shifted.setdefault(group, []).append(pltpu.roll(piece, shift, 1) if shift else piece)
        packed = jnp.zeros((group_rows, LANES), jnp.float32)
        for found in shifted.values():
            whole = jnp.concatenate(found, 0) if len(found) > 1 else found[0]
            if whole.shape[0] < group_rows:
                fill = jnp.zeros((group_rows - whole.shape[0], LANES), jnp.float32)
                whole = jnp.concatenate([whole, fill], 0)
            packed = packed + whole
        return packed

    def unpack(packed, starts):
        found = {0: [], 1: []}
        for group, at, part, start, count in layout:
            piece = packed[at : at + count]
            shift = (starts[part] - group * tail) % LANES
            piece = pltpu.roll(piece, shift, 1) if shift else piece
            found[part].append(jnp.where(inside_part(starts, part), piece, 0.0))
        return jnp.concatenate(found[0], 0) + jnp.concatenate(found[1], 0)

    def quarter_starts(quarter):
        first = quarter % 2 * quarter_lanes
        return (first, first + part_lanes)

    def make_table(start, piece, lanes):
        cos_f, sin_f = start[0, piece, :fine_rows, lanes], start[1, piece, :fine_rows, lanes]

        @pl.loop(0, length // fine_rows, unroll=2)
        def _(block):
            at = pl.ds(fine_rows + block, 1)
            cos_c, sin_c = start[0, piece, at][:, lanes], start[1, piece, at][:, lanes]
            span = pl.ds(pl.multiple_of(block * fine_rows, fine_rows), fine_rows)
            value_high, value_low = halves(cos_c * cos_f - sin_c * sin_f)
            table[0, span, lanes] = value_high
            table[1, span, lanes] = value_low

    def keep(result, piece):
        for slab in range(slabs):
            w = piece * slabs + slab
            sent_a[w] = result[slab * rows : (slab + 1) * rows, :LANES]
            sent_b[w] = result[slab * rows : (slab + 1) * rows, LANES:]

    front, behind = slice(0, LANES), slice(LANES, 2 * LANES)
    ahead_wave = ahead * columns + lane % HALF
    nearby = lax.broadcasted_iota(jnp.int32, (fine_rows, 1), 0)
    afar = lax.broadcasted_iota(jnp.int32, (length // fine_rows, 1), 0) * fine_rows
    store_circle(first_seeds, slice(0, fine_rows), nearby * ahead_wave + lane // HALF * (length // 4), length)
    store_circle(first_seeds, slice(fine_rows, fine_rows + length // fine_rows), afar * ahead_wave, length)
    make_table(first_seeds, 0, front)

    def first_rows(span):
        high, low = halves(grid[span])
        grid_parts[0, span] = high
        grid_parts[1, span] = low
        return product((grid_parts[0, span], grid_parts[1, span]), (table[0, :, front], table[1, :, front]))

    grid_loads[0].wait()
    result = first_rows(spans[0])
    sent_a[ahead * slabs] = result[:rows]
    if early > rows:
        sent_a[ahead * slabs + 1, : early - rows] = result[rows:]
    pl.semaphore_wait(barrier, wav - 1 + level)
    push(sent_a, got_a, 0, 0, ahead * slabs)
    grid_loads[1].wait()
    sent_a[ahead * slabs + 1, early - rows :] = first_rows(spans[1])
    push(sent_a, got_a, 0, 0, ahead * slabs + 1)
    seeds_load.wait()
    make_table(seeds, ahead, behind)
    result = product((grid_parts[0], grid_parts[1]), (table[0, :, behind], table[1, :, behind]))
    for slab in range(slabs):
        sent_b[ahead * slabs + slab] = result[slab * rows : (slab + 1) * rows]

    later = (
        (limit_hbm, limit_ref), (order_hbm, order_ref), (strength_hbm, strength_ref), (mass_hbm, mass_ref),
        (twiddle_hbm, twiddle), (base_hbm, base), (back_seeds_hbm, back_seeds),
    )
    other_loads = [load(source, target, n) for n, (source, target) in enumerate(later)]

    @pl.loop(0, quarters)
    def _(step):
        plain_step = (step + quarters - 1) // quarters
        piece = quarter_of(step) * plain_step + quarters * (1 - plain_step)
        make_table(seeds, piece, slice(0, 2 * LANES))
        keep(product((grid_parts[0], grid_parts[1]), (table[0], table[1])), piece)

        @pl.when(step == 0)
        def _():
            for quarter in range(quarters):
                from_ref = sent_b if quarter // 2 else sent_a
                for slab in range(slabs):
                    sent_c[quarter * slabs + slab] = pack(
                        lambda start, many: from_ref[wav + slab, start : start + many], quarter_starts(quarter)
                    )
            push_all(sent_c, got_c, 2, 2)

        @pl.when(step > 0)
        def _():
            push_quarter(sent_a, got_a, 0, 0, piece)

        @pl.when(step == quarters - 1)
        def _():
            push_all(sent_b, got_b, 1, 1)

    for other in range(lev - 1):
        @pl.when(other < level)
        def _():
            pl.semaphore_signal(ready, inc=1, device_id=(other, me), device_id_type=MESH)

    for other_load in other_loads:
        other_load.wait()
    place = lax.broadcasted_iota(jnp.int32, (1, 3 * LANES), 1)
    column = place // LANES * HALF + place % HALF
    wave = my_quarter * columns + column
    valid = (column < columns) | ((column == columns) & (wave == half))
    single = (wave == 0) | (wave == half)
    out_weight = jnp.where(single, 1.0, 2.0) / float(length) ** 2
    energy_weight = jnp.where(single, 1.0, 0.5)
    all_limits = limit_ref[...].reshape(1, length)
    limits = jnp.full((1, 3 * LANES), -1, jnp.int32)
    for quarter in range(quarters):
        found = []
        for tile in range(3):
            start = quarter * columns + tile * HALF
            found += [all_limits[:, start : start + HALF]] * 2
        limits = jnp.where(my_quarter == quarter, jnp.concatenate(found, 1), limits)
    limits = jnp.where(valid, limits, -1)
    order = order_ref[my_slab]
    strength = strength_ref[my_slab]
    wave_square = wave.astype(jnp.float32) ** 2

    @pl.loop(0, wav)
    def _(m):
        row = lax.broadcasted_iota(jnp.int32, (padded, 1), 0)
        q = row * wav + m
        signed_q = jnp.where(q < half, q, q - length)
        radius = (wave_square + signed_q.astype(jnp.float32) ** 2) / (0.5 * length) ** 2
        square = radius * radius
        powered = jnp.where(order >= 3, square, 1.0) * jnp.where(order % 2 == 1, radius, square)
        inside = (jnp.abs(signed_q) <= limits) & (row < rows)
        damp[m] = jnp.where(inside, out_weight / (1.0 + strength * powered), 0.0)
        work[m, rows:] = jnp.zeros((padded - rows, LANES), jnp.float32)

    blocks = LANES // fine_rows
    plain = 2 * quarters * blocks

    def back_piece(at, target, span):
        row = pl.ds(fine_rows + at, 1)
        cos_c, sin_c = back_seeds[0, row], back_seeds[1, row]
        value_high, value_low = halves(cos_c * back_seeds[0, :fine_rows] - sin_c * back_seeds[1, :fine_rows])
        target[0, span] = value_high
        target[1, span] = value_low

    @pl.loop(0, 2 * quarters)
    def _(n):
        @pl.loop(0, blocks)
        def _(block):
            span = pl.ds(pl.multiple_of(block * fine_rows, fine_rows), fine_rows)
            back_piece(n * blocks + block, back_table.at[n], span)

    for target, steps in ((near_table, (0, quarters - 1)), (tail_table, range(1, quarters - 1))):
        for place_of, step in enumerate(steps):
            for part in range(2):
                block = 2 * place_of + part
                at = plain + 2 * quarter_of(step) + part
                back_piece(at, target, slice(block * fine_rows, (block + 1) * fine_rows))

    sum_ref[...] = jnp.zeros_like(sum_ref)
    energy_sums[...] = jnp.zeros_like(energy_sums)

    def along(value):
        value_high, value_low = halves(value)
        stacked = jnp.concatenate([value_high, value_high, value_low], 0)
        return jnp.dot(base[...], stacked, preferred_element_type=jnp.float32)

    block_rows = 24
    batch = 2

    def in_blocks(body):
        for start in range(0, rows, block_rows):
            body(start, min(block_rows, rows - start))

    def middle(tile, source, target):
        span_of = slice(tile * LANES, (tile + 1) * LANES)
        all_signs = jnp.concatenate([signs] * batch, 1)

        def split(start, many):
            span = pl.ds(start, many)
            for m, value in enumerate(eight_points([source[w, span] for w in range(wav)], -1, signs)):
                work[m, span] = value

        in_blocks(split)

        def residues(first, sums):
            found = range(first, first + batch)
            beside = lambda pick: jnp.concatenate([pick(m) for m in found], 1)
            packed_turn = beside(lambda m: twiddle[m])
            other_turn = swap(packed_turn)
            low = jnp.concatenate([lane] * batch, 1) < HALF
            cos_t = jnp.where(low, packed_turn, other_turn)
            sin_t = jnp.where(low, other_turn, -packed_turn)
            value = beside(lambda m: work[m])
            both = along(value * cos_t + swap(value) * sin_t)
            value = both[:padded] + swap(both[padded:]) * all_signs
            value = value * beside(lambda m: damp[m, :, span_of])
            sums = sums + jnp.sum((value * value).reshape(padded // 8, 8, batch * LANES), axis=0)
            both = along(value)
            value = both[:padded] - swap(both[padded:]) * all_signs
            value = value * cos_t - swap(value) * sin_t
            for n, m in enumerate(found):
                work[m] = value[:, n * LANES : (n + 1) * LANES]
            return sums

        sums = jnp.zeros((8, batch * LANES), jnp.float32)
        for first in range(0, wav, batch):
            sums = residues(first, sums)
        sums = sum(sums[:, n * LANES : (n + 1) * LANES] for n in range(batch))
        energy_sums[...] += sums * energy_weight[:, span_of]

        if tile == 1:
            announce()

        def join(start, many):
            span = pl.ds(start, many)
            for w, value in enumerate(eight_points([work[m, span] for m in range(wav)], 1, signs)):
                target[w, span] = value

        in_blocks(join)

    def wav_copy(target, slot, count=1):
        return pltpu.make_async_remote_copy(
            src_ref=energy_wav.at[pl.ds(slot, count)], dst_ref=energy_wav.at[pl.ds(slot, count)],
            send_sem=energy_sems.at[0], recv_sem=energy_sems.at[1],
            device_id=(level, target), device_id_type=MESH,
        )

    def lev_copy(target, slot, count=1):
        return pltpu.make_async_remote_copy(
            src_ref=energy_lev.at[pl.ds(slot, count)], dst_ref=energy_lev.at[pl.ds(slot, count)],
            send_sem=energy_sems.at[0], recv_sem=energy_sems.at[2],
            device_id=(target, me), device_id_type=MESH,
        )

    def announce():
        energy_wav[me] = jnp.sum(energy_sums[...], axis=0, keepdims=True)

        @pl.loop(1, wav)
        def _(step):
            wav_copy((me + step) % wav, me).start()

    arrive(sent_c, got_c, 2, 2, wav - 1)

    @pl.loop(0, wav)
    def _(w):
        rest[w] = unpack(got_c[w], wide)

    middle(2, rest, rest)

    @pl.loop(0, wav)
    def _(w):
        back_c[w] = pack(lambda start, many: rest[w, start : start + many], wide)

    arrive(sent_a, got_a, 0, 0, wav - 1)
    middle(0, got_a, back_a)
    sent_all(sent_a, got_a, 0)
    push_all(back_a, home_a, 0, 3)
    arrive(sent_b, got_b, 1, 1, wav - 1)
    middle(1, got_b, back_b)
    sent_all(sent_b, got_b, 1)
    sent_all(sent_c, got_c, 2)
    near_steps, far_steps = (0, quarters - 1), range(1, quarters - 1)
    near_count = 2 * slabs - 1
    push_steps(back_b, home_b, 1, 4, near_steps)
    push_steps(back_c, home_c, 2, 5, near_steps)
    push_steps(back_b, home_b, 1, 6, far_steps)
    for n, step in enumerate(far_steps):
        push_steps(back_c, home_c, 2, 7 + n, (step,))

    def add_pair(tile, home, steps):
        found, right = [], ([], [])
        for step in steps:
            quarter = quarter_of(step)
            found.append(jnp.concatenate([home[quarter * slabs + slab] for slab in range(slabs)], 0))
            for part in range(2):
                right[part].append(back_table[tile * quarters + quarter, part])
        left = halves(jnp.concatenate(found, 1))
        sum_ref[...] += product(left, [jnp.concatenate(part, 0) for part in right])

    arrive(back_a, home_a, 0, 3, wav - 1)

    @pl.loop(0, quarters, step=2)
    def _(step):
        add_pair(0, home_a, (step, step + 1))

    wav_copy((me + 1) % wav, 0, wav - 1).wait()

    slab_sums = []
    for slab in range(slabs):
        total = energy_wav[slab]
        for quarter in range(1, quarters):
            total = total + energy_wav[quarter * slabs + slab]
        slab_sums.append(total)
    weighted = slab_sums[0] * mass_ref[0]
    for slab in range(1, slabs):
        weighted = weighted + slab_sums[slab] * mass_ref[slab]
    energy_lev[level] = weighted

    @pl.when(level < lev - 1)
    def _():
        pl.semaphore_wait(ready, lev - 1 - level)

    for other in range(lev):
        @pl.when(level != other)
        def _():
            lev_copy(other, level).start()

    def collect_energies():
        lev_copy((level + 1) % lev, 0, lev - 1).wait()

        total = energy_lev[0]
        for other in range(1, lev):
            total = total + energy_lev[other]
        fill = jnp.zeros((8 - slabs - 1, LANES), jnp.float32)
        energy_ref[...] = jnp.concatenate(slab_sums + [total / (lev * slabs), fill], 0)

    def with_tails(values, step, place_of):
        found = []
        for slab in range(slabs):
            value = unpack(home_c[quarter_of(step) * slabs + slab], quarter_starts(place_of))
            found.append(value if values is None else values[slab] + value)
        return found

    arrive(back_b, home_b, 1, 4, near_count)
    add_pair(1, home_b, near_steps)
    arrive(back_c, home_c, 2, 5, near_count)
    values = None
    for place_of, step in enumerate(near_steps):
        values = with_tails(values, step, place_of)
    sum_ref[...] += product(halves(jnp.concatenate(values, 0)), (near_table[0], near_table[1]))
    arrive(back_b, home_b, 1, 6, (quarters - 2) * slabs)
    add_pair(1, home_b, far_steps)
    sent_all(back_a, home_a, 0)
    sent_all(back_b, home_b, 1)
    collect_energies()
    values = None
    for n, step in enumerate(far_steps):
        arrive(back_c, home_c, 2, 7 + n, slabs)
        values = with_tails(values, step, n)
    for slab, value in enumerate(values):
        for part, found in enumerate(halves(value)):
            tail_ref[part, slab * rows : (slab + 1) * rows] = found
    sent_all(back_c, home_c, 2)


def last_kernel(
    slabs, spans, sum_ref, tail_ref, tail_table, energy_ref, out_hbm, energies_hbm, total_hbm,
    out, energies, total, sems,
):
    for span in spans:
        out[:, span] = sum_ref[:, span] + product(
            (tail_ref[0], tail_ref[1]), (tail_table[0, :, span], tail_table[1, :, span])
        )
        pltpu.make_async_copy(out.at[:, span], out_hbm.at[:, span], sems.at[0]).start()
    sums = jnp.sum(energy_ref[...], axis=1, keepdims=True)
    for slab in range(slabs):
        energies[slab] = sums[slab, 0]
    total[0] = sums[slabs, 0]
    copies = [
        pltpu.make_async_copy(energies, energies_hbm, sems.at[1]),
        pltpu.make_async_copy(total, total_hbm, sems.at[2]),
    ]
    for copy in copies:
        copy.start()
    for copy in copies + [pltpu.make_async_copy(out, out_hbm, sems.at[0])]:
        copy.wait()


def cos_sin(phases, length):
    angles = 2.0 * np.pi / length * (phases % length)
    return np.stack([np.cos(angles), np.sin(angles)])


def fused(grid_field, truncation_limit, diffusion_order, diffusion_strength, mass_weight):
    slabs, rows, length = grid_field.shape
    wav, lev = lax.axis_size("wav"), lax.axis_size("lev")
    quarters = wav // slabs
    columns = length // 2 // quarters
    tail = columns + 1 - LANES
    groups = LANES // tail
    group_rows = -(-2 * rows // groups)
    padded = -(-rows // 16) * 16
    fine_rows = 32
    sizes = (slabs, rows, length, wav, lev, quarters, columns, padded, tail, groups, group_rows, fine_rows)
    turn = length // 4
    place = np.arange(2 * LANES)
    starts = np.arange(quarters) * columns
    plain_waves = starts[:, None] + (place // LANES * HALF + place % HALF)[None]
    plain_phase = np.broadcast_to((place % LANES >= HALF) * turn, plain_waves.shape)
    part = LANES // 4
    tail_waves = (starts[place // HALF] + LANES + place % part)[None]
    tail_phase = (place % HALF >= part)[None] * turn
    waves = np.concatenate([plain_waves, tail_waves])
    phase = np.concatenate([plain_phase, tail_phase])
    steps = np.arange(length // fine_rows) * fine_rows
    near = np.arange(fine_rows)
    positions = np.arange(length)
    single = lambda array: jnp.asarray(array, jnp.float32)
    seeds = single(
        np.concatenate(
            [
                cos_sin(near[None, :, None] * waves[:, None, :] + phase[:, None, :], length),
                cos_sin(steps[None, :, None] * waves[:, None, :], length),
            ],
            2,
        )
    )
    by_tile = lambda array: np.concatenate(
        [array[:quarters, :LANES].ravel(), array[:quarters, LANES:].ravel(), array[quarters]]
    )[::fine_rows]
    back_seeds = single(
        np.concatenate(
            [
                cos_sin(near[:, None] * positions[None], length),
                cos_sin(by_tile(waves)[:, None] * positions[None] + by_tile(phase)[:, None], length),
            ],
            1,
        )
    )
    inner = np.arange(padded)
    turns = cos_sin(np.arange(wav)[:, None, None] * inner[None, :, None], length)
    twiddle = single(np.repeat(turns, HALF, 3).transpose(1, 2, 0, 3).reshape(wav, padded, LANES))
    base_exact = cos_sin(wav * inner[:, None] * inner[None], length)
    base_exact = base_exact * ((inner[:, None] < rows) & (inner[None] < rows))
    base_exact = base_exact.reshape(2 * padded, padded).astype(np.float32)
    base_high = base_exact.astype(jnp.bfloat16)
    base_low = (base_exact - base_high.astype(np.float32)).astype(jnp.bfloat16)
    base = jnp.asarray(np.concatenate([base_high, base_low, base_high], 1))
    vmem, hbm = pl.BlockSpec(memory_space=pltpu.VMEM), pl.BlockSpec(memory_space=pltpu.HBM)
    f32, bf16, i32 = jnp.float32, jnp.bfloat16, jnp.int32
    sent = pltpu.VMEM((wav + slabs, rows, LANES), f32)
    whole = pltpu.VMEM((wav, rows, LANES), f32)
    small = pltpu.VMEM((wav, group_rows, LANES), f32)
    dma = pltpu.SemaphoreType.DMA
    partial_sum, tails, tail_table, energy_rows = pl.pallas_call(
        functools.partial(fused_kernel, sizes),
        out_shape=(
            jax.ShapeDtypeStruct((slabs * rows, length), f32),
            jax.ShapeDtypeStruct((2, slabs * rows, LANES), bf16),
            jax.ShapeDtypeStruct((2, LANES, length), bf16),
            jax.ShapeDtypeStruct((8, LANES), f32),
        ),
        in_specs=[hbm] * 9,
        out_specs=(vmem,) * 4,
        scratch_shapes=[
            pltpu.VMEM((slabs * rows, length), f32),
            pltpu.VMEM((length,), i32),
            pltpu.SMEM((slabs,), i32),
            pltpu.SMEM((slabs,), f32),
            pltpu.SMEM((slabs,), f32),
            pltpu.VMEM(seeds.shape, f32),
            pltpu.VMEM((2, 1, seeds.shape[2], LANES), f32),
            pltpu.VMEM(back_seeds.shape, f32),
            pltpu.VMEM(twiddle.shape, f32),
            pltpu.VMEM(base.shape, bf16),
            pltpu.VMEM((2, slabs * rows, length), bf16),
            pltpu.VMEM((2, length, 2 * LANES), bf16),
            pltpu.VMEM((2 * quarters, 2, LANES, length), bf16),
            pltpu.VMEM((2, LANES, length), bf16),
            sent, sent, small, whole, whole, small, whole, whole, small, whole, whole, small,
            whole,
            pltpu.VMEM((wav, padded, LANES), f32),
            pltpu.VMEM((wav, padded, 3 * LANES), f32),
            pltpu.VMEM((8, LANES), f32),
            pltpu.VMEM((wav, 1, LANES), f32),
            pltpu.VMEM((lev, 1, LANES), f32),
            dma((7,)), dma((3,)), dma((5 + quarters,)), dma((3,)),
            pltpu.SemaphoreType.REGULAR,
        ],
        compiler_params=pltpu.CompilerParams(
            collective_id=0, has_side_effects=True, vmem_limit_bytes=40 * 1024 * 1024
        ),
        name="fused_step",
    )(
        *(
            pltpu.with_memory_space_constraint(array, pltpu.HBM)
            for array in (
                grid_field.reshape(slabs * rows, length), truncation_limit, diffusion_order,
                diffusion_strength, mass_weight, seeds, back_seeds, twiddle, base,
            )
        )
    )
    spans = [slice(at, min(at + 2 * LANES, length)) for at in range(0, length, 2 * LANES)]
    filtered, energies, total = pl.pallas_call(
        functools.partial(last_kernel, slabs, spans),
        out_shape=(
            jax.ShapeDtypeStruct((slabs * rows, length), f32),
            jax.ShapeDtypeStruct((slabs,), f32),
            jax.ShapeDtypeStruct((1,), f32),
        ),
        in_specs=[vmem] * 4,
        out_specs=(hbm,) * 3,
        scratch_shapes=[
            pltpu.VMEM((slabs * rows, length), f32),
            pltpu.SMEM((slabs,), f32),
            pltpu.SMEM((1,), f32),
            dma((3,)),
        ],
        compiler_params=pltpu.CompilerParams(vmem_limit_bytes=12 * 1024 * 1024),
        name="last_product",
    )(partial_sum, tails, tail_table, energy_rows)
    return filtered.reshape(slabs, rows, length), energies, total[0]


def fits(shape):
    slabs, rows, length = shape
    wav = lax.axis_size("wav")
    if wav != 8 or slabs != 2 or rows % 8 or length % 16 or length != rows * wav:
        return False
    columns = length * slabs // 2 // wav
    return length % 32 == 0 and LANES <= columns < LANES + LANES // 4


def local(grid_field, truncation_limit, diffusion_order, diffusion_strength, mass_weight):
    slab_count, row_count, length = grid_field.shape
    if fits(grid_field.shape):
        return fused(
            grid_field, truncation_limit, diffusion_order, diffusion_strength, mass_weight
        )
    cosine_table, sine_table = tables(length)
    filtered, partial_value = half_plane(
        grid_field, truncation_limit, diffusion_order, diffusion_strength, cosine_table, sine_table
    )
    total_slabs = lax.axis_size("lev") * slab_count
    energies = lax.psum(partial_value, "wav")
    weighted_sum = lax.psum(jnp.sum(mass_weight * energies), "lev")
    total_energy = weighted_sum / total_slabs
    return (filtered, energies, total_energy)


def solution(mesh):
    placed = (P("lev", "wav", None), P(), P("lev"), P("lev"), P("lev"))
    return jax.shard_map(
        local,
        mesh=mesh,
        in_specs=placed,
        out_specs=(P("lev", "wav", None), P("lev"), P()),
        check_vma=False,
    )
```

```python
import functools

import jax
import jax.numpy as jnp
import numpy as np
from jax import lax
from jax.experimental import pallas as pl
from jax.experimental.pallas import tpu as pltpu
from jax.sharding import PartitionSpec as P

product_precision = lax.Precision.HIGH


def tables(length):
    step = 32
    coarse = -(-length // step)
    columns = np.arange(length)
    high = 2.0 * np.pi / length * (np.arange(coarse)[:, None] * step * columns[None, :] % length)
    low = 2.0 * np.pi / length * (np.arange(step)[:, None] * columns[None, :] % length)
    cos_high, sin_high = (jnp.asarray(f(high), jnp.float32)[:, None] for f in (np.cos, np.sin))
    cos_low, sin_low = (jnp.asarray(f(low), jnp.float32)[None] for f in (np.cos, np.sin))
    cosine = cos_high * cos_low - sin_high * sin_low
    sine = sin_high * cos_low + cos_high * sin_low
    return tuple(t.reshape(coarse * step, length)[:length] for t in (cosine, sine))


def signed(positions, length):
    return jnp.where(positions < length // 2, positions, positions - length)


def transform(values, cosine_table, sine_table, direction):
    with_cosine = jnp.einsum("scpi,iq->scpq", values, cosine_table, precision=product_precision)
    with_sine = jnp.einsum("scpi,iq->scpq", values, sine_table, precision=product_precision)
    if direction < 0:
        real_part = with_cosine[:, 0] + with_sine[:, 1]
        imaginary = with_cosine[:, 1] - with_sine[:, 0]
    else:
        real_part = with_cosine[:, 0] - with_sine[:, 1]
        imaginary = with_cosine[:, 1] + with_sine[:, 0]
    return jnp.stack([real_part, imaginary], axis=1)


def damping(wave_rows, limits, length, diffusion_order, diffusion_strength):
    wave_first = signed(jnp.arange(length, dtype=jnp.int32), length)
    rows_float = wave_rows.astype(jnp.float32)
    first_float = wave_first.astype(jnp.float32)
    scaled_radius = (rows_float[:, None] ** 2 + first_float[None, :] ** 2) / (0.5 * length) ** 2
    inside = (jnp.abs(wave_first)[None, :] <= limits[:, None]).astype(jnp.float32)
    powered = jnp.power(scaled_radius[None], diffusion_order.astype(jnp.float32)[:, None, None])
    return inside[None] / (1.0 + diffusion_strength[:, None, None] * powered)


def mirrored(values):
    return jnp.roll(jnp.flip(values, -1), 1, -1)


def half_plane(
    grid_field, truncation_limit, diffusion_order, diffusion_strength, cosine_table, sine_table
):
    length = grid_field.shape[2]
    half = length // 2
    row_real = jnp.einsum("sij,jl->sli", grid_field, cosine_table[:, :half], precision=product_precision)
    row_imag = -jnp.einsum("sij,jl->sli", grid_field, sine_table[:, :half], precision=product_precision)
    nyquist = jnp.einsum("sij,j->si", grid_field, cosine_table[:, half], precision=product_precision)
    zero_row = (jnp.arange(half, dtype=jnp.int32) == 0)[None, :, None]
    row_imag = jnp.where(zero_row, nyquist[:, None, :], row_imag)
    along_rows = jnp.stack([row_real, row_imag], axis=1)
    spectrum = transform(
        lax.all_to_all(along_rows, "wav", split_axis=2, concat_axis=3, tiled=True),
        cosine_table,
        sine_table,
        -1,
    )
    column_count = spectrum.shape[2]
    wav_index = lax.axis_index("wav")
    offset = wav_index * column_count
    wave_rows = offset + jnp.arange(column_count, dtype=jnp.int32)
    limits = lax.dynamic_slice(truncation_limit, (offset,), (column_count,))
    damp_main = damping(wave_rows, limits, length, diffusion_order, diffusion_strength)
    nyquist_rows = signed(jnp.full((1,), half, jnp.int32), length)
    damp_top = damping(
        nyquist_rows, truncation_limit[half : half + 1], length, diffusion_order, diffusion_strength
    )[:, 0]
    damped = spectrum * damp_main[:, None]
    packed_real = spectrum[:, 0, 0, :]
    packed_imag = spectrum[:, 1, 0, :]
    back_real = mirrored(packed_real)
    back_imag = mirrored(packed_imag)
    zero_real = (packed_real + back_real) * 0.5 * damp_main[:, 0]
    zero_imag = (packed_imag - back_imag) * 0.5 * damp_main[:, 0]
    top_real = (packed_imag + back_imag) * 0.5 * damp_top
    top_imag = (back_real - packed_real) * 0.5 * damp_top
    is_zero = wave_rows == 0
    column_weight = jnp.where(is_zero, 0.0, 2.0).astype(jnp.float32)
    edge = jnp.sum(zero_real**2 + zero_imag**2 + top_real**2 + top_imag**2, axis=-1)
    main_sum = jnp.sum(damped * damped * column_weight[None, None, :, None], axis=(1, 2, 3))
    partial_value = (main_sum + jnp.where(wav_index == 0, edge, 0.0)) / float(length) ** 4
    zero_column = is_zero[None, :, None]
    repacked = jnp.stack(
        [
            jnp.where(zero_column, (zero_real - top_imag)[:, None, :], damped[:, 0]),
            jnp.where(zero_column, (zero_imag + top_real)[:, None, :], damped[:, 1]),
        ],
        axis=1,
    )
    along_first = transform(repacked, cosine_table, sine_table, 1)
    inverse_area = 1.0 / float(length) ** 2
    received = lax.all_to_all(along_first, "wav", split_axis=3, concat_axis=2, tiled=True)
    row_weight = jnp.where(jnp.arange(half, dtype=jnp.int32) == 0, 1.0, 2.0).astype(jnp.float32)[
        :, None
    ]
    with_cosine = jnp.einsum(
        "spi,pj->sij", received[:, 0] * row_weight, cosine_table[:half], precision=product_precision
    )
    with_sine = jnp.einsum(
        "spi,pj->sij", received[:, 1] * row_weight, sine_table[:half], precision=product_precision
    )
    top_term = received[:, 1, 0, :][:, :, None] * cosine_table[half][None, None, :]
    filtered = (with_cosine - with_sine + top_term) * inverse_area
    return (filtered, partial_value)


LANES = 128
HALF = LANES // 2
MESH = pl.DeviceIdType.MESH


def halves(values):
    high = values.astype(jnp.bfloat16)
    return high, (values - high.astype(jnp.float32)).astype(jnp.bfloat16)


def product(left, right):
    left = jnp.concatenate([left[0], left[1], left[0]], 1)
    right = jnp.concatenate([right[0], right[0], right[1]], 0)
    return jnp.dot(left, right, preferred_element_type=jnp.float32)


def swap(value):
    count = value.shape[1] // LANES
    turned = [pltpu.roll(value[:, n * LANES : (n + 1) * LANES], HALF, 1) for n in range(count)]
    return jnp.concatenate(turned, 1) if count > 1 else turned[0]


def eight_points(x, sign, signs):
    turn = signs if sign < 0 else -signs

    def four(p, q, r, t):
        a0, a1, a2, a3 = p + r, p - r, q + t, swap(q - t) * turn
        return a0 + a2, a1 + a3, a0 - a2, a1 - a3

    e = four(x[0], x[2], x[4], x[6])
    o = four(x[1], x[3], x[5], x[7])
    root = 0.5**0.5
    odd = (
        o[0],
        root * (o[1] + swap(o[1]) * turn),
        swap(o[2]) * turn,
        root * (swap(o[3]) * turn - o[3]),
    )
    return [e[n] + odd[n] for n in range(4)] + [e[n] - odd[n] for n in range(4)]


def pieces(rows, group_rows, groups):
    found = []
    for group in range(groups):
        start, stop = group * group_rows, min((group + 1) * group_rows, 2 * rows)
        while start < stop:
            part = start // rows
            end = min(stop, (part + 1) * rows)
            found.append((group, start - group * group_rows, part, start - part * rows, end - start))
            start = end
    return found


def store_circle(target, span, steps, length):
    steps = steps.astype(jnp.float32)
    turn = jnp.floor(steps * (4.0 / length) + 0.5)
    angle = (steps - turn * (length // 4)) * (2.0 * np.pi / length)
    square = angle * angle
    cosine, sine = jnp.ones_like(angle), jnp.ones_like(angle)
    for n in range(10, 0, -2):
        cosine = 1.0 - cosine * square * (1.0 / (n * (n - 1)))
        sine = 1.0 - sine * square * (1.0 / (n * (n + 1)))
    sine = sine * angle
    quadrant = turn.astype(jnp.int32) % 4
    odd = quadrant % 2 == 1
    cos_part, sin_part = jnp.where(odd, sine, cosine), jnp.where(odd, cosine, sine)
    target[0, 0, span] = jnp.where((quadrant == 1) | (quadrant == 2), -cos_part, cos_part)
    target[1, 0, span] = jnp.where(quadrant >= 2, -sin_part, sin_part)


def fused_kernel(
    sizes,
    grid_hbm, limit_hbm, order_hbm, strength_hbm, mass_hbm, seeds_hbm, back_seeds_hbm, twiddle_hbm, base_hbm,
    sum_ref, tail_ref, tail_table, energy_ref,
    grid, limit_ref, order_ref, strength_ref, mass_ref, seeds, first_seeds, back_seeds, twiddle, base,
    grid_parts, table, back_table, near_table,
    sent_a, sent_b, sent_c, got_a, got_b, got_c, back_a, back_b, back_c, home_a, home_b, home_c,
    rest, work, damp, energy_sums, energy_wav, energy_lev,
    load_sems, send_sems, recv_sems, energy_sems, ready,
):
    slabs, rows, length, wav, lev, quarters, columns, padded, tail, groups, group_rows, fine_rows = sizes
    half = length // 2
    quarter_lanes = LANES // 2
    part_lanes = quarter_lanes // 2
    me = lax.axis_index("wav")
    level = lax.axis_index("lev")
    my_quarter, my_slab = me // slabs, me % slabs

    barrier = pltpu.get_barrier_semaphore()

    def quarter_of(step):
        down, across = 1 - step % 2, 1 - step // 2
        y, x = my_quarter // 2, my_quarter % 2
        return (y + down - 2 * y * down) * 2 + (x + across - 2 * x * across)

    early = -(-rows // 16) * 16
    spans = [slice(0, early), slice(early, slabs * rows)]
    ahead = quarter_of(0)
    def load(source, target, sem):
        copy = pltpu.make_async_copy(source, target, load_sems.at[sem])
        copy.start()
        return copy

    grid_loads = [load(grid_hbm.at[span], grid.at[span], n) for n, span in enumerate(spans)]
    seeds_load = load(seeds_hbm, seeds, len(spans))

    @pl.loop(1, wav)
    def _(step):
        pl.semaphore_signal(barrier, inc=1, device_id=(level, (me + step) % wav), device_id_type=MESH)

    for other in range(1, lev):
        @pl.when(level < other)
        def _():
            pl.semaphore_signal(barrier, inc=1, device_id=(other, me), device_id_type=MESH)

    def push(source, target, phase, recv, w):
        @pl.when(w != me)
        def _():
            pltpu.make_async_remote_copy(
                src_ref=source.at[w], dst_ref=target.at[me],
                send_sem=send_sems.at[phase], recv_sem=recv_sems.at[recv],
                device_id=(level, w), device_id_type=MESH,
            ).start()

        @pl.when(w == me)
        def _():
            target[w] = source[w]

    def push_quarter(source, target, phase, recv, quarter):
        for n in range(slabs):
            push(source, target, phase, recv, quarter * slabs + n)

    def push_all(source, target, phase, recv):
        @pl.loop(0, quarters)
        def _(step):
            push_quarter(source, target, phase, recv, quarter_of(step))

    def push_steps(source, target, phase, recv, steps):
        for step in steps:
            push_quarter(source, target, phase, recv, quarter_of(step))

    def batch_of(source, target, phase, recv, first, count):
        return pltpu.make_async_remote_copy(
            src_ref=source.at[pl.ds(first, count)], dst_ref=target.at[pl.ds(first, count)],
            send_sem=send_sems.at[phase], recv_sem=recv_sems.at[recv],
            device_id=(level, (me + 1) % wav), device_id_type=MESH,
        )

    def arrive(source, target, phase, recv, count):
        batch_of(source, target, phase, recv, 0, count).wait_recv()

    def sent_all(source, target, phase):
        batch_of(source, target, phase, 0, 0, wav - 1).wait_send()

    lane = lax.broadcasted_iota(jnp.int32, (1, LANES), 1)
    signs = jnp.where(lane < HALF, 1.0, -1.0)
    layout = pieces(rows, group_rows, groups)
    wide = (0, HALF)

    def inside_part(starts, part):
        return (lane >= starts[part]) & (lane < starts[part] + tail)

    def pack(tile, starts):
        shifted = {}
        for group, at, part, start, count in layout:
            piece = jnp.where(inside_part(starts, part), tile(start, count), 0.0)
            shift = (group * tail - starts[part]) % LANES
            shifted.setdefault(group, []).append(pltpu.roll(piece, shift, 1) if shift else piece)
        packed = jnp.zeros((group_rows, LANES), jnp.float32)
        for found in shifted.values():
            whole = jnp.concatenate(found, 0) if len(found) > 1 else found[0]
            if whole.shape[0] < group_rows:
                fill = jnp.zeros((group_rows - whole.shape[0], LANES), jnp.float32)
                whole = jnp.concatenate([whole, fill], 0)
            packed = packed + whole
        return packed

    def unpack(packed, starts):
        found = {0: [], 1: []}
        for group, at, part, start, count in layout:
            piece = packed[at : at + count]
            shift = (starts[part] - group * tail) % LANES
            piece = pltpu.roll(piece, shift, 1) if shift else piece
            found[part].append(jnp.where(inside_part(starts, part), piece, 0.0))
        return jnp.concatenate(found[0], 0) + jnp.concatenate(found[1], 0)

    def quarter_starts(quarter):
        first = quarter % 2 * quarter_lanes
        return (first, first + part_lanes)

    def make_table(start, piece, lanes):
        cos_f, sin_f = start[0, piece, :fine_rows, lanes], start[1, piece, :fine_rows, lanes]

        @pl.loop(0, length // fine_rows, unroll=2)
        def _(block):
            at = pl.ds(fine_rows + block, 1)
            cos_c, sin_c = start[0, piece, at][:, lanes], start[1, piece, at][:, lanes]
            span = pl.ds(pl.multiple_of(block * fine_rows, fine_rows), fine_rows)
            value_high, value_low = halves(cos_c * cos_f - sin_c * sin_f)
            table[0, span, lanes] = value_high
            table[1, span, lanes] = value_low

    def keep(result, piece):
        for slab in range(slabs):
            w = piece * slabs + slab
            sent_a[w] = result[slab * rows : (slab + 1) * rows, :LANES]
            sent_b[w] = result[slab * rows : (slab + 1) * rows, LANES:]

    front, behind = slice(0, LANES), slice(LANES, 2 * LANES)
    ahead_wave = ahead * columns + lane % HALF
    nearby = lax.broadcasted_iota(jnp.int32, (fine_rows, 1), 0)
    afar = lax.broadcasted_iota(jnp.int32, (length // fine_rows, 1), 0) * fine_rows
    store_circle(first_seeds, slice(0, fine_rows), nearby * ahead_wave + lane // HALF * (length // 4), length)
    store_circle(first_seeds, slice(fine_rows, fine_rows + length // fine_rows), afar * ahead_wave, length)
    make_table(first_seeds, 0, front)

    def first_rows(span):
        high, low = halves(grid[span])
        grid_parts[0, span] = high
        grid_parts[1, span] = low
        return product((grid_parts[0, span], grid_parts[1, span]), (table[0, :, front], table[1, :, front]))

    grid_loads[0].wait()
    result = first_rows(spans[0])
    sent_a[ahead * slabs] = result[:rows]
    if early > rows:
        sent_a[ahead * slabs + 1, : early - rows] = result[rows:]
    pl.semaphore_wait(barrier, wav - 1 + level)
    push(sent_a, got_a, 0, 0, ahead * slabs)
    grid_loads[1].wait()
    sent_a[ahead * slabs + 1, early - rows :] = first_rows(spans[1])
    push(sent_a, got_a, 0, 0, ahead * slabs + 1)
    seeds_load.wait()
    make_table(seeds, ahead, behind)
    result = product((grid_parts[0], grid_parts[1]), (table[0, :, behind], table[1, :, behind]))
    for slab in range(slabs):
        sent_b[ahead * slabs + slab] = result[slab * rows : (slab + 1) * rows]

    later = (
        (limit_hbm, limit_ref), (order_hbm, order_ref), (strength_hbm, strength_ref), (mass_hbm, mass_ref),
        (twiddle_hbm, twiddle), (base_hbm, base), (back_seeds_hbm, back_seeds),
    )
    other_loads = [load(source, target, n) for n, (source, target) in enumerate(later)]

    @pl.loop(0, quarters)
    def _(step):
        plain_step = (step + quarters - 1) // quarters
        piece = quarter_of(step) * plain_step + quarters * (1 - plain_step)
        make_table(seeds, piece, slice(0, 2 * LANES))
        keep(product((grid_parts[0], grid_parts[1]), (table[0], table[1])), piece)

        @pl.when(step == 0)
        def _():
            for quarter in range(quarters):
                from_ref = sent_b if quarter // 2 else sent_a
                for slab in range(slabs):
                    sent_c[quarter * slabs + slab] = pack(
                        lambda start, many: from_ref[wav + slab, start : start + many], quarter_starts(quarter)
                    )
            push_all(sent_c, got_c, 2, 2)

        @pl.when(step > 0)
        def _():
            push_quarter(sent_a, got_a, 0, 0, piece)

        @pl.when(step == quarters - 1)
        def _():
            push_all(sent_b, got_b, 1, 1)

    for other in range(lev - 1):
        @pl.when(other < level)
        def _():
            pl.semaphore_signal(ready, inc=1, device_id=(other, me), device_id_type=MESH)

    for other_load in other_loads:
        other_load.wait()
    place = lax.broadcasted_iota(jnp.int32, (1, 3 * LANES), 1)
    column = place // LANES * HALF + place % HALF
    wave = my_quarter * columns + column
    valid = (column < columns) | ((column == columns) & (wave == half))
    single = (wave == 0) | (wave == half)
    out_weight = jnp.where(single, 1.0, 2.0) / float(length) ** 2
    energy_weight = jnp.where(single, 1.0, 0.5)
    all_limits = limit_ref[...].reshape(1, length)
    limits = jnp.full((1, 3 * LANES), -1, jnp.int32)
    for quarter in range(quarters):
        found = []
        for tile in range(3):
            start = quarter * columns + tile * HALF
            found += [all_limits[:, start : start + HALF]] * 2
        limits = jnp.where(my_quarter == quarter, jnp.concatenate(found, 1), limits)
    limits = jnp.where(valid, limits, -1)
    order = order_ref[my_slab]
    strength = strength_ref[my_slab]
    wave_square = wave.astype(jnp.float32) ** 2

    @pl.loop(0, wav)
    def _(m):
        row = lax.broadcasted_iota(jnp.int32, (padded, 1), 0)
        q = row * wav + m
        signed_q = jnp.where(q < half, q, q - length)
        radius = (wave_square + signed_q.astype(jnp.float32) ** 2) / (0.5 * length) ** 2
        square = radius * radius
        powered = jnp.where(order >= 3, square, 1.0) * jnp.where(order % 2 == 1, radius, square)
        inside = (jnp.abs(signed_q) <= limits) & (row < rows)
        damp[m] = jnp.where(inside, out_weight / (1.0 + strength * powered), 0.0)
        work[m, rows:] = jnp.zeros((padded - rows, LANES), jnp.float32)

    blocks = LANES // fine_rows
    plain = 2 * quarters * blocks

    def back_piece(at, target, span):
        row = pl.ds(fine_rows + at, 1)
        cos_c, sin_c = back_seeds[0, row], back_seeds[1, row]
        value_high, value_low = halves(cos_c * back_seeds[0, :fine_rows] - sin_c * back_seeds[1, :fine_rows])
        target[0, span] = value_high
        target[1, span] = value_low

    @pl.loop(0, 2 * quarters)
    def _(n):
        @pl.loop(0, blocks)
        def _(block):
            span = pl.ds(pl.multiple_of(block * fine_rows, fine_rows), fine_rows)
            back_piece(n * blocks + block, back_table.at[n], span)

    for target, steps in ((near_table, (0, quarters - 1)), (tail_table, range(1, quarters - 1))):
        for place_of, step in enumerate(steps):
            for part in range(2):
                block = 2 * place_of + part
                at = plain + 2 * quarter_of(step) + part
                back_piece(at, target, slice(block * fine_rows, (block + 1) * fine_rows))

    sum_ref[...] = jnp.zeros_like(sum_ref)
    energy_sums[...] = jnp.zeros_like(energy_sums)

    def along(value):
        value_high, value_low = halves(value)
        stacked = jnp.concatenate([value_high, value_high, value_low], 0)
        return jnp.dot(base[...], stacked, preferred_element_type=jnp.float32)

    block_rows = 24
    batch = 2

    def in_blocks(body):
        for start in range(0, rows, block_rows):
            body(start, min(block_rows, rows - start))

    def middle(tile, source, target):
        span_of = slice(tile * LANES, (tile + 1) * LANES)
        all_signs = jnp.concatenate([signs] * batch, 1)

        def split(start, many):
            span = pl.ds(start, many)
            for m, value in enumerate(eight_points([source[w, span] for w in range(wav)], -1, signs)):
                work[m, span] = value

        in_blocks(split)

        def residues(first, sums):
            found = range(first, first + batch)
            beside = lambda pick: jnp.concatenate([pick(m) for m in found], 1)
            packed_turn = beside(lambda m: twiddle[m])
            other_turn = swap(packed_turn)
            low = jnp.concatenate([lane] * batch, 1) < HALF
            cos_t = jnp.where(low, packed_turn, other_turn)
            sin_t = jnp.where(low, other_turn, -packed_turn)
            value = beside(lambda m: work[m])
            both = along(value * cos_t + swap(value) * sin_t)
            value = both[:padded] + swap(both[padded:]) * all_signs
            value = value * beside(lambda m: damp[m, :, span_of])
            sums = sums + jnp.sum((value * value).reshape(padded // 8, 8, batch * LANES), axis=0)
            both = along(value)
            value = both[:padded] - swap(both[padded:]) * all_signs
            value = value * cos_t - swap(value) * sin_t
            for n, m in enumerate(found):
                work[m] = value[:, n * LANES : (n + 1) * LANES]
            return sums

        sums = jnp.zeros((8, batch * LANES), jnp.float32)
        for first in range(0, wav, batch):
            sums = residues(first, sums)
        sums = sum(sums[:, n * LANES : (n + 1) * LANES] for n in range(batch))
        energy_sums[...] += sums * energy_weight[:, span_of]

        if tile == 1:
            announce()

        def join(start, many):
            span = pl.ds(start, many)
            for w, value in enumerate(eight_points([work[m, span] for m in range(wav)], 1, signs)):
                target[w, span] = value

        in_blocks(join)

    def wav_copy(target, slot, count=1):
        return pltpu.make_async_remote_copy(
            src_ref=energy_wav.at[pl.ds(slot, count)], dst_ref=energy_wav.at[pl.ds(slot, count)],
            send_sem=energy_sems.at[0], recv_sem=energy_sems.at[1],
            device_id=(level, target), device_id_type=MESH,
        )

    def lev_copy(target, slot, count=1):
        return pltpu.make_async_remote_copy(
            src_ref=energy_lev.at[pl.ds(slot, count)], dst_ref=energy_lev.at[pl.ds(slot, count)],
            send_sem=energy_sems.at[0], recv_sem=energy_sems.at[2],
            device_id=(target, me), device_id_type=MESH,
        )

    def announce():
        energy_wav[me] = jnp.sum(energy_sums[...], axis=0, keepdims=True)

        @pl.loop(1, wav)
        def _(step):
            wav_copy((me + step) % wav, me).start()

    arrive(sent_c, got_c, 2, 2, wav - 1)

    @pl.loop(0, wav)
    def _(w):
        rest[w] = unpack(got_c[w], wide)

    middle(2, rest, rest)

    @pl.loop(0, wav)
    def _(w):
        back_c[w] = pack(lambda start, many: rest[w, start : start + many], wide)

    arrive(sent_a, got_a, 0, 0, wav - 1)
    middle(0, got_a, back_a)
    sent_all(sent_a, got_a, 0)
    push_all(back_a, home_a, 0, 3)
    arrive(sent_b, got_b, 1, 1, wav - 1)
    middle(1, got_b, back_b)
    sent_all(sent_b, got_b, 1)
    sent_all(sent_c, got_c, 2)
    near_steps, far_steps = (0, quarters - 1), range(1, quarters - 1)
    near_count = 2 * slabs - 1
    push_steps(back_b, home_b, 1, 4, near_steps)
    push_steps(back_c, home_c, 2, 5, near_steps)
    push_steps(back_b, home_b, 1, 6, far_steps)
    for n, step in enumerate(far_steps):
        push_steps(back_c, home_c, 2, 7 + n, (step,))

    def add_pair(tile, home, steps):
        found, right = [], ([], [])
        for step in steps:
            quarter = quarter_of(step)
            found.append(jnp.concatenate([home[quarter * slabs + slab] for slab in range(slabs)], 0))
            for part in range(2):
                right[part].append(back_table[tile * quarters + quarter, part])
        left = halves(jnp.concatenate(found, 1))
        sum_ref[...] += product(left, [jnp.concatenate(part, 0) for part in right])

    arrive(back_a, home_a, 0, 3, wav - 1)

    @pl.loop(0, quarters, step=2)
    def _(step):
        add_pair(0, home_a, (step, step + 1))

    wav_copy((me + 1) % wav, 0, wav - 1).wait()

    slab_sums = []
    for slab in range(slabs):
        total = energy_wav[slab]
        for quarter in range(1, quarters):
            total = total + energy_wav[quarter * slabs + slab]
        slab_sums.append(total)
    weighted = slab_sums[0] * mass_ref[0]
    for slab in range(1, slabs):
        weighted = weighted + slab_sums[slab] * mass_ref[slab]
    energy_lev[level] = weighted

    @pl.when(level < lev - 1)
    def _():
        pl.semaphore_wait(ready, lev - 1 - level)

    for other in range(lev):
        @pl.when(level != other)
        def _():
            lev_copy(other, level).start()

    def collect_energies():
        lev_copy((level + 1) % lev, 0, lev - 1).wait()

        total = energy_lev[0]
        for other in range(1, lev):
            total = total + energy_lev[other]
        fill = jnp.zeros((8 - slabs - 1, LANES), jnp.float32)
        found = jnp.concatenate(slab_sums + [total / (lev * slabs), fill], 0)
        energy_ref[...] = jnp.broadcast_to(jnp.sum(found, axis=1, keepdims=True), found.shape)

    def with_tails(values, step, place_of):
        found = []
        for slab in range(slabs):
            value = unpack(home_c[quarter_of(step) * slabs + slab], quarter_starts(place_of))
            found.append(value if values is None else values[slab] + value)
        return found

    arrive(back_b, home_b, 1, 4, near_count)
    add_pair(1, home_b, near_steps)
    arrive(back_c, home_c, 2, 5, near_count)
    values = None
    for place_of, step in enumerate(near_steps):
        values = with_tails(values, step, place_of)
    sum_ref[...] += product(halves(jnp.concatenate(values, 0)), (near_table[0], near_table[1]))
    arrive(back_b, home_b, 1, 6, (quarters - 2) * slabs)
    add_pair(1, home_b, far_steps)
    sent_all(back_a, home_a, 0)
    sent_all(back_b, home_b, 1)
    collect_energies()
    values = None
    for n, step in enumerate(far_steps):
        arrive(back_c, home_c, 2, 7 + n, slabs)
        values = with_tails(values, step, n)
    for slab, value in enumerate(values):
        for part, found in enumerate(halves(value)):
            tail_ref[part, slab * rows : (slab + 1) * rows] = found
    sent_all(back_c, home_c, 2)


def last_kernel(
    slabs, spans, sum_ref, tail_ref, tail_table, energy_ref, out_hbm, energies_hbm, total_hbm,
    out, energies, total, sems,
):
    for slab in range(slabs):
        energies[slab] = energy_ref[slab, 0]
    total[0] = energy_ref[slabs, 0]
    copies = [
        pltpu.make_async_copy(energies, energies_hbm, sems.at[1]),
        pltpu.make_async_copy(total, total_hbm, sems.at[2]),
    ]
    for copy in copies:
        copy.start()
    for span in spans:
        out[:, span] = sum_ref[:, span] + product(
            (tail_ref[0], tail_ref[1]), (tail_table[0, :, span], tail_table[1, :, span])
        )
        pltpu.make_async_copy(out.at[:, span], out_hbm.at[:, span], sems.at[0]).start()
    for copy in copies + [pltpu.make_async_copy(out, out_hbm, sems.at[0])]:
        copy.wait()


def cos_sin(phases, length):
    angles = 2.0 * np.pi / length * (phases % length)
    return np.stack([np.cos(angles), np.sin(angles)])


def fused(grid_field, truncation_limit, diffusion_order, diffusion_strength, mass_weight):
    slabs, rows, length = grid_field.shape
    wav, lev = lax.axis_size("wav"), lax.axis_size("lev")
    quarters = wav // slabs
    columns = length // 2 // quarters
    tail = columns + 1 - LANES
    groups = LANES // tail
    group_rows = -(-2 * rows // groups)
    padded = -(-rows // 16) * 16
    fine_rows = 32
    sizes = (slabs, rows, length, wav, lev, quarters, columns, padded, tail, groups, group_rows, fine_rows)
    turn = length // 4
    place = np.arange(2 * LANES)
    starts = np.arange(quarters) * columns
    plain_waves = starts[:, None] + (place // LANES * HALF + place % HALF)[None]
    plain_phase = np.broadcast_to((place % LANES >= HALF) * turn, plain_waves.shape)
    part = LANES // 4
    tail_waves = (starts[place // HALF] + LANES + place % part)[None]
    tail_phase = (place % HALF >= part)[None] * turn
    waves = np.concatenate([plain_waves, tail_waves])
    phase = np.concatenate([plain_phase, tail_phase])
    steps = np.arange(length // fine_rows) * fine_rows
    near = np.arange(fine_rows)
    positions = np.arange(length)
    single = lambda array: jnp.asarray(array, jnp.float32)
    seeds = single(
        np.concatenate(
            [
                cos_sin(near[None, :, None] * waves[:, None, :] + phase[:, None, :], length),
                cos_sin(steps[None, :, None] * waves[:, None, :], length),
            ],
            2,
        )
    )
    by_tile = lambda array: np.concatenate(
        [array[:quarters, :LANES].ravel(), array[:quarters, LANES:].ravel(), array[quarters]]
    )[::fine_rows]
    back_seeds = single(
        np.concatenate(
            [
                cos_sin(near[:, None] * positions[None], length),
                cos_sin(by_tile(waves)[:, None] * positions[None] + by_tile(phase)[:, None], length),
            ],
            1,
        )
    )
    inner = np.arange(padded)
    turns = cos_sin(np.arange(wav)[:, None, None] * inner[None, :, None], length)
    twiddle = single(np.repeat(turns, HALF, 3).transpose(1, 2, 0, 3).reshape(wav, padded, LANES))
    base_exact = cos_sin(wav * inner[:, None] * inner[None], length)
    base_exact = base_exact * ((inner[:, None] < rows) & (inner[None] < rows))
    base_exact = base_exact.reshape(2 * padded, padded).astype(np.float32)
    base_high = base_exact.astype(jnp.bfloat16)
    base_low = (base_exact - base_high.astype(np.float32)).astype(jnp.bfloat16)
    base = jnp.asarray(np.concatenate([base_high, base_low, base_high], 1))
    vmem, hbm = pl.BlockSpec(memory_space=pltpu.VMEM), pl.BlockSpec(memory_space=pltpu.HBM)
    f32, bf16, i32 = jnp.float32, jnp.bfloat16, jnp.int32
    sent = pltpu.VMEM((wav + slabs, rows, LANES), f32)
    whole = pltpu.VMEM((wav, rows, LANES), f32)
    small = pltpu.VMEM((wav, group_rows, LANES), f32)
    dma = pltpu.SemaphoreType.DMA
    partial_sum, tails, tail_table, energy_rows = pl.pallas_call(
        functools.partial(fused_kernel, sizes),
        out_shape=(
            jax.ShapeDtypeStruct((slabs * rows, length), f32),
            jax.ShapeDtypeStruct((2, slabs * rows, LANES), bf16),
            jax.ShapeDtypeStruct((2, LANES, length), bf16),
            jax.ShapeDtypeStruct((8, LANES), f32),
        ),
        in_specs=[hbm] * 9,
        out_specs=(vmem,) * 4,
        scratch_shapes=[
            pltpu.VMEM((slabs * rows, length), f32),
            pltpu.VMEM((length,), i32),
            pltpu.SMEM((slabs,), i32),
            pltpu.SMEM((slabs,), f32),
            pltpu.SMEM((slabs,), f32),
            pltpu.VMEM(seeds.shape, f32),
            pltpu.VMEM((2, 1, seeds.shape[2], LANES), f32),
            pltpu.VMEM(back_seeds.shape, f32),
            pltpu.VMEM(twiddle.shape, f32),
            pltpu.VMEM(base.shape, bf16),
            pltpu.VMEM((2, slabs * rows, length), bf16),
            pltpu.VMEM((2, length, 2 * LANES), bf16),
            pltpu.VMEM((2 * quarters, 2, LANES, length), bf16),
            pltpu.VMEM((2, LANES, length), bf16),
            sent, sent, small, whole, whole, small, whole, whole, small, whole, whole, small,
            whole,
            pltpu.VMEM((wav, padded, LANES), f32),
            pltpu.VMEM((wav, padded, 3 * LANES), f32),
            pltpu.VMEM((8, LANES), f32),
            pltpu.VMEM((wav, 1, LANES), f32),
            pltpu.VMEM((lev, 1, LANES), f32),
            dma((7,)), dma((3,)), dma((5 + quarters,)), dma((3,)),
            pltpu.SemaphoreType.REGULAR,
        ],
        compiler_params=pltpu.CompilerParams(
            collective_id=0, has_side_effects=True, vmem_limit_bytes=40 * 1024 * 1024
        ),
        name="fused_step",
    )(
        *(
            pltpu.with_memory_space_constraint(array, pltpu.HBM)
            for array in (
                grid_field.reshape(slabs * rows, length), truncation_limit, diffusion_order,
                diffusion_strength, mass_weight, seeds, back_seeds, twiddle, base,
            )
        )
    )
    spans = [slice(at, min(at + 2 * LANES, length)) for at in range(0, length, 2 * LANES)]
    filtered, energies, total = pl.pallas_call(
        functools.partial(last_kernel, slabs, spans),
        out_shape=(
            jax.ShapeDtypeStruct((slabs * rows, length), f32),
            jax.ShapeDtypeStruct((slabs,), f32),
            jax.ShapeDtypeStruct((1,), f32),
        ),
        in_specs=[vmem] * 4,
        out_specs=(hbm,) * 3,
        scratch_shapes=[
            pltpu.VMEM((slabs * rows, length), f32),
            pltpu.SMEM((slabs,), f32),
            pltpu.SMEM((1,), f32),
            dma((3,)),
        ],
        compiler_params=pltpu.CompilerParams(vmem_limit_bytes=12 * 1024 * 1024),
        name="last_product",
    )(partial_sum, tails, tail_table, energy_rows)
    return filtered.reshape(slabs, rows, length), energies, total[0]


def fits(shape):
    slabs, rows, length = shape
    wav = lax.axis_size("wav")
    if wav != 8 or slabs != 2 or rows % 8 or length % 16 or length != rows * wav:
        return False
    columns = length * slabs // 2 // wav
    return length % 32 == 0 and LANES <= columns < LANES + LANES // 4


def local(grid_field, truncation_limit, diffusion_order, diffusion_strength, mass_weight):
    slab_count, row_count, length = grid_field.shape
    if fits(grid_field.shape):
        return fused(
            grid_field, truncation_limit, diffusion_order, diffusion_strength, mass_weight
        )
    cosine_table, sine_table = tables(length)
    filtered, partial_value = half_plane(
        grid_field, truncation_limit, diffusion_order, diffusion_strength, cosine_table, sine_table
    )
    total_slabs = lax.axis_size("lev") * slab_count
    energies = lax.psum(partial_value, "wav")
    weighted_sum = lax.psum(jnp.sum(mass_weight * energies), "lev")
    total_energy = weighted_sum / total_slabs
    return (filtered, energies, total_energy)


def solution(mesh):
    placed = (P("lev", "wav", None), P(), P("lev"), P("lev"), P("lev"))
    return jax.shard_map(
        local,
        mesh=mesh,
        in_specs=placed,
        out_specs=(P("lev", "wav", None), P("lev"), P()),
        check_vma=False,
    )
```

```python
import functools

import jax
import jax.numpy as jnp
import numpy as np
from jax import lax
from jax.experimental import pallas as pl
from jax.experimental.pallas import tpu as pltpu
from jax.sharding import PartitionSpec as P

product_precision = lax.Precision.HIGH


def tables(length):
    step = 32
    coarse = -(-length // step)
    columns = np.arange(length)
    high = 2.0 * np.pi / length * (np.arange(coarse)[:, None] * step * columns[None, :] % length)
    low = 2.0 * np.pi / length * (np.arange(step)[:, None] * columns[None, :] % length)
    cos_high, sin_high = (jnp.asarray(f(high), jnp.float32)[:, None] for f in (np.cos, np.sin))
    cos_low, sin_low = (jnp.asarray(f(low), jnp.float32)[None] for f in (np.cos, np.sin))
    cosine = cos_high * cos_low - sin_high * sin_low
    sine = sin_high * cos_low + cos_high * sin_low
    return tuple(t.reshape(coarse * step, length)[:length] for t in (cosine, sine))


def signed(positions, length):
    return jnp.where(positions < length // 2, positions, positions - length)


def transform(values, cosine_table, sine_table, direction):
    with_cosine = jnp.einsum("scpi,iq->scpq", values, cosine_table, precision=product_precision)
    with_sine = jnp.einsum("scpi,iq->scpq", values, sine_table, precision=product_precision)
    if direction < 0:
        real_part = with_cosine[:, 0] + with_sine[:, 1]
        imaginary = with_cosine[:, 1] - with_sine[:, 0]
    else:
        real_part = with_cosine[:, 0] - with_sine[:, 1]
        imaginary = with_cosine[:, 1] + with_sine[:, 0]
    return jnp.stack([real_part, imaginary], axis=1)


def damping(wave_rows, limits, length, diffusion_order, diffusion_strength):
    wave_first = signed(jnp.arange(length, dtype=jnp.int32), length)
    rows_float = wave_rows.astype(jnp.float32)
    first_float = wave_first.astype(jnp.float32)
    scaled_radius = (rows_float[:, None] ** 2 + first_float[None, :] ** 2) / (0.5 * length) ** 2
    inside = (jnp.abs(wave_first)[None, :] <= limits[:, None]).astype(jnp.float32)
    powered = jnp.power(scaled_radius[None], diffusion_order.astype(jnp.float32)[:, None, None])
    return inside[None] / (1.0 + diffusion_strength[:, None, None] * powered)


def mirrored(values):
    return jnp.roll(jnp.flip(values, -1), 1, -1)


def half_plane(
    grid_field, truncation_limit, diffusion_order, diffusion_strength, cosine_table, sine_table
):
    length = grid_field.shape[2]
    half = length // 2
    row_real = jnp.einsum("sij,jl->sli", grid_field, cosine_table[:, :half], precision=product_precision)
    row_imag = -jnp.einsum("sij,jl->sli", grid_field, sine_table[:, :half], precision=product_precision)
    nyquist = jnp.einsum("sij,j->si", grid_field, cosine_table[:, half], precision=product_precision)
    zero_row = (jnp.arange(half, dtype=jnp.int32) == 0)[None, :, None]
    row_imag = jnp.where(zero_row, nyquist[:, None, :], row_imag)
    along_rows = jnp.stack([row_real, row_imag], axis=1)
    spectrum = transform(
        lax.all_to_all(along_rows, "wav", split_axis=2, concat_axis=3, tiled=True),
        cosine_table,
        sine_table,
        -1,
    )
    column_count = spectrum.shape[2]
    wav_index = lax.axis_index("wav")
    offset = wav_index * column_count
    wave_rows = offset + jnp.arange(column_count, dtype=jnp.int32)
    limits = lax.dynamic_slice(truncation_limit, (offset,), (column_count,))
    damp_main = damping(wave_rows, limits, length, diffusion_order, diffusion_strength)
    nyquist_rows = signed(jnp.full((1,), half, jnp.int32), length)
    damp_top = damping(
        nyquist_rows, truncation_limit[half : half + 1], length, diffusion_order, diffusion_strength
    )[:, 0]
    damped = spectrum * damp_main[:, None]
    packed_real = spectrum[:, 0, 0, :]
    packed_imag = spectrum[:, 1, 0, :]
    back_real = mirrored(packed_real)
    back_imag = mirrored(packed_imag)
    zero_real = (packed_real + back_real) * 0.5 * damp_main[:, 0]
    zero_imag = (packed_imag - back_imag) * 0.5 * damp_main[:, 0]
    top_real = (packed_imag + back_imag) * 0.5 * damp_top
    top_imag = (back_real - packed_real) * 0.5 * damp_top
    is_zero = wave_rows == 0
    column_weight = jnp.where(is_zero, 0.0, 2.0).astype(jnp.float32)
    edge = jnp.sum(zero_real**2 + zero_imag**2 + top_real**2 + top_imag**2, axis=-1)
    main_sum = jnp.sum(damped * damped * column_weight[None, None, :, None], axis=(1, 2, 3))
    partial_value = (main_sum + jnp.where(wav_index == 0, edge, 0.0)) / float(length) ** 4
    zero_column = is_zero[None, :, None]
    repacked = jnp.stack(
        [
            jnp.where(zero_column, (zero_real - top_imag)[:, None, :], damped[:, 0]),
            jnp.where(zero_column, (zero_imag + top_real)[:, None, :], damped[:, 1]),
        ],
        axis=1,
    )
    along_first = transform(repacked, cosine_table, sine_table, 1)
    inverse_area = 1.0 / float(length) ** 2
    received = lax.all_to_all(along_first, "wav", split_axis=3, concat_axis=2, tiled=True)
    row_weight = jnp.where(jnp.arange(half, dtype=jnp.int32) == 0, 1.0, 2.0).astype(jnp.float32)[
        :, None
    ]
    with_cosine = jnp.einsum(
        "spi,pj->sij", received[:, 0] * row_weight, cosine_table[:half], precision=product_precision
    )
    with_sine = jnp.einsum(
        "spi,pj->sij", received[:, 1] * row_weight, sine_table[:half], precision=product_precision
    )
    top_term = received[:, 1, 0, :][:, :, None] * cosine_table[half][None, None, :]
    filtered = (with_cosine - with_sine + top_term) * inverse_area
    return (filtered, partial_value)


LANES = 128
HALF = LANES // 2
MESH = pl.DeviceIdType.MESH


def halves(values):
    high = values.astype(jnp.bfloat16)
    return high, (values - high.astype(jnp.float32)).astype(jnp.bfloat16)


def product(left, right):
    left = jnp.concatenate([left[0], left[1], left[0]], 1)
    right = jnp.concatenate([right[0], right[0], right[1]], 0)
    return jnp.dot(left, right, preferred_element_type=jnp.float32)


def swap(value):
    count = value.shape[1] // LANES
    turned = [pltpu.roll(value[:, n * LANES : (n + 1) * LANES], HALF, 1) for n in range(count)]
    return jnp.concatenate(turned, 1) if count > 1 else turned[0]


def eight_points(x, sign, signs):
    turn = signs if sign < 0 else -signs

    def four(p, q, r, t):
        a0, a1, a2, a3 = p + r, p - r, q + t, swap(q - t) * turn
        return a0 + a2, a1 + a3, a0 - a2, a1 - a3

    e = four(x[0], x[2], x[4], x[6])
    o = four(x[1], x[3], x[5], x[7])
    root = 0.5**0.5
    odd = (
        o[0],
        root * (o[1] + swap(o[1]) * turn),
        swap(o[2]) * turn,
        root * (swap(o[3]) * turn - o[3]),
    )
    return [e[n] + odd[n] for n in range(4)] + [e[n] - odd[n] for n in range(4)]


def pieces(rows, group_rows, groups):
    found = []
    for group in range(groups):
        start, stop = group * group_rows, min((group + 1) * group_rows, 2 * rows)
        while start < stop:
            part = start // rows
            end = min(stop, (part + 1) * rows)
            found.append((group, start - group * group_rows, part, start - part * rows, end - start))
            start = end
    return found


def store_circle(target, span, steps, length):
    steps = steps.astype(jnp.float32)
    turn = jnp.floor(steps * (4.0 / length) + 0.5)
    angle = (steps - turn * (length // 4)) * (2.0 * np.pi / length)
    square = angle * angle
    cosine, sine = jnp.ones_like(angle), jnp.ones_like(angle)
    for n in range(10, 0, -2):
        cosine = 1.0 - cosine * square * (1.0 / (n * (n - 1)))
        sine = 1.0 - sine * square * (1.0 / (n * (n + 1)))
    sine = sine * angle
    quadrant = turn.astype(jnp.int32) % 4
    odd = quadrant % 2 == 1
    cos_part, sin_part = jnp.where(odd, sine, cosine), jnp.where(odd, cosine, sine)
    target[0, 0, span] = jnp.where((quadrant == 1) | (quadrant == 2), -cos_part, cos_part)
    target[1, 0, span] = jnp.where(quadrant >= 2, -sin_part, sin_part)


def fused_kernel(
    sizes,
    grid_hbm, limit_hbm, order_hbm, strength_hbm, mass_hbm, seeds_hbm, back_seeds_hbm, twiddle_hbm, base_hbm,
    sum_ref, tail_ref, tail_table, energy_ref,
    grid, limit_ref, order_ref, strength_ref, mass_ref, seeds, first_seeds, back_seeds, twiddle, base,
    grid_parts, table, back_table, near_table,
    sent_a, sent_b, sent_c, got_a, got_b, got_c, back_a, back_b, back_c, home_a, home_b, home_c,
    rest, work, damp, energy_sums, energy_wav, energy_lev,
    load_sems, send_sems, recv_sems, energy_sems, ready,
):
    slabs, rows, length, wav, lev, quarters, columns, padded, tail, groups, group_rows, fine_rows = sizes
    half = length // 2
    quarter_lanes = LANES // 2
    part_lanes = quarter_lanes // 2
    me = lax.axis_index("wav")
    level = lax.axis_index("lev")
    my_quarter, my_slab = me // slabs, me % slabs

    barrier = pltpu.get_barrier_semaphore()

    def quarter_of(step):
        down, across = 1 - step % 2, 1 - step // 2
        y, x = my_quarter // 2, my_quarter % 2
        return (y + down - 2 * y * down) * 2 + (x + across - 2 * x * across)

    early = -(-rows // 16) * 16
    spans = [slice(0, early), slice(early, slabs * rows)]
    ahead = quarter_of(0)
    def load(source, target, sem):
        copy = pltpu.make_async_copy(source, target, load_sems.at[sem])
        copy.start()
        return copy

    grid_loads = [load(grid_hbm.at[span], grid.at[span], n) for n, span in enumerate(spans)]
    seeds_load = load(seeds_hbm, seeds, len(spans))

    @pl.loop(1, wav)
    def _(step):
        pl.semaphore_signal(barrier, inc=1, device_id=(level, (me + step) % wav), device_id_type=MESH)

    for other in range(1, lev):
        @pl.when(level < other)
        def _():
            pl.semaphore_signal(barrier, inc=1, device_id=(other, me), device_id_type=MESH)

    def push(source, target, phase, recv, w):
        @pl.when(w != me)
        def _():
            pltpu.make_async_remote_copy(
                src_ref=source.at[w], dst_ref=target.at[me],
                send_sem=send_sems.at[phase], recv_sem=recv_sems.at[recv],
                device_id=(level, w), device_id_type=MESH,
            ).start()

        @pl.when(w == me)
        def _():
            target[w] = source[w]

    def push_quarter(source, target, phase, recv, quarter):
        for n in range(slabs):
            push(source, target, phase, recv, quarter * slabs + n)

    def push_all(source, target, phase, recv):
        @pl.loop(0, quarters)
        def _(step):
            push_quarter(source, target, phase, recv, quarter_of(step))

    def push_steps(source, target, phase, recv, steps):
        for step in steps:
            push_quarter(source, target, phase, recv, quarter_of(step))

    def batch_of(source, target, phase, recv, first, count):
        return pltpu.make_async_remote_copy(
            src_ref=source.at[pl.ds(first, count)], dst_ref=target.at[pl.ds(first, count)],
            send_sem=send_sems.at[phase], recv_sem=recv_sems.at[recv],
            device_id=(level, (me + 1) % wav), device_id_type=MESH,
        )

    def arrive(source, target, phase, recv, count):
        batch_of(source, target, phase, recv, 0, count).wait_recv()

    def sent_all(source, target, phase):
        batch_of(source, target, phase, 0, 0, wav - 1).wait_send()

    lane = lax.broadcasted_iota(jnp.int32, (1, LANES), 1)
    signs = jnp.where(lane < HALF, 1.0, -1.0)
    layout = pieces(rows, group_rows, groups)
    wide = (0, HALF)

    def inside_part(starts, part):
        return (lane >= starts[part]) & (lane < starts[part] + tail)

    def pack(tile, starts):
        shifted = {}
        for group, at, part, start, count in layout:
            piece = jnp.where(inside_part(starts, part), tile(start, count), 0.0)
            shift = (group * tail - starts[part]) % LANES
            shifted.setdefault(group, []).append(pltpu.roll(piece, shift, 1) if shift else piece)
        packed = jnp.zeros((group_rows, LANES), jnp.float32)
        for found in shifted.values():
            whole = jnp.concatenate(found, 0) if len(found) > 1 else found[0]
            if whole.shape[0] < group_rows:
                fill = jnp.zeros((group_rows - whole.shape[0], LANES), jnp.float32)
                whole = jnp.concatenate([whole, fill], 0)
            packed = packed + whole
        return packed

    def unpack(packed, starts):
        found = {0: [], 1: []}
        for group, at, part, start, count in layout:
            piece = packed[at : at + count]
            shift = (starts[part] - group * tail) % LANES
            piece = pltpu.roll(piece, shift, 1) if shift else piece
            found[part].append(jnp.where(inside_part(starts, part), piece, 0.0))
        return jnp.concatenate(found[0], 0) + jnp.concatenate(found[1], 0)

    def quarter_starts(quarter):
        first = quarter % 2 * quarter_lanes
        return (first, first + part_lanes)

    def make_table(start, piece, lanes):
        cos_f, sin_f = start[0, piece, :fine_rows, lanes], start[1, piece, :fine_rows, lanes]

        @pl.loop(0, length // fine_rows, unroll=2)
        def _(block):
            at = pl.ds(fine_rows + block, 1)
            cos_c, sin_c = start[0, piece, at][:, lanes], start[1, piece, at][:, lanes]
            span = pl.ds(pl.multiple_of(block * fine_rows, fine_rows), fine_rows)
            value_high, value_low = halves(cos_c * cos_f - sin_c * sin_f)
            table[0, span, lanes] = value_high
            table[1, span, lanes] = value_low

    def keep(result, piece):
        for slab in range(slabs):
            w = piece * slabs + slab
            sent_a[w] = result[slab * rows : (slab + 1) * rows, :LANES]
            sent_b[w] = result[slab * rows : (slab + 1) * rows, LANES:]

    front, behind = slice(0, LANES), slice(LANES, 2 * LANES)
    ahead_wave = ahead * columns + lane % HALF
    nearby = lax.broadcasted_iota(jnp.int32, (fine_rows, 1), 0)
    afar = lax.broadcasted_iota(jnp.int32, (length // fine_rows, 1), 0) * fine_rows
    store_circle(first_seeds, slice(0, fine_rows), nearby * ahead_wave + lane // HALF * (length // 4), length)
    store_circle(first_seeds, slice(fine_rows, fine_rows + length // fine_rows), afar * ahead_wave, length)
    make_table(first_seeds, 0, front)

    def first_rows(span):
        high, low = halves(grid[span])
        grid_parts[0, span] = high
        grid_parts[1, span] = low
        return product((grid_parts[0, span], grid_parts[1, span]), (table[0, :, front], table[1, :, front]))

    grid_loads[0].wait()
    result = first_rows(spans[0])
    sent_a[ahead * slabs] = result[:rows]
    if early > rows:
        sent_a[ahead * slabs + 1, : early - rows] = result[rows:]
    pl.semaphore_wait(barrier, wav - 1 + level)
    push(sent_a, got_a, 0, 0, ahead * slabs)
    grid_loads[1].wait()
    sent_a[ahead * slabs + 1, early - rows :] = first_rows(spans[1])
    push(sent_a, got_a, 0, 0, ahead * slabs + 1)
    seeds_load.wait()
    make_table(seeds, ahead, behind)
    result = product((grid_parts[0], grid_parts[1]), (table[0, :, behind], table[1, :, behind]))
    for slab in range(slabs):
        sent_b[ahead * slabs + slab] = result[slab * rows : (slab + 1) * rows]

    later = (
        (limit_hbm, limit_ref), (order_hbm, order_ref), (strength_hbm, strength_ref), (mass_hbm, mass_ref),
        (twiddle_hbm, twiddle), (base_hbm, base), (back_seeds_hbm, back_seeds),
    )
    other_loads = [load(source, target, n) for n, (source, target) in enumerate(later)]

    @pl.loop(0, quarters)
    def _(step):
        plain_step = (step + quarters - 1) // quarters
        piece = quarter_of(step) * plain_step + quarters * (1 - plain_step)
        make_table(seeds, piece, slice(0, 2 * LANES))
        keep(product((grid_parts[0], grid_parts[1]), (table[0], table[1])), piece)

        @pl.when(step == 0)
        def _():
            for quarter in range(quarters):
                from_ref = sent_b if quarter // 2 else sent_a
                for slab in range(slabs):
                    sent_c[quarter * slabs + slab] = pack(
                        lambda start, many: from_ref[wav + slab, start : start + many], quarter_starts(quarter)
                    )
            push_all(sent_c, got_c, 2, 2)

        @pl.when(step > 0)
        def _():
            push_quarter(sent_a, got_a, 0, 0, piece)

        @pl.when(step == quarters - 1)
        def _():
            push_all(sent_b, got_b, 1, 1)

    for other in range(lev - 1):
        @pl.when(other < level)
        def _():
            pl.semaphore_signal(ready, inc=1, device_id=(other, me), device_id_type=MESH)

    for other_load in other_loads:
        other_load.wait()
    place = lax.broadcasted_iota(jnp.int32, (1, 3 * LANES), 1)
    column = place // LANES * HALF + place % HALF
    wave = my_quarter * columns + column
    valid = (column < columns) | ((column == columns) & (wave == half))
    single = (wave == 0) | (wave == half)
    out_weight = jnp.where(single, 1.0, 2.0) / float(length) ** 2
    energy_weight = jnp.where(single, 1.0, 0.5)
    all_limits = limit_ref[...].reshape(1, length)
    limits = jnp.full((1, 3 * LANES), -1, jnp.int32)
    for quarter in range(quarters):
        found = []
        for tile in range(3):
            start = quarter * columns + tile * HALF
            found += [all_limits[:, start : start + HALF]] * 2
        limits = jnp.where(my_quarter == quarter, jnp.concatenate(found, 1), limits)
    limits = jnp.where(valid, limits, -1)
    order = order_ref[my_slab]
    strength = strength_ref[my_slab]
    wave_square = wave.astype(jnp.float32) ** 2

    @pl.loop(0, wav)
    def _(m):
        row = lax.broadcasted_iota(jnp.int32, (padded, 1), 0)
        q = row * wav + m
        signed_q = jnp.where(q < half, q, q - length)
        radius = (wave_square + signed_q.astype(jnp.float32) ** 2) / (0.5 * length) ** 2
        square = radius * radius
        powered = jnp.where(order >= 3, square, 1.0) * jnp.where(order % 2 == 1, radius, square)
        inside = (jnp.abs(signed_q) <= limits) & (row < rows)
        damp[m] = jnp.where(inside, out_weight / (1.0 + strength * powered), 0.0)
        work[m, rows:] = jnp.zeros((padded - rows, LANES), jnp.float32)

    blocks = LANES // fine_rows
    plain = 2 * quarters * blocks

    def back_piece(at, target, span):
        row = pl.ds(fine_rows + at, 1)
        cos_c, sin_c = back_seeds[0, row], back_seeds[1, row]
        value_high, value_low = halves(cos_c * back_seeds[0, :fine_rows] - sin_c * back_seeds[1, :fine_rows])
        target[0, span] = value_high
        target[1, span] = value_low

    @pl.loop(0, 2 * quarters)
    def _(n):
        @pl.loop(0, blocks)
        def _(block):
            span = pl.ds(pl.multiple_of(block * fine_rows, fine_rows), fine_rows)
            back_piece(n * blocks + block, back_table.at[n], span)

    for target, steps in ((near_table, (0, quarters - 1)), (tail_table, range(quarters - 2, 0, -1))):
        for place_of, step in enumerate(steps):
            for part in range(2):
                block = 2 * place_of + part
                at = plain + 2 * quarter_of(step) + part
                back_piece(at, target, slice(block * fine_rows, (block + 1) * fine_rows))

    sum_ref[...] = jnp.zeros_like(sum_ref)
    energy_sums[...] = jnp.zeros_like(energy_sums)

    def along(value):
        value_high, value_low = halves(value)
        stacked = jnp.concatenate([value_high, value_high, value_low], 0)
        return jnp.dot(base[...], stacked, preferred_element_type=jnp.float32)

    block_rows = 24
    batch = 2

    def in_blocks(body):
        for start in range(0, rows, block_rows):
            body(start, min(block_rows, rows - start))

    def middle(tile, source, target):
        span_of = slice(tile * LANES, (tile + 1) * LANES)
        all_signs = jnp.concatenate([signs] * batch, 1)

        def split(start, many):
            span = pl.ds(start, many)
            for m, value in enumerate(eight_points([source[w, span] for w in range(wav)], -1, signs)):
                work[m, span] = value

        in_blocks(split)

        def residues(first, sums):
            found = range(first, first + batch)
            beside = lambda pick: jnp.concatenate([pick(m) for m in found], 1)
            packed_turn = beside(lambda m: twiddle[m])
            other_turn = swap(packed_turn)
            low = jnp.concatenate([lane] * batch, 1) < HALF
            cos_t = jnp.where(low, packed_turn, other_turn)
            sin_t = jnp.where(low, other_turn, -packed_turn)
            value = beside(lambda m: work[m])
            both = along(value * cos_t + swap(value) * sin_t)
            value = both[:padded] + swap(both[padded:]) * all_signs
            value = value * beside(lambda m: damp[m, :, span_of])
            sums = sums + jnp.sum((value * value).reshape(padded // 8, 8, batch * LANES), axis=0)
            both = along(value)
            value = both[:padded] - swap(both[padded:]) * all_signs
            value = value * cos_t - swap(value) * sin_t
            for n, m in enumerate(found):
                work[m] = value[:, n * LANES : (n + 1) * LANES]
            return sums

        sums = jnp.zeros((8, batch * LANES), jnp.float32)
        for first in range(0, wav, batch):
            sums = residues(first, sums)
        sums = sum(sums[:, n * LANES : (n + 1) * LANES] for n in range(batch))
        energy_sums[...] += sums * energy_weight[:, span_of]

        if tile == 1:
            announce()

        def join(start, many):
            span = pl.ds(start, many)
            for w, value in enumerate(eight_points([work[m, span] for m in range(wav)], 1, signs)):
                target[w, span] = value

        in_blocks(join)

    def wav_copy(target, slot, count=1):
        return pltpu.make_async_remote_copy(
            src_ref=energy_wav.at[pl.ds(slot, count)], dst_ref=energy_wav.at[pl.ds(slot, count)],
            send_sem=energy_sems.at[0], recv_sem=energy_sems.at[1],
            device_id=(level, target), device_id_type=MESH,
        )

    def lev_copy(target, slot, count=1):
        return pltpu.make_async_remote_copy(
            src_ref=energy_lev.at[pl.ds(slot, count)], dst_ref=energy_lev.at[pl.ds(slot, count)],
            send_sem=energy_sems.at[0], recv_sem=energy_sems.at[2],
            device_id=(target, me), device_id_type=MESH,
        )

    def announce():
        energy_wav[me] = jnp.sum(energy_sums[...], axis=0, keepdims=True)

        @pl.loop(1, wav)
        def _(step):
            wav_copy((me + step) % wav, me).start()

    arrive(sent_c, got_c, 2, 2, wav - 1)

    @pl.loop(0, wav)
    def _(w):
        rest[w] = unpack(got_c[w], wide)

    middle(2, rest, rest)

    @pl.loop(0, wav)
    def _(w):
        back_c[w] = pack(lambda start, many: rest[w, start : start + many], wide)

    arrive(sent_a, got_a, 0, 0, wav - 1)
    middle(0, got_a, back_a)
    sent_all(sent_a, got_a, 0)
    push_all(back_a, home_a, 0, 3)
    arrive(sent_b, got_b, 1, 1, wav - 1)
    middle(1, got_b, back_b)
    sent_all(sent_b, got_b, 1)
    sent_all(sent_c, got_c, 2)
    near_steps, far_steps = (0, quarters - 1), range(quarters - 2, 0, -1)
    near_count = 2 * slabs - 1
    push_steps(back_b, home_b, 1, 4, near_steps)
    push_steps(back_c, home_c, 2, 5, near_steps)
    push_steps(back_b, home_b, 1, 6, far_steps)
    for n, step in enumerate(far_steps):
        push_steps(back_c, home_c, 2, 7 + n, (step,))

    def add_pair(tile, home, steps):
        found, right = [], ([], [])
        for step in steps:
            quarter = quarter_of(step)
            found.append(jnp.concatenate([home[quarter * slabs + slab] for slab in range(slabs)], 0))
            for part in range(2):
                right[part].append(back_table[tile * quarters + quarter, part])
        left = halves(jnp.concatenate(found, 1))
        sum_ref[...] += product(left, [jnp.concatenate(part, 0) for part in right])

    arrive(back_a, home_a, 0, 3, wav - 1)

    @pl.loop(0, quarters, step=2)
    def _(step):
        add_pair(0, home_a, (step, step + 1))

    wav_copy((me + 1) % wav, 0, wav - 1).wait()

    slab_sums = []
    for slab in range(slabs):
        total = energy_wav[slab]
        for quarter in range(1, quarters):
            total = total + energy_wav[quarter * slabs + slab]
        slab_sums.append(total)
    weighted = slab_sums[0] * mass_ref[0]
    for slab in range(1, slabs):
        weighted = weighted + slab_sums[slab] * mass_ref[slab]
    energy_lev[level] = weighted

    @pl.when(level < lev - 1)
    def _():
        pl.semaphore_wait(ready, lev - 1 - level)

    for other in range(lev):
        @pl.when(level != other)
        def _():
            lev_copy(other, level).start()

    def collect_energies():
        lev_copy((level + 1) % lev, 0, lev - 1).wait()

        total = energy_lev[0]
        for other in range(1, lev):
            total = total + energy_lev[other]
        fill = jnp.zeros((8 - slabs - 1, LANES), jnp.float32)
        energy_ref[...] = jnp.concatenate(slab_sums + [total / (lev * slabs), fill], 0)

    def with_tails(values, step, place_of):
        found = []
        for slab in range(slabs):
            value = unpack(home_c[quarter_of(step) * slabs + slab], quarter_starts(place_of))
            found.append(value if values is None else values[slab] + value)
        return found

    arrive(back_b, home_b, 1, 4, near_count)
    add_pair(1, home_b, near_steps)
    arrive(back_c, home_c, 2, 5, near_count)
    values = None
    for place_of, step in enumerate(near_steps):
        values = with_tails(values, step, place_of)
    sum_ref[...] += product(halves(jnp.concatenate(values, 0)), (near_table[0], near_table[1]))
    arrive(back_b, home_b, 1, 6, (quarters - 2) * slabs)
    add_pair(1, home_b, far_steps)
    sent_all(back_a, home_a, 0)
    sent_all(back_b, home_b, 1)
    collect_energies()
    values = None
    for n, step in enumerate(far_steps):
        arrive(back_c, home_c, 2, 7 + n, slabs)
        values = with_tails(values, step, n)
    for slab, value in enumerate(values):
        for part, found in enumerate(halves(value)):
            tail_ref[part, slab * rows : (slab + 1) * rows] = found
    sent_all(back_c, home_c, 2)


def last_kernel(
    slabs, spans, sum_ref, tail_ref, tail_table, energy_ref, out_hbm, energies_hbm, total_hbm,
    out, energies, total, sems,
):
    for span in spans:
        out[:, span] = sum_ref[:, span] + product(
            (tail_ref[0], tail_ref[1]), (tail_table[0, :, span], tail_table[1, :, span])
        )
        pltpu.make_async_copy(out.at[:, span], out_hbm.at[:, span], sems.at[0]).start()
    sums = jnp.sum(energy_ref[...], axis=1, keepdims=True)
    for slab in range(slabs):
        energies[slab] = sums[slab, 0]
    total[0] = sums[slabs, 0]
    copies = [
        pltpu.make_async_copy(energies, energies_hbm, sems.at[1]),
        pltpu.make_async_copy(total, total_hbm, sems.at[2]),
    ]
    for copy in copies:
        copy.start()
    for copy in copies + [pltpu.make_async_copy(out, out_hbm, sems.at[0])]:
        copy.wait()


def cos_sin(phases, length):
    angles = 2.0 * np.pi / length * (phases % length)
    return np.stack([np.cos(angles), np.sin(angles)])


def fused(grid_field, truncation_limit, diffusion_order, diffusion_strength, mass_weight):
    slabs, rows, length = grid_field.shape
    wav, lev = lax.axis_size("wav"), lax.axis_size("lev")
    quarters = wav // slabs
    columns = length // 2 // quarters
    tail = columns + 1 - LANES
    groups = LANES // tail
    group_rows = -(-2 * rows // groups)
    padded = -(-rows // 16) * 16
    fine_rows = 32
    sizes = (slabs, rows, length, wav, lev, quarters, columns, padded, tail, groups, group_rows, fine_rows)
    turn = length // 4
    place = np.arange(2 * LANES)
    starts = np.arange(quarters) * columns
    plain_waves = starts[:, None] + (place // LANES * HALF + place % HALF)[None]
    plain_phase = np.broadcast_to((place % LANES >= HALF) * turn, plain_waves.shape)
    part = LANES // 4
    tail_waves = (starts[place // HALF] + LANES + place % part)[None]
    tail_phase = (place % HALF >= part)[None] * turn
    waves = np.concatenate([plain_waves, tail_waves])
    phase = np.concatenate([plain_phase, tail_phase])
    steps = np.arange(length // fine_rows) * fine_rows
    near = np.arange(fine_rows)
    positions = np.arange(length)
    single = lambda array: jnp.asarray(array, jnp.float32)
    seeds = single(
        np.concatenate(
            [
                cos_sin(near[None, :, None] * waves[:, None, :] + phase[:, None, :], length),
                cos_sin(steps[None, :, None] * waves[:, None, :], length),
            ],
            2,
        )
    )
    by_tile = lambda array: np.concatenate(
        [array[:quarters, :LANES].ravel(), array[:quarters, LANES:].ravel(), array[quarters]]
    )[::fine_rows]
    back_seeds = single(
        np.concatenate(
            [
                cos_sin(near[:, None] * positions[None], length),
                cos_sin(by_tile(waves)[:, None] * positions[None] + by_tile(phase)[:, None], length),
            ],
            1,
        )
    )
    inner = np.arange(padded)
    turns = cos_sin(np.arange(wav)[:, None, None] * inner[None, :, None], length)
    twiddle = single(np.repeat(turns, HALF, 3).transpose(1, 2, 0, 3).reshape(wav, padded, LANES))
    base_exact = cos_sin(wav * inner[:, None] * inner[None], length)
    base_exact = base_exact * ((inner[:, None] < rows) & (inner[None] < rows))
    base_exact = base_exact.reshape(2 * padded, padded).astype(np.float32)
    base_high = base_exact.astype(jnp.bfloat16)
    base_low = (base_exact - base_high.astype(np.float32)).astype(jnp.bfloat16)
    base = jnp.asarray(np.concatenate([base_high, base_low, base_high], 1))
    vmem, hbm = pl.BlockSpec(memory_space=pltpu.VMEM), pl.BlockSpec(memory_space=pltpu.HBM)
    f32, bf16, i32 = jnp.float32, jnp.bfloat16, jnp.int32
    sent = pltpu.VMEM((wav + slabs, rows, LANES), f32)
    whole = pltpu.VMEM((wav, rows, LANES), f32)
    small = pltpu.VMEM((wav, group_rows, LANES), f32)
    dma = pltpu.SemaphoreType.DMA
    partial_sum, tails, tail_table, energy_rows = pl.pallas_call(
        functools.partial(fused_kernel, sizes),
        out_shape=(
            jax.ShapeDtypeStruct((slabs * rows, length), f32),
            jax.ShapeDtypeStruct((2, slabs * rows, LANES), bf16),
            jax.ShapeDtypeStruct((2, LANES, length), bf16),
            jax.ShapeDtypeStruct((8, LANES), f32),
        ),
        in_specs=[hbm] * 9,
        out_specs=(vmem,) * 4,
        scratch_shapes=[
            pltpu.VMEM((slabs * rows, length), f32),
            pltpu.VMEM((length,), i32),
            pltpu.SMEM((slabs,), i32),
            pltpu.SMEM((slabs,), f32),
            pltpu.SMEM((slabs,), f32),
            pltpu.VMEM(seeds.shape, f32),
            pltpu.VMEM((2, 1, seeds.shape[2], LANES), f32),
            pltpu.VMEM(back_seeds.shape, f32),
            pltpu.VMEM(twiddle.shape, f32),
            pltpu.VMEM(base.shape, bf16),
            pltpu.VMEM((2, slabs * rows, length), bf16),
            pltpu.VMEM((2, length, 2 * LANES), bf16),
            pltpu.VMEM((2 * quarters, 2, LANES, length), bf16),
            pltpu.VMEM((2, LANES, length), bf16),
            sent, sent, small, whole, whole, small, whole, whole, small, whole, whole, small,
            whole,
            pltpu.VMEM((wav, padded, LANES), f32),
            pltpu.VMEM((wav, padded, 3 * LANES), f32),
            pltpu.VMEM((8, LANES), f32),
            pltpu.VMEM((wav, 1, LANES), f32),
            pltpu.VMEM((lev, 1, LANES), f32),
            dma((7,)), dma((3,)), dma((5 + quarters,)), dma((3,)),
            pltpu.SemaphoreType.REGULAR,
        ],
        compiler_params=pltpu.CompilerParams(
            collective_id=0, has_side_effects=True, vmem_limit_bytes=40 * 1024 * 1024
        ),
        name="fused_step",
    )(
        *(
            pltpu.with_memory_space_constraint(array, pltpu.HBM)
            for array in (
                grid_field.reshape(slabs * rows, length), truncation_limit, diffusion_order,
                diffusion_strength, mass_weight, seeds, back_seeds, twiddle, base,
            )
        )
    )
    spans = [slice(at, min(at + 2 * LANES, length)) for at in range(0, length, 2 * LANES)]
    filtered, energies, total = pl.pallas_call(
        functools.partial(last_kernel, slabs, spans),
        out_shape=(
            jax.ShapeDtypeStruct((slabs * rows, length), f32),
            jax.ShapeDtypeStruct((slabs,), f32),
            jax.ShapeDtypeStruct((1,), f32),
        ),
        in_specs=[vmem] * 4,
        out_specs=(hbm,) * 3,
        scratch_shapes=[
            pltpu.VMEM((slabs * rows, length), f32),
            pltpu.SMEM((slabs,), f32),
            pltpu.SMEM((1,), f32),
            dma((3,)),
        ],
        compiler_params=pltpu.CompilerParams(vmem_limit_bytes=12 * 1024 * 1024),
        name="last_product",
    )(partial_sum, tails, tail_table, energy_rows)
    return filtered.reshape(slabs, rows, length), energies, total[0]


def fits(shape):
    slabs, rows, length = shape
    wav = lax.axis_size("wav")
    if wav != 8 or slabs != 2 or rows % 8 or length % 16 or length != rows * wav:
        return False
    columns = length * slabs // 2 // wav
    return length % 32 == 0 and LANES <= columns < LANES + LANES // 4


def local(grid_field, truncation_limit, diffusion_order, diffusion_strength, mass_weight):
    slab_count, row_count, length = grid_field.shape
    if fits(grid_field.shape):
        return fused(
            grid_field, truncation_limit, diffusion_order, diffusion_strength, mass_weight
        )
    cosine_table, sine_table = tables(length)
    filtered, partial_value = half_plane(
        grid_field, truncation_limit, diffusion_order, diffusion_strength, cosine_table, sine_table
    )
    total_slabs = lax.axis_size("lev") * slab_count
    energies = lax.psum(partial_value, "wav")
    weighted_sum = lax.psum(jnp.sum(mass_weight * energies), "lev")
    total_energy = weighted_sum / total_slabs
    return (filtered, energies, total_energy)


def solution(mesh):
    placed = (P("lev", "wav", None), P(), P("lev"), P("lev"), P("lev"))
    return jax.shard_map(
        local,
        mesh=mesh,
        in_specs=placed,
        out_specs=(P("lev", "wav", None), P("lev"), P()),
        check_vma=False,
    )
```
